32 devices in a mesh: gx: 4 (over y, x), gy: 4 (over z), gz: 2 (over core).
Axes of the slice: x: 2, y: 2, z: 4, core: 2. Of those that a mesh axis runs over, the one named last changes fastest.
Arguments:
- right_side: float32 [128, 128, 256], P('gx', 'gy', 'gz'), may hold values from -1 to 1
- z_faces: float32 [256], P('gz'), may hold values from 0.5 to 2, as said below
- xy_coupling: float32 [5], replicated, as said below
- block_inverse: float32 [5, 256, 128], P(None, 'gz'), as said below
Outputs:
- solution: float32 [128, 128, 256], P('gx', 'gy', 'gz')
- residual: float32 [128, 128, 256], P('gx', 'gy', 'gz')
The draws below stay inside these ranges and needn't reach their ends.
Inputs may be any that keep to these rules, and one draw needn't show every extreme that they name: z_faces is positive. xy_coupling[l] lies between 2.9 * 4^-l / 128^2 and 5.5 * 4^-l / 128^2. block_inverse[l] holds, block by block, the inverses of the 128 x 128 diagonal blocks of M_l built from z_faces and xy_coupling[l].
All inputs are finite; a program needn't handle non-finite values.
Results may differ from the reference program's by a relative error of at most 0.028.
Values sent between devices are 32-bit elements; how exact they have to be, the bound alone decides.
A program may use at most 128 MiB of HBM per device.

```python
import jax
import jax.numpy as jnp
from jax import lax

CZ = 128
LEVELS = 5
SWEEPS = 2
NX = 128
NY = 128
NZ = 256


def coefficient_set(key):
    face_key = jax.random.fold_in(key, 101)
    level_key = jax.random.fold_in(key, 202)
    face_values = jnp.exp(jax.random.uniform(face_key, (NZ,), jnp.float32, jnp.log(0.5), jnp.log(2.0)))
    spread = jnp.exp(jax.random.uniform(level_key, (LEVELS,), jnp.float32, -0.3, 0.3))
    lateral = 4.0 / (CZ * CZ) * spread * 0.25 ** jnp.arange(LEVELS).astype(jnp.float32)
    return (face_values, lateral)


def draw_right_side(key, part):
    rough_key = jax.random.fold_in(key, 303)
    amplitude = 0.03
    rough = jnp.clip(jax.random.normal(rough_key, (NX, NY, NZ), jnp.float32), -4.0, 4.0)
    field = amplitude * rough
    return field.astype(jnp.float32)


def draw_z_faces(key, part):
    return coefficient_set(key)[0].astype(jnp.float32)


def draw_xy_coupling(key, part):
    return coefficient_set(key)[1].astype(jnp.float32)


def draw_block_inverse(key, part):
    face_values, lateral = coefficient_set(key)
    blocks_count = NZ // CZ
    up_values = jnp.concatenate([face_values[1:], jnp.ones((1,), jnp.float32)])
    down_rows = face_values.reshape(blocks_count, CZ)
    up_rows = up_values.reshape(blocks_count, CZ)
    identity = jnp.eye(CZ, dtype=jnp.float32)
    upper_shift = jnp.eye(CZ, k=1, dtype=jnp.float32)
    coupling = up_rows[:, :, None] * upper_shift
    base_matrix = (down_rows + up_rows)[:, :, None] * identity - coupling - jnp.swapaxes(coupling, 1, 2)
    matrices = base_matrix[None] + (4.0 * lateral)[:, None, None, None] * identity
    return jnp.linalg.inv(matrices).reshape(LEVELS, NZ, CZ).astype(jnp.float32)


def setup_inputs(seed: int = 0) -> dict:
    streams_of = jax.random.split(jax.random.key(seed), 5)
    right_side = draw_right_side(jax.random.fold_in(streams_of[4], 71), 0)
    z_faces = draw_z_faces(jax.random.fold_in(streams_of[4], 71), 0)
    xy_coupling = draw_xy_coupling(jax.random.fold_in(streams_of[4], 71), 0)
    block_inverse = draw_block_inverse(jax.random.fold_in(streams_of[4], 71), 0)
    return {"right_side": right_side, "z_faces": z_faces, "xy_coupling": xy_coupling, "block_inverse": block_inverse}


damping = 0.8
highest = lax.Precision.HIGHEST

def interface_setup(corner_aa, corner_ab, corner_ba, corner_bb, couplings):
    determinant = corner_aa * corner_bb - corner_ab * corner_ba
    corner_inverse = jnp.stack([jnp.stack([corner_bb, -corner_ab], -1), jnp.stack([-corner_ba, corner_aa], -1)], -2) / determinant[:, None, None]
    blocks_count = corner_aa.shape[0]
    identity = jnp.eye(blocks_count, dtype=corner_inverse.dtype)
    diagonal_part = jnp.einsum('kab,kl->kalb', corner_inverse, identity, precision=highest).reshape(2 * blocks_count, 2 * blocks_count)
    link_values = jnp.zeros((2 * blocks_count - 1,), corner_inverse.dtype).at[1::2].set(-couplings)
    schur_matrix = diagonal_part + jnp.diag(link_values, 1) + jnp.diag(link_values, -1)
    return (corner_inverse, diagonal_part, jnp.linalg.cholesky(schur_matrix))

def level_setup(block_inverse, z_faces, level):
    block_len = block_inverse.shape[2]
    blocks_count = z_faces.shape[0] // block_len
    inverse_blocks = block_inverse[level].reshape(blocks_count, block_len, block_len)
    last_cell = block_len - 1
    couplings = z_faces.reshape(blocks_count, block_len)[1:, 0]
    corner_inverse, diagonal_part, factor = interface_setup(inverse_blocks[:, 0, 0], inverse_blocks[:, 0, last_cell], inverse_blocks[:, last_cell, 0], inverse_blocks[:, last_cell, last_cell], couplings)
    return (inverse_blocks, corner_inverse, factor, couplings)

def line_solve(source, inverse_blocks, corner_inverse, factor, couplings):
    first_extent, second_extent, depth = source.shape
    blocks_count, block_len = (inverse_blocks.shape[0], inverse_blocks.shape[1])
    blocked = source.reshape(first_extent, second_extent, blocks_count, block_len)
    local_part = jnp.einsum('xykj,kij->xyki', blocked, inverse_blocks, precision=highest)
    end_values = jnp.stack([local_part[..., 0], local_part[..., block_len - 1]], -1)
    reduced_source = jnp.einsum('kab,xykb->kaxy', corner_inverse, end_values, precision=highest).reshape(2 * blocks_count, first_extent * second_extent)
    forward = lax.linalg.triangular_solve(factor, reduced_source, left_side=True, lower=True)
    interfaces = lax.linalg.triangular_solve(factor, forward, left_side=True, lower=True, transpose_a=True)
    interfaces = interfaces.reshape(blocks_count, 2, first_extent, second_extent).transpose(2, 3, 0, 1)
    zero_plane = jnp.zeros((first_extent, second_extent, 1), local_part.dtype)
    below_last = jnp.concatenate([zero_plane, interfaces[:, :, :-1, 1]], 2)
    above_first = jnp.concatenate([interfaces[:, :, 1:, 0], zero_plane], 2)
    zero_single = jnp.zeros((1,), couplings.dtype)
    down_coupling = jnp.concatenate([zero_single, couplings])
    up_coupling = jnp.concatenate([couplings, zero_single])
    result = local_part + (down_coupling * below_last)[..., None] * inverse_blocks[:, :, 0] + (up_coupling * above_first)[..., None] * inverse_blocks[:, :, block_len - 1]
    return result.reshape(first_extent, second_extent, depth)

def apply_operator(iterate, lateral_weight, down_faces, up_faces):
    padded = jnp.pad(iterate, 1)
    lateral = padded[:-2, 1:-1, 1:-1] + padded[2:, 1:-1, 1:-1] + padded[1:-1, :-2, 1:-1] + padded[1:-1, 2:, 1:-1]
    return lateral_weight * (4.0 * iterate - lateral) + down_faces * (iterate - padded[1:-1, 1:-1, :-2]) + up_faces * (iterate - padded[1:-1, 1:-1, 2:])

def restrict(field):
    first_extent, second_extent, depth = field.shape
    return field.reshape(first_extent // 2, 2, second_extent // 2, 2, depth).sum(axis=(1, 3)) * 0.25

def prolong(padded):
    first_extent = padded.shape[0] - 2
    second_extent = padded.shape[1] - 2
    depth = padded.shape[2]
    even_rows = 0.75 * padded[1:-1] + 0.25 * padded[:-2]
    odd_rows = 0.75 * padded[1:-1] + 0.25 * padded[2:]
    widened = jnp.stack([even_rows, odd_rows], 1).reshape(2 * first_extent, second_extent + 2, depth)
    even_rows = 0.75 * widened[:, 1:-1] + 0.25 * widened[:, :-2]
    odd_rows = 0.75 * widened[:, 1:-1] + 0.25 * widened[:, 2:]
    return jnp.stack([even_rows, odd_rows], 2).reshape(2 * first_extent, 2 * second_extent, depth)

def reference(right_side, z_faces, xy_coupling, block_inverse):
    up_faces = jnp.concatenate([z_faces[1:], jnp.ones((1,), z_faces.dtype)])
    setups = [level_setup(block_inverse, z_faces, level) for level in range(LEVELS)]

    def operator(iterate, level):
        return apply_operator(iterate, xy_coupling[level], z_faces, up_faces)

    def smooth(source, level):
        return line_solve(source, *setups[level])

    def multigrid_cycle(source, level):
        iterate = damping * smooth(source, level)
        for sweep in range(SWEEPS - 1):
            iterate = iterate + damping * smooth(source - operator(iterate, level), level)
        if level == LEVELS - 1:
            return iterate
        coarse = multigrid_cycle(restrict(source - operator(iterate, level)), level + 1)
        iterate = iterate + prolong(jnp.pad(coarse, ((1, 1), (1, 1), (0, 0))))
        for sweep in range(SWEEPS):
            iterate = iterate + damping * smooth(source - operator(iterate, level), level)
        return iterate
    solution = multigrid_cycle(right_side, 0)
    return (solution, right_side - operator(solution, 0))
```

```python
import functools

import jax
import jax.numpy as jnp
from jax import lax
from jax.experimental import pallas as pl
from jax.experimental.pallas import tpu as pltpu
from jax.sharding import PartitionSpec as P

LEVELS = 5
SWEEPS = 2


damping = 0.8
highest = lax.Precision.HIGHEST


def extended(cells, sides, width):
    for axis, dim in sides:
        count = lax.axis_size(axis)
        ends = count - 1
        head = lax.slice_in_dim(cells, 0, width, axis=dim)
        tail = lax.slice_in_dim(cells, cells.shape[dim] - width, cells.shape[dim], axis=dim)
        cells = jnp.concatenate(
            [
                lax.ppermute(tail, axis, [(i, (i + 1) % count) for i in range(ends)]),
                cells,
                lax.ppermute(head, axis, [((i + 1) % count, i) for i in range(ends)]),
            ],
            axis=dim,
        )
    return cells


def interface_setup(corner_aa, corner_ab, corner_ba, corner_bb, couplings):
    determinant = corner_aa * corner_bb - corner_ab * corner_ba
    corner_inverse = (
        jnp.stack(
            [jnp.stack([corner_bb, -corner_ab], -1), jnp.stack([-corner_ba, corner_aa], -1)], -2
        )
        / determinant[:, None, None]
    )
    blocks_count = corner_aa.shape[0]
    identity = jnp.eye(blocks_count, dtype=corner_inverse.dtype)
    diagonal_part = jnp.einsum("kab,kl->kalb", corner_inverse, identity, precision=highest).reshape(
        2 * blocks_count, 2 * blocks_count
    )
    link_values = jnp.zeros((2 * blocks_count - 1,), corner_inverse.dtype).at[1::2].set(-couplings)
    schur_matrix = diagonal_part + jnp.diag(link_values, 1) + jnp.diag(link_values, -1)
    return (corner_inverse, diagonal_part, jnp.linalg.cholesky(schur_matrix))


def make_solver(inverse_block, corner_rows, couplings, device_index, down_coupling, up_coupling):
    corner_inverse, diagonal_part, factor = interface_setup(
        corner_rows[:, 0], corner_rows[:, 1], corner_rows[:, 2], corner_rows[:, 3], couplings
    )
    block_len = inverse_block.shape[0]
    forward = lax.linalg.triangular_solve(factor, diagonal_part, left_side=True, lower=True)
    reach = lax.linalg.triangular_solve(
        factor, forward, left_side=True, lower=True, transpose_a=True
    )
    padded_reach = jnp.pad(reach, ((1, 1), (0, 0)))
    slice_rows = lax.dynamic_slice_in_dim(padded_reach, 2 * device_index, 4, 0)
    needed = jnp.stack([slice_rows[0], slice_rows[3]])

    def neighbours(end_values):
        zero_carry = jnp.zeros(end_values.shape, jnp.float32)
        nearby = zero_carry + jnp.dot(
            needed, lax.all_gather(end_values, "gz", axis=0, tiled=True), precision=highest
        )
        return (nearby[0], nearby[1])

    def solve(source):
        first_extent, second_extent, depth = source.shape
        line_count = first_extent * second_extent
        local_part = jnp.einsum("xyj,ij->xyi", source, inverse_block, precision=highest)
        end_values = jnp.stack(
            [
                local_part[:, :, 0].reshape(line_count),
                local_part[:, :, block_len - 1].reshape(line_count),
            ]
        )
        below_last, above_first = neighbours(end_values)
        return (
            local_part
            + (down_coupling * below_last).reshape(first_extent, second_extent, 1)
            * inverse_block[:, 0]
            + (up_coupling * above_first).reshape(first_extent, second_extent, 1)
            * inverse_block[:, block_len - 1]
        )

    return solve


def apply_operator(iterate, lateral_weight, down_faces, up_faces):
    padded = extended(iterate, (("gx", 0), ("gy", 1), ("gz", 2)), 1)
    lateral = (
        padded[:-2, 1:-1, 1:-1]
        + padded[2:, 1:-1, 1:-1]
        + padded[1:-1, :-2, 1:-1]
        + padded[1:-1, 2:, 1:-1]
    )
    return (
        lateral_weight * (4.0 * iterate - lateral)
        + down_faces * (iterate - padded[1:-1, 1:-1, :-2])
        + up_faces * (iterate - padded[1:-1, 1:-1, 2:])
    )


def restrict(field):
    first_extent, second_extent, depth = field.shape
    return field.reshape(first_extent // 2, 2, second_extent // 2, 2, depth).sum(axis=(1, 3)) * 0.25


def prolong(padded):
    first_extent = padded.shape[0] - 2
    second_extent = padded.shape[1] - 2
    depth = padded.shape[2]
    even_rows = 0.75 * padded[1:-1] + 0.25 * padded[:-2]
    odd_rows = 0.75 * padded[1:-1] + 0.25 * padded[2:]
    widened = jnp.stack([even_rows, odd_rows], 1).reshape(
        2 * first_extent, second_extent + 2, depth
    )
    even_rows = 0.75 * widened[:, 1:-1] + 0.25 * widened[:, :-2]
    odd_rows = 0.75 * widened[:, 1:-1] + 0.25 * widened[:, 2:]
    return jnp.stack([even_rows, odd_rows], 2).reshape(2 * first_extent, 2 * second_extent, depth)


def body(right_side, z_faces, xy_coupling, block_inverse):
    device_index = lax.axis_index("gz")
    levels_count = block_inverse.shape[0]
    last_cell = block_inverse.shape[1] - 1
    corner = jnp.stack(
        [
            block_inverse[:, 0, 0],
            block_inverse[:, 0, last_cell],
            block_inverse[:, last_cell, 0],
            block_inverse[:, last_cell, last_cell],
        ],
        -1,
    )[None]
    corners, firsts = (
        lax.all_gather(corner, "gz", axis=0, tiled=True),
        lax.all_gather(z_faces[:1], "gz", axis=0, tiled=True),
    )
    couplings = firsts[1:]
    edge_faces = jnp.concatenate([firsts, jnp.ones((1,), jnp.float32)])
    top_face = lax.dynamic_slice_in_dim(edge_faces, device_index + 1, 1, 0)
    up_faces = jnp.concatenate([z_faces[1:], top_face])
    solvers = [
        make_solver(
            block_inverse[level],
            corners[:, level],
            couplings,
            device_index,
            z_faces[0],
            top_face[0],
        )
        for level in range(levels_count)
    ]

    def operator(iterate, level):
        return apply_operator(iterate, xy_coupling[level], z_faces, up_faces)

    def multigrid_cycle(source, level):
        iterate = damping * solvers[level](source)
        iterate = iterate + damping * solvers[level](source - operator(iterate, level))
        if level == LEVELS - 1:
            return iterate
        coarse = multigrid_cycle(restrict(source - operator(iterate, level)), level + 1)
        widened = extended(coarse, (("gx", 0), ("gy", 1)), 1)
        iterate = iterate + prolong(widened)
        for sweep in range(SWEEPS):
            iterate = iterate + damping * solvers[level](source - operator(iterate, level))
        return iterate

    solution = multigrid_cycle(right_side, 0)
    return (solution, right_side - operator(solution, 0))


MESH = pl.DeviceIdType.MESH
HALOS = (4, 6, 6)
ROWS = (4, 5, 6)
YPAD = 8
SPARE = 32
DEEPEST = 3


def block_range(offset, own, halo, extent):
    start = offset * own - halo
    low = max(0, start)
    high = min(extent, (offset + 1) * own + halo)
    return low, high - low, low - start


def round_up(value, unit):
    return -(-value // unit) * unit


def split_planes(count, rows):
    return max(c for c in range(1, count + 1) if count % c == 0 and c * rows <= 448)


def cycle_kernel(geometry, f_hbm, z_hbm, e_hbm, g_hbm, sol_ref, res_ref, *scratch):
    gx_n, gy_n, gz_n, nx, ny, depth, levels = geometry
    refs = iter(scratch)
    take = lambda count: [next(refs) for _ in range(count)]
    sinv, g_all, z_all, gather, f_v, e_ref = take(6)
    X = [take(4) for _ in range(DEEPEST + 1)]
    X.append(take(2))
    C = take(DEEPEST + 1)
    E = take(DEEPEST + 1)
    (U1, G1, U2, G2, c3u, c3g, c4u, c4g, cwu, cwg) = take(10)
    UP, GP = [None, U1, U2, c3u, c4u], [None, G1, G2, c3g, c4g]
    OWN = [None] + take(DEEPEST)
    (in_sem, g_send, g_recv, h_send, h_recv, y_send, y_recv) = take(7)
    (x_send, x_recv, o_send, o_recv) = take(4)

    ix, iy, iz = lax.axis_index("gx"), lax.axis_index("gy"), lax.axis_index("gz")
    bx = ix * gz_n + iz
    bx_n = gx_n * gz_n
    f32 = jnp.float32

    def owned(level):
        return nx >> level, ny >> level

    def copy(src, dst, send, recv, device):
        return pltpu.make_async_remote_copy(
            src_ref=src,
            dst_ref=dst,
            send_sem=send,
            recv_sem=recv,
            device_id=device,
            device_id_type=MESH,
        )

    def inside(x, y):
        return (x >= 0) & (x < gx_n) & (y >= 0) & (y < gy_n)

    reach_all = max(
        gz_n - 1 - (-HALOS[0] // nx), *[-(-HALOS[k] // owned(k)[0]) for k in (1, 2)]
    )
    barrier = pltpu.get_barrier_semaphore()
    partners = jnp.int32(0)
    for dx in range(1 - bx_n, bx_n):
        for dy in range(1 - gy_n, gy_n):
            close = abs(dx) <= reach_all and abs(dy) <= 1
            if (dx == 0 and dy == 0) or not (close or dx == 0 or dy == 0):
                continue
            x, y = bx + dx, iy + dy
            ok = (x >= 0) & (x < bx_n) & (y >= 0) & (y < gy_n)

            @pl.when(ok)
            def _():
                pl.semaphore_signal(
                    barrier,
                    inc=1,
                    device_id=(x // gz_n, y, lax.rem(x, gz_n)),
                    device_id_type=MESH,
                )

            partners = partners + jnp.where(ok, 1, 0).astype(jnp.int32)

    parts = 4
    span = f_v.shape[0] // parts
    loads = [
        pltpu.make_async_copy(
            f_hbm.at[pl.ds(i * span, span)], f_v.at[pl.ds(i * span, span)], in_sem.at[i]
        )
        for i in range(parts)
    ]
    loads_g = [
        pltpu.make_async_copy(g_hbm.at[k], g_all.at[k, iz], in_sem.at[parts + k])
        for k in range(levels)
    ]
    loads_g.append(pltpu.make_async_copy(z_hbm, z_all.at[iz], in_sem.at[parts + levels]))
    loads_g.append(pltpu.make_async_copy(e_hbm, e_ref, in_sem.at[parts + levels + 2]))
    for c in loads:
        c.start()
    for c in loads_g:
        c.start()

    def setup_copies(other):
        here = (ix, iy, lax.rem(iz + other, gz_n))
        out = []
        for level in range(levels):
            block = g_all.at[level, iz]
            out.append(
                copy(block, block, g_send.at[other, level], g_recv.at[other, level], here)
            )
        face = z_all.at[iz]
        out.append(copy(face, face, g_send.at[other, levels], g_recv.at[other, levels], here))
        return out

    def start_copies():
        out = []
        reach = -(-HALOS[0] // nx)
        for t in range(-reach, gz_n + reach):
            xs, xn, xd = block_range(t, nx, HALOS[0], nx * gz_n)
            dgx, target = t // gz_n, t % gz_n
            for dy in (-1, 0, 1):
                ys, yn, yd = block_range(dy, ny, ROWS[0], ny)
                yd += YPAD - ROWS[0]
                out.append((t, dgx, target, dy, (xs, xn, xd), (ys, yn, yd)))
        return out

    plan0 = start_copies()
    R0 = X[0][0]
    local0 = []
    for entry in plan0:
        t, dgx, target, dy, (xs, xn, xd), (ys, yn, yd) = entry
        if dgx == 0 and dy == 0:
            move = pltpu.make_async_copy(
                f_hbm.at[pl.ds(xs, xn)],
                R0.at[pl.ds(xd, xn), target, pl.ds(yd, yn), :],
                in_sem.at[parts + levels + 1],
            )
            local0.append((target, move))

    for target, move in local0:

        @pl.when(iz == target)
        def _():
            move.start()

    def copy0(entry, source_z, device):
        t, dgx, target, dy, (xs, xn, xd), (ys, yn, yd) = entry
        slot = (t + gz_n) * 3 + dy + 1
        return copy(
            f_v.at[pl.ds(xs, xn), pl.ds(ys, yn), :],
            R0.at[pl.ds(xd, xn), source_z, pl.ds(yd, yn), :],
            h_send.at[0, slot],
            h_recv.at[0, slot, source_z],
            device,
        )

    def send0(start):
        for entry in plan0:
            t, dgx, target, dy = entry[:4]
            ok = inside(ix + dgx, iy + dy)
            if dgx == 0 and dy == 0:
                ok = ok & (iz != target)

            @pl.when(ok)
            def _():
                c = copy0(entry, iz, (ix + dgx, iy + dy, target))
                c.start() if start else c.wait_send()

    def recv0():
        for entry in plan0:
            t, dgx, target, dy = entry[:4]
            for source_z in range(gz_n):
                if dgx == 0 and dy == 0 and source_z == target:
                    continue

                @pl.when((iz == target) & inside(ix - dgx, iy - dy))
                def _():
                    copy0(entry, source_z, (ix - dgx, iy - dy, source_z)).wait_recv()

    for c in loads:
        c.wait()
    pl.semaphore_wait(barrier, partners)
    send0(True)
    for c in loads_g:
        c.wait()
    for other in range(1, gz_n):
        for c in setup_copies(other):
            c.start()

    def clear_edges():
        for level in range(DEEPEST):
            window = X[level][0]
            planes, zb, rows, lanes = window.shape
            halo = HALOS[level]
            n0, n1 = owned(level)
            reach = -(-halo // n0)
            for t in range(1, reach + 1):
                low = max(0, halo - t * n0)
                high = halo - (t - 1) * n0
                plane = jnp.zeros((high - low, zb, n1 + 2 * YPAD, lanes), f32)

                @pl.when(bx - t < 0)
                def _():
                    window[low:high, :, pl.ds(0, n1 + 2 * YPAD)] = plane

                low2, high2 = planes - high, planes - low

                @pl.when(bx + t >= bx_n)
                def _():
                    window[low2:high2, :, pl.ds(0, n1 + 2 * YPAD)] = plane

            edge = jnp.zeros((zb, YPAD, lanes), f32)

            @pl.when(iy == 0)
            def _():
                lax.fori_loop(0, planes, lambda i, c: zero_rows(window, i, 0, edge), 0)

            @pl.when(iy == gy_n - 1)
            def _():
                lax.fori_loop(
                    0, planes, lambda i, c: zero_rows(window, i, YPAD + n1, edge), 0
                )

    def fill(ref):
        zero = jnp.zeros(ref.shape[1:], f32)

        def step(i, _):
            ref[i] = zero
            return 0

        lax.fori_loop(0, ref.shape[0], step, 0)

    def clear_coarse():
        for ref in (*X[3][:3], C[3], X[4][0], c3u, c3g, c4u, c4g):
            fill(ref)

    def assemble(level, _):
        merged = g_all[level, 0]
        for k in range(1, gz_n):
            block = g_all[level, k]
            size, cz = merged.shape[0], block.shape[0]
            face = z_all[k][:, 0:1]
            a, d = block[0:1, 0:1], merged[size - 1 : size, size - 1 : size]
            last, first = merged[size - 1 : size], block[0:1]
            scale = face / (1.0 - face * face * a * d)
            p_row = jnp.concatenate([face * a * last, first], 1) * scale
            q_row = jnp.concatenate([last, face * d * first], 1) * scale
            top = jnp.concatenate([merged, jnp.zeros((size, cz), f32)], 1)
            low = jnp.concatenate([jnp.zeros((cz, size), f32), block], 1)
            top = top + merged[:, size - 1 : size] * p_row
            low = low + block[:, 0:1] * q_row
            merged = jnp.concatenate([top, low], 0)
        sinv[level] = (damping * merged).astype(jnp.bfloat16)
        return 0

    def plane_mask(level, i):
        n0 = owned(level)[0]
        x = bx * n0 - HALOS[level] + i
        return jnp.where((x >= 0) & (x < bx_n * n0), 1.0, 0.0).astype(f32)

    def row_mask(level, first, rows, stride):
        n1 = owned(level)[1]
        y = lax.broadcasted_iota(jnp.int32, (rows, depth), 0) * stride + first
        y = y + iy * n1 - YPAD
        return jnp.where((y >= 0) & (y < gy_n * n1), 1.0, 0.0).astype(f32)

    def region(level, shrink):
        if level < DEEPEST:
            n0, n1 = owned(level)
            h = ROWS[level] - shrink
            return HALOS[level] - h, n0 + 2 * h, YPAD - h, round_up(n1 + 2 * h, 8)
        window = X[level][0].shape
        return 1, window[0] - 2, YPAD, window[2] - 2 * YPAD

    def weights(level, p, c, r0, rows):
        e = e_ref[level]
        if level >= DEEPEST:
            return e
        mask = row_mask(level, r0, rows, 1)
        return jnp.stack([mask * (e * plane_mask(level, p + i)) for i in range(c)])

    def chunks(where):
        p0, planes, r0, rows = where
        c = split_planes(planes, rows)
        return [(p0 + s * c, c, r0, rows) for s in range(planes // c)]

    def around(src, k, p, c, r0, rows):
        at = lambda dp, dr: src[pl.ds(p + dp, c), k, pl.ds(r0 + dr, rows)]
        return (at(-1, 0) + at(1, 0)) + (at(0, -1) + at(0, 1))

    def line_solve(level, fields):
        flat = [v.reshape(-1, depth) for v in fields]
        lhs = jnp.concatenate(flat, 1).astype(jnp.bfloat16)
        out = jnp.dot(lhs, sinv[level], preferred_element_type=f32)
        shape = fields[0].shape
        return [out[:, k * depth : (k + 1) * depth].reshape(shape) for k in range(len(flat))]

    def relax(level, src, dst, where, place=None):
        for p, c, r0, rows in chunks(where):
            w = weights(level, p, c, r0, rows)
            total = [around(src, k, p, c, r0, rows) * w for k in range(gz_n)]
            out = line_solve(level, total)
            for k in range(gz_n):
                value = (1.0 - damping) * src[pl.ds(p, c), k, pl.ds(r0, rows)] + out[k]
                if place is None:
                    dst[pl.ds(p, c), k, pl.ds(r0, rows)] = value
                else:
                    dst[k, pl.ds(place + p - where[0], c)] = value

    def collect(level, where, place=None, offset=0):
        for p, c, r0, rows in chunks(where):
            at = lambda ref, k: ref[pl.ds(p, c), k, pl.ds(r0, rows)]
            total = []
            for k in range(gz_n):
                part = [at(ref, k) for ref in X[level]]
                while len(part) > 1:
                    part = [part[i] + part[i + 1] for i in range(0, len(part), 2)]
                total.append(part[0])
            out = line_solve(level, total)
            for k in range(gz_n):
                u = out[k] if level > DEEPEST else out[k] + at(C[level], k)
                if level == 0:
                    sol_ref[k, pl.ds(place + p - where[0], c)] = u
                    continue
                g = damping * total[k] + (4.0 * (e_ref[level - 1] - e_ref[level])) * u
                if level <= DEEPEST:
                    g = g + at(E[level], k)
                UP[level][pl.ds(p + offset, c), k, pl.ds(r0, rows)] = u
                GP[level][pl.ds(p + offset, c), k, pl.ds(r0, rows)] = g

    def restrict_planes(level, dst, planes, x0, y0, to_plane, to_row, rows):
        src = X[level][2]
        for j in range(planes):
            for k in range(gz_n):
                total = None
                for a in (0, 1):
                    for b in (0, 1):
                        part = src[x0 + 2 * j + a, k, pl.ds(y0 + b, rows, 2), :]
                        total = part if total is None else total + part
                dst[to_plane + j, k, pl.ds(to_row, rows), :] = total * 0.25

    def prolong(level, x0, y0, coarse):
        shift = 1 if level >= DEEPEST else 0
        p0, planes, r0, rows = region(level, 1)
        low, high = p0 - shift, p0 - shift + planes
        first = r0 // 2 * 2
        half = round_up((r0 + rows - first + 1) // 2, 8) if level < DEEPEST else rows // 2
        start = y0 + (first // 2 if level < DEEPEST else 0)
        masks = [
            row_mask(level, first + b, half, 2) if level < DEEPEST else None for b in (0, 1)
        ]
        mixes = {}

        def mixed(src, index, j, k):
            key = (index, j, k)
            if key not in mixes:
                load = lambda dy: src[x0 + j, k, pl.ds(start + dy, half), :]
                quarter = 0.25 * load(0)
                near = load(0) - quarter
                out = []
                for dy in (-1, 1):
                    value = near + 0.25 * load(dy)
                    far = 0.25 * value
                    out.append((value - far, far))
                mixes[key] = out
            return mixes[key]

        for j in range(low // 2, (high - 1) // 2 + 1):
            for a in (0, 1):
                p = 2 * j + a
                if not low <= p < high:
                    continue
                for b in (0, 1):
                    if level < DEEPEST:
                        mask = masks[b] * plane_mask(level, p)
                    for index, (src, dst) in enumerate(coarse):
                        for k in range(gz_n):
                            near = mixed(src, index, j, k)[b][0]
                            value = near + mixed(src, index, j + 2 * a - 1, k)[b][1]
                            if level < DEEPEST:
                                value = value * mask
                            dst[p + shift, k, pl.ds(first + b, half, 2), :] = value

    def correct(level, coarse_u, coarse_g, x0, y0):
        prolong(level, x0, y0, [(coarse_u, C[level]), (coarse_g, E[level])])
        where = region(level, 2)
        target = X[level][2]
        for p, c, r0, rows in chunks(where):
            w = weights(level, p, c, r0, rows)
            for k in range(gz_n):
                at = lambda ref: ref[pl.ds(p, c), k, pl.ds(r0, rows)]
                total = around(C[level], k, p, c, r0, rows) * w
                target[pl.ds(p, c), k, pl.ds(r0, rows)] = at(target) + (total - at(E[level]))

    def exchange(level, meanwhile):
        n0, n1 = owned(level)
        halo = HALOS[level]
        own = OWN[level]
        reach = -(-halo // n0)
        window = X[level][0]

        def each(act):
            slot = 0
            for t in range(-reach, reach + 1):
                xs, xn, xd = block_range(t, n0, halo, n0)
                for dy in (-1, 0, 1):
                    if t == 0 and dy == 0:
                        continue
                    ys, yn, yd = block_range(dy, n1, ROWS[level], n1)
                    yd += YPAD - ROWS[level]
                    act(t, dy, (xs, xn, xd), (ys, yn, yd), slot)
                    slot += 1

        def build(t, dy, x, y, slot):
            there = bx + t + bx_n
            return copy(
                own.at[pl.ds(x[0], x[1]), :, pl.ds(y[0], y[1]), :],
                window.at[pl.ds(x[2], x[1]), :, pl.ds(y[2], y[1]), :],
                h_send.at[level, slot],
                h_recv.at[level, slot, 0],
                (there // gz_n - gx_n, iy + dy, lax.rem(there, gz_n)),
            )

        def valid(x, y):
            return (x >= 0) & (x < bx_n) & (y >= 0) & (y < gy_n)

        def start(t, dy, x, y, slot):
            @pl.when(valid(bx + t, iy + dy))
            def _():
                build(t, dy, x, y, slot).start()

        def finish(t, dy, x, y, slot):
            @pl.when(valid(bx - t, iy - dy))
            def _():
                build(t, dy, x, y, slot).wait_recv()

        def drain(t, dy, x, y, slot):
            @pl.when(valid(bx + t, iy + dy))
            def _():
                build(t, dy, x, y, slot).wait_send()

        each(start)
        for i in range(n0):
            window[i + halo, :, pl.ds(YPAD, n1), :] = own[i]
        meanwhile()
        each(finish)
        return lambda: each(drain)

    def gather_all():
        own3 = OWN[3]

        def line_y(other, slot):
            return copy(
                own3,
                gather.at[bx, slot],
                y_send.at[other],
                y_recv.at[slot],
                (ix, other, iz),
            )

        def line_x(src, other, slot_x, slot_y):
            return copy(
                src,
                gather.at[slot_x, slot_y],
                x_send.at[other, slot_y],
                x_recv.at[slot_x, slot_y],
                (other // gz_n, iy, lax.rem(other, gz_n)),
            )

        def others(me, count, act):
            for s in range(1, count):
                act(lax.rem(me + s, count))

        others(iy, gy_n, lambda y: line_y(y, iy).start())
        others(bx, bx_n, lambda x: line_x(own3, x, bx, iy).start())
        gather[bx, iy] = own3[...]
        for distance in range(1, gy_n):
            for y in (iy + distance, iy - distance):

                @pl.when((y >= 0) & (y < gy_n))
                def _():
                    line_y(y, y).wait_recv()
                    block = gather.at[bx, y]
                    others(bx, bx_n, lambda x: line_x(block, x, bx, y).start())

        def arrive(x):
            for y in range(gy_n):
                line_x(own3, x, x, y).wait_recv()

        others(bx, bx_n, arrive)
        n0, n1 = owned(3)
        window = X[3][0]

        def place(b, _):
            for i in range(n0):
                for y in range(gy_n):
                    window[1 + b * n0 + i, :, pl.ds(YPAD + y * n1, n1), :] = gather[b, y, i]
            return 0

        lax.fori_loop(0, bx_n, place, 0)

        def drains():
            others(iy, gy_n, lambda y: line_y(y, iy).wait_send())

            def leave(x):
                for y in range(gy_n):
                    line_x(own3, x, bx, y).wait_send()

            others(bx, bx_n, leave)

        return drains

    clear_edges()
    for other in range(1, gz_n):
        for c in setup_copies(other):
            c.wait()
    assemble(0, 0)
    for target, move in local0:

        @pl.when(iz == target)
        def _():
            move.wait()

    recv0()
    drains = [lambda: send0(False)]

    def later():
        lax.fori_loop(1, levels, assemble, 0)

    for level in range(DEEPEST):
        one, two = X[level][1], X[level][2]
        relax(level, X[level][0], one, region(level, 1))
        relax(level, one, two, region(level, 2))
        n0, n1 = owned(level + 1)
        restrict_planes(level, OWN[level + 1], n0, HALOS[level], YPAD, 0, 0, n1)
        if level < DEEPEST - 1:
            drains.append(exchange(level + 1, (later, clear_coarse)[level]))
        else:
            drains.append(gather_all())

    whole3, whole4 = region(3, 0), region(4, 0)
    relax(3, X[3][0], X[3][1], whole3)
    relax(3, X[3][1], X[3][2], whole3)
    restrict_planes(3, X[4][0], whole4[1], 1, YPAD, 1, YPAD, whole4[3])
    relax(4, X[4][0], X[4][1], whole4)
    collect(4, whole4)
    correct(3, c4u, c4g, 1, YPAD)
    relax(3, X[3][2], X[3][3], whole3)
    pad3 = HALOS[2] // 2 + 1
    collect(3, whole3, offset=pad3 - 1)
    n0, n1 = owned(3)
    margin = YPAD // 2
    for y in range(gy_n):

        @pl.when(iy == y)
        def _():
            for j in range(HALOS[2] + 2 * n0):
                for src, dst in ((c3u, cwu), (c3g, cwg)):
                    dst[j, :, pl.ds(margin, n1 + 4 * margin), :] = src[
                        bx * n0 + j, :, pl.ds(y * n1, n1 + 4 * margin), :
                    ]

    for level in (2, 1, 0):
        if level == 2:
            correct(2, cwu, cwg, 1, YPAD)
        else:
            x0 = HALOS[level + 1] - HALOS[level] // 2
            correct(level, UP[level + 1], GP[level + 1], x0, YPAD // 2)
        where = region(level, 3)
        relax(level, X[level][2], X[level][3], where)
        if level:
            collect(level, where)

    def out_copies(which):
        ref = (sol_ref, res_ref)[which]
        out = []
        for other in range(1, gz_n):
            there = lax.rem(iz + other, gz_n)
            block = ref.at[there, pl.ds(iz * nx, nx)]
            out.append(
                copy(
                    block,
                    block,
                    o_send.at[which, other],
                    o_recv.at[which, other],
                    (ix, iy, there),
                )
            )
        return out

    own0 = (HALOS[0], nx, YPAD, ny)
    collect(0, own0, place=iz * nx)
    for c in out_copies(0):
        c.start()
    relax(0, X[0][3], res_ref, own0, place=iz * nx)
    for c in out_copies(1):
        c.start()
    for drain in drains:
        drain()
    for which in (0, 1):
        for c in out_copies(which):
            c.wait()


def zero_rows(ref, i, at, value):
    ref[i, :, pl.ds(at, YPAD), :] = value
    return 0


def store_kernel(pieces, sol_v, res_v, sol_hbm, res_hbm, sem):
    iz = lax.axis_index("gz")
    span = sol_hbm.shape[0] // pieces
    moves = []
    for which, (src, dst) in enumerate(((sol_v, sol_hbm), (res_v, res_hbm))):
        for i in range(pieces):
            at = pl.ds(i * span, span)
            moves.append(
                pltpu.make_async_copy(src.at[iz, at], dst.at[at], sem.at[which, i])
            )
    for move in moves:
        move.start()
    for move in moves:
        move.wait()


def fits(mesh, shape, inverse_shape):
    gx_n, gy_n, gz_n = (mesh.shape[a] for a in ("gx", "gy", "gz"))
    nx, ny = shape[0] // (gx_n * gz_n), shape[1] // gy_n
    return (
        inverse_shape[0] == LEVELS == 5
        and SWEEPS == 2
        and inverse_shape[2] == 128
        and nx % 8 == 0
        and ny % 32 == 0
        and (shape[1] >> 4) % 8 == 0
        and gz_n <= 2
    )


def fused_body(mesh, right_side, z_faces, xy_coupling, block_inverse):
    gx_n, gy_n, gz_n = (mesh.shape[a] for a in ("gx", "gy", "gz"))
    levels, _, depth = block_inverse.shape
    nx, ny = right_side.shape[0] // gz_n, right_side.shape[1]
    windows = []
    for level in range(levels):
        if level < DEEPEST:
            size = ((nx >> level) + 2 * HALOS[level], (ny >> level) + SPARE)
        else:
            size = (
                ((nx * gx_n * gz_n) >> level) + 2,
                ((ny * gy_n) >> level) + 2 * YPAD,
            )
        windows.append((size[0], gz_n, size[1], depth))
    vmem = lambda shape: pltpu.VMEM(shape, jnp.float32)
    full3, full4 = windows[3], windows[4]
    pad3 = HALOS[2] // 2 + 1
    c4 = full4
    c3 = (full3[0] - 2 + 2 * pad3,) + full3[1:]
    cw = (windows[2][0] // 2 + 2, gz_n, (ny >> 3) + 28, depth)
    reach = 2 * max(-(-HALOS[k] // (nx >> k)) for k in range(3)) + 1
    slots = 3 * max(reach, 3 * gz_n + 1)
    bx_n = gx_n * gz_n
    dma = pltpu.SemaphoreType.DMA
    own = lambda k: (nx >> k, gz_n, ny >> k, depth)
    scratch = (
        [
            pltpu.VMEM((levels, gz_n * depth, gz_n * depth), jnp.bfloat16),
            vmem((levels, gz_n, depth, depth)),
            vmem((gz_n, 1, depth)),
            vmem((bx_n, gy_n) + own(3)),
            vmem(right_side.shape),
            pltpu.SMEM((levels,), jnp.float32),
        ]
        + [vmem(w) for w in windows[: DEEPEST + 1] for _ in range(4)]
        + [vmem(full4)] * 2
        + [vmem(w) for w in windows[: DEEPEST + 1]] * 2
        + [vmem(windows[1])] * 2
        + [vmem(windows[2])] * 2
        + [vmem(c3), vmem(c3), vmem(c4), vmem(c4), vmem(cw), vmem(cw)]
        + [vmem(own(1)), vmem(own(2)), vmem(own(3))]
        + [dma((levels + 8,))]
        + [dma((gz_n, levels + 1))] * 2
        + [dma((3, slots)), dma((3, slots, gz_n))]
        + [dma((gy_n,))] * 2
        + [dma((bx_n, gy_n))] * 2
        + [dma((2, gz_n))] * 2
    )
    in_vmem = pl.BlockSpec(memory_space=pltpu.VMEM)
    in_hbm = pl.BlockSpec(memory_space=pltpu.HBM)
    staged = (gz_n,) + right_side.shape
    hold = lambda x: pltpu.with_memory_space_constraint(x, pltpu.HBM)
    halves = pl.pallas_call(
        functools.partial(cycle_kernel, (gx_n, gy_n, gz_n, nx, ny, depth, levels)),
        out_shape=[pltpu.VMEM(staged, jnp.float32)] * 2,
        in_specs=[
            in_hbm,
            in_hbm,
            in_hbm,
            in_hbm,
        ],
        out_specs=[in_vmem, in_vmem],
        scratch_shapes=scratch,
        compiler_params=pltpu.CompilerParams(
            collective_id=0, has_side_effects=True, vmem_limit_bytes=48 * 1024 * 1024
        ),
    )(hold(right_side), hold(z_faces.reshape(1, -1)), hold(xy_coupling), hold(block_inverse))
    pieces = 4
    return tuple(
        pl.pallas_call(
            functools.partial(store_kernel, pieces),
            out_shape=[jax.ShapeDtypeStruct(right_side.shape, jnp.float32)] * 2,
            in_specs=[in_vmem, in_vmem],
            out_specs=[in_hbm, in_hbm],
            scratch_shapes=[dma((2, pieces))],
        )(*[pltpu.with_memory_space_constraint(x, pltpu.VMEM) for x in halves])
    )


def solution(mesh):
    def call(right_side, z_faces, xy_coupling, block_inverse):
        local = body
        if fits(mesh, right_side.shape, block_inverse.shape):
            local = functools.partial(fused_body, mesh)
        return jax.shard_map(
            local,
            mesh=mesh,
            in_specs=(P("gx", "gy", "gz"), P("gz"), P(), P(None, "gz", None)),
            out_specs=(P("gx", "gy", "gz"), P("gx", "gy", "gz")),
            check_vma=False,
        )(right_side, z_faces, xy_coupling, block_inverse)

    return call
```

```python
import functools

import jax
import jax.numpy as jnp
from jax import lax
from jax.experimental import pallas as pl
from jax.experimental.pallas import tpu as pltpu
from jax.sharding import PartitionSpec as P

LEVELS = 5
SWEEPS = 2


damping = 0.8
highest = lax.Precision.HIGHEST


def extended(cells, sides, width):
    for axis, dim in sides:
        count = lax.axis_size(axis)
        ends = count - 1
        head = lax.slice_in_dim(cells, 0, width, axis=dim)
        tail = lax.slice_in_dim(cells, cells.shape[dim] - width, cells.shape[dim], axis=dim)
        cells = jnp.concatenate(
            [
                lax.ppermute(tail, axis, [(i, (i + 1) % count) for i in range(ends)]),
                cells,
                lax.ppermute(head, axis, [((i + 1) % count, i) for i in range(ends)]),
            ],
            axis=dim,
        )
    return cells


def interface_setup(corner_aa, corner_ab, corner_ba, corner_bb, couplings):
    determinant = corner_aa * corner_bb - corner_ab * corner_ba
    corner_inverse = (
        jnp.stack(
            [jnp.stack([corner_bb, -corner_ab], -1), jnp.stack([-corner_ba, corner_aa], -1)], -2
        )
        / determinant[:, None, None]
    )
    blocks_count = corner_aa.shape[0]
    identity = jnp.eye(blocks_count, dtype=corner_inverse.dtype)
    diagonal_part = jnp.einsum("kab,kl->kalb", corner_inverse, identity, precision=highest).reshape(
        2 * blocks_count, 2 * blocks_count
    )
    link_values = jnp.zeros((2 * blocks_count - 1,), corner_inverse.dtype).at[1::2].set(-couplings)
    schur_matrix = diagonal_part + jnp.diag(link_values, 1) + jnp.diag(link_values, -1)
    return (corner_inverse, diagonal_part, jnp.linalg.cholesky(schur_matrix))


def make_solver(inverse_block, corner_rows, couplings, device_index, down_coupling, up_coupling):
    corner_inverse, diagonal_part, factor = interface_setup(
        corner_rows[:, 0], corner_rows[:, 1], corner_rows[:, 2], corner_rows[:, 3], couplings
    )
    block_len = inverse_block.shape[0]
    forward = lax.linalg.triangular_solve(factor, diagonal_part, left_side=True, lower=True)
    reach = lax.linalg.triangular_solve(
        factor, forward, left_side=True, lower=True, transpose_a=True
    )
    padded_reach = jnp.pad(reach, ((1, 1), (0, 0)))
    slice_rows = lax.dynamic_slice_in_dim(padded_reach, 2 * device_index, 4, 0)
    needed = jnp.stack([slice_rows[0], slice_rows[3]])

    def neighbours(end_values):
        zero_carry = jnp.zeros(end_values.shape, jnp.float32)
        nearby = zero_carry + jnp.dot(
            needed, lax.all_gather(end_values, "gz", axis=0, tiled=True), precision=highest
        )
        return (nearby[0], nearby[1])

    def solve(source):
        first_extent, second_extent, depth = source.shape
        line_count = first_extent * second_extent
        local_part = jnp.einsum("xyj,ij->xyi", source, inverse_block, precision=highest)
        end_values = jnp.stack(
            [
                local_part[:, :, 0].reshape(line_count),
                local_part[:, :, block_len - 1].reshape(line_count),
            ]
        )
        below_last, above_first = neighbours(end_values)
        return (
            local_part
            + (down_coupling * below_last).reshape(first_extent, second_extent, 1)
            * inverse_block[:, 0]
            + (up_coupling * above_first).reshape(first_extent, second_extent, 1)
            * inverse_block[:, block_len - 1]
        )

    return solve


def apply_operator(iterate, lateral_weight, down_faces, up_faces):
    padded = extended(iterate, (("gx", 0), ("gy", 1), ("gz", 2)), 1)
    lateral = (
        padded[:-2, 1:-1, 1:-1]
        + padded[2:, 1:-1, 1:-1]
        + padded[1:-1, :-2, 1:-1]
        + padded[1:-1, 2:, 1:-1]
    )
    return (
        lateral_weight * (4.0 * iterate - lateral)
        + down_faces * (iterate - padded[1:-1, 1:-1, :-2])
        + up_faces * (iterate - padded[1:-1, 1:-1, 2:])
    )


def restrict(field):
    first_extent, second_extent, depth = field.shape
    return field.reshape(first_extent // 2, 2, second_extent // 2, 2, depth).sum(axis=(1, 3)) * 0.25


def prolong(padded):
    first_extent = padded.shape[0] - 2
    second_extent = padded.shape[1] - 2
    depth = padded.shape[2]
    even_rows = 0.75 * padded[1:-1] + 0.25 * padded[:-2]
    odd_rows = 0.75 * padded[1:-1] + 0.25 * padded[2:]
    widened = jnp.stack([even_rows, odd_rows], 1).reshape(
        2 * first_extent, second_extent + 2, depth
    )
    even_rows = 0.75 * widened[:, 1:-1] + 0.25 * widened[:, :-2]
    odd_rows = 0.75 * widened[:, 1:-1] + 0.25 * widened[:, 2:]
    return jnp.stack([even_rows, odd_rows], 2).reshape(2 * first_extent, 2 * second_extent, depth)


def body(right_side, z_faces, xy_coupling, block_inverse):
    device_index = lax.axis_index("gz")
    levels_count = block_inverse.shape[0]
    last_cell = block_inverse.shape[1] - 1
    corner = jnp.stack(
        [
            block_inverse[:, 0, 0],
            block_inverse[:, 0, last_cell],
            block_inverse[:, last_cell, 0],
            block_inverse[:, last_cell, last_cell],
        ],
        -1,
    )[None]
    corners, firsts = (
        lax.all_gather(corner, "gz", axis=0, tiled=True),
        lax.all_gather(z_faces[:1], "gz", axis=0, tiled=True),
    )
    couplings = firsts[1:]
    edge_faces = jnp.concatenate([firsts, jnp.ones((1,), jnp.float32)])
    top_face = lax.dynamic_slice_in_dim(edge_faces, device_index + 1, 1, 0)
    up_faces = jnp.concatenate([z_faces[1:], top_face])
    solvers = [
        make_solver(
            block_inverse[level],
            corners[:, level],
            couplings,
            device_index,
            z_faces[0],
            top_face[0],
        )
        for level in range(levels_count)
    ]

    def operator(iterate, level):
        return apply_operator(iterate, xy_coupling[level], z_faces, up_faces)

    def multigrid_cycle(source, level):
        iterate = damping * solvers[level](source)
        iterate = iterate + damping * solvers[level](source - operator(iterate, level))
        if level == LEVELS - 1:
            return iterate
        coarse = multigrid_cycle(restrict(source - operator(iterate, level)), level + 1)
        widened = extended(coarse, (("gx", 0), ("gy", 1)), 1)
        iterate = iterate + prolong(widened)
        for sweep in range(SWEEPS):
            iterate = iterate + damping * solvers[level](source - operator(iterate, level))
        return iterate

    solution = multigrid_cycle(right_side, 0)
    return (solution, right_side - operator(solution, 0))


MESH = pl.DeviceIdType.MESH
HALOS = (4, 6, 6)
ROWS = (4, 5, 6)
YPAD = 8
SPARE = 32
DEEPEST = 3


def block_range(offset, own, halo, extent):
    start = offset * own - halo
    low = max(0, start)
    high = min(extent, (offset + 1) * own + halo)
    return low, high - low, low - start


def round_up(value, unit):
    return -(-value // unit) * unit


def split_planes(count, rows):
    return max(c for c in range(1, count + 1) if count % c == 0 and c * rows <= 448)


def cycle_kernel(geometry, f_hbm, z_hbm, e_hbm, g_hbm, sol_ref, res_ref, *scratch):
    gx_n, gy_n, gz_n, nx, ny, depth, levels = geometry
    refs = iter(scratch)
    take = lambda count: [next(refs) for _ in range(count)]
    sinv, g_all, z_all, gather, f_v, e_ref = take(6)
    X = [take(4) for _ in range(DEEPEST + 1)]
    X.append(take(2))
    C = take(DEEPEST + 1)
    E = take(DEEPEST + 1)
    (U1, G1, U2, G2, c3u, c3g, c4u, c4g, cwu, cwg) = take(10)
    UP, GP = [None, U1, U2, c3u, c4u], [None, G1, G2, c3g, c4g]
    own3, pool = take(2)
    (in_sem, g_send, g_recv, h_send, h_recv, y_recv, p_sem) = take(7)
    y_send, x_send, x_recv, o_send, o_recv = [p_sem.at[i] for i in range(5)]

    ix, iy, iz = lax.axis_index("gx"), lax.axis_index("gy"), lax.axis_index("gz")
    bx = ix * gz_n + iz
    bx_n = gx_n * gz_n
    f32 = jnp.float32

    def owned(level):
        return nx >> level, ny >> level

    def copy(src, dst, send, recv, device):
        return pltpu.make_async_remote_copy(
            src_ref=src,
            dst_ref=dst,
            send_sem=send,
            recv_sem=recv,
            device_id=device,
            device_id_type=MESH,
        )

    def inside(x, y):
        return (x >= 0) & (x < gx_n) & (y >= 0) & (y < gy_n)

    parts = 4
    span = f_v.shape[0] // parts
    for i in range(parts):
        at = pl.ds(i * span, span)
        pltpu.make_async_copy(f_hbm.at[at], f_v.at[at], in_sem.at[0]).start()
    f_load = pltpu.make_async_copy(f_hbm, f_v, in_sem.at[0])
    rest = pl.ds(1, levels - 1)
    loads = [
        pltpu.make_async_copy(z_hbm, z_all.at[iz], in_sem.at[1]),
        pltpu.make_async_copy(g_hbm.at[0], g_all.at[0, iz], in_sem.at[2]),
        pltpu.make_async_copy(g_hbm.at[rest], g_all.at[rest, iz], in_sem.at[3]),
        pltpu.make_async_copy(e_hbm, e_ref, in_sem.at[4]),
    ]
    for c in loads:
        c.start()

    reach_all = max(
        gz_n - 1 - (-HALOS[0] // nx), *[-(-HALOS[k] // owned(k)[0]) for k in (1, 2)]
    )
    barrier = pltpu.get_barrier_semaphore()
    partners = jnp.int32(0)
    for dx in range(1 - bx_n, bx_n):
        for dy in range(1 - gy_n, gy_n):
            close = abs(dx) <= reach_all and abs(dy) <= 1
            if (dx == 0 and dy == 0) or not (close or dx == 0 or dy == 0):
                continue
            x, y = bx + dx, iy + dy
            ok = (x >= 0) & (x < bx_n) & (y >= 0) & (y < gy_n)

            @pl.when(ok)
            def _():
                pl.semaphore_signal(
                    barrier,
                    inc=1,
                    device_id=(x // gz_n, y, lax.rem(x, gz_n)),
                    device_id_type=MESH,
                )

            partners = partners + jnp.where(ok, 1, 0).astype(jnp.int32)

    def setup_copies(other):
        here = (ix, iy, lax.rem(iz + other, gz_n))
        out = []
        for i, block in enumerate((z_all.at[iz], g_all.at[0, iz], g_all.at[rest, iz])):
            out.append(copy(block, block, g_send.at[other, i], g_recv.at[other, i], here))
        return out

    def runs(count, key):
        out = []
        for i in range(count):
            if out and key(i) == out[-1][2]:
                out[-1][1] = i
            else:
                out.append([i, i, key(i)])
        return [(low, high) for low, high, _ in out]

    def take_rows(sem, rows):
        block = pool.at[pl.ds(0, rows)]
        pltpu.make_async_copy(block, block, sem).wait()

    def settle(sem, total):
        table = [[total(b, y) for y in range(gy_n)] for b in range(bx_n)]
        for low, high in runs(bx_n, lambda b: table[b]):
            for first, last in runs(gy_n, lambda y: [row[y] for row in table]):

                @pl.when((bx >= low) & (bx <= high) & (iy >= first) & (iy <= last))
                def _():
                    take_rows(sem, table[low][first])

    def start_copies():
        out = []
        reach = -(-HALOS[0] // nx)
        for t in range(-reach, gz_n + reach):
            xs, xn, xd = block_range(t, nx, HALOS[0], nx * gz_n)
            dgx, target = t // gz_n, t % gz_n
            for dy in (-1, 0, 1):
                ys, yn, yd = block_range(dy, ny, ROWS[0], ny)
                yd += YPAD - ROWS[0]
                out.append((t, dgx, target, dy, (xs, xn, xd), (ys, yn, yd)))
        return out

    plan0 = start_copies()
    R0 = X[0][0]
    local0 = []
    for entry in plan0:
        t, dgx, target, dy, (xs, xn, xd), (ys, yn, yd) = entry
        if dgx == 0 and dy == 0:
            move = pltpu.make_async_copy(
                f_hbm.at[pl.ds(xs, xn)],
                R0.at[pl.ds(xd, xn), target, pl.ds(yd, yn), :],
                in_sem.at[5],
            )
            local0.append((target, move))

    for target, move in local0:

        @pl.when(iz == target)
        def _():
            move.start()

    def copy0(entry, source_z, device):
        t, dgx, target, dy, (xs, xn, xd), (ys, yn, yd) = entry
        return copy(
            f_v.at[pl.ds(xs, xn), pl.ds(ys, yn), :],
            R0.at[pl.ds(xd, xn), source_z, pl.ds(yd, yn), :],
            h_send.at[0],
            h_recv.at[0],
            device,
        )

    def send0():
        for entry in plan0:
            t, dgx, target, dy = entry[:4]
            ok = inside(ix + dgx, iy + dy)
            if dgx == 0 and dy == 0:
                ok = ok & (iz != target)

            @pl.when(ok)
            def _():
                copy0(entry, iz, (ix + dgx, iy + dy, target)).start()

    def in_grid(b, y):
        return 0 <= b < bx_n and 0 <= y < gy_n

    def sent0(b, y):
        total = 0
        for t, dgx, target, dy, (_, xn, _), (_, yn, _) in plan0:
            there = (b // gz_n + dgx) * gz_n + target
            if in_grid(there, y + dy) and (there, dy) != (b, 0):
                total += xn * yn
        return total

    def received0(b, y):
        total = 0
        for t, dgx, target, dy, (_, xn, _), (_, yn, _) in plan0:
            for source_z in range(gz_n):
                there = (b // gz_n - dgx) * gz_n + source_z
                if target == b % gz_n and in_grid(there, y - dy) and (there, dy) != (b, 0):
                    total += xn * yn
        return total

    def clear_edges():
        for level in range(DEEPEST):
            window = X[level][0]
            planes, zb, rows, lanes = window.shape
            halo = HALOS[level]
            n0, n1 = owned(level)
            reach = -(-halo // n0)
            for t in range(1, reach + 1):
                low = max(0, halo - t * n0)
                high = halo - (t - 1) * n0
                plane = jnp.zeros((high - low, zb, n1 + 2 * YPAD, lanes), f32)

                @pl.when(bx - t < 0)
                def _():
                    window[low:high, :, pl.ds(0, n1 + 2 * YPAD)] = plane

                low2, high2 = planes - high, planes - low

                @pl.when(bx + t >= bx_n)
                def _():
                    window[low2:high2, :, pl.ds(0, n1 + 2 * YPAD)] = plane

            edge = jnp.zeros((zb, YPAD, lanes), f32)

            @pl.when(iy == 0)
            def _():
                lax.fori_loop(0, planes, lambda i, c: zero_rows(window, i, 0, edge), 0)

            @pl.when(iy == gy_n - 1)
            def _():
                lax.fori_loop(
                    0, planes, lambda i, c: zero_rows(window, i, YPAD + n1, edge), 0
                )

    def fill(ref):
        zero = jnp.zeros(ref.shape[1:], f32)

        def step(i, _):
            ref[i] = zero
            return 0

        lax.fori_loop(0, ref.shape[0], step, 0)

    def clear_coarse():
        for ref in (*X[3][:3], C[3], X[4][0], c3u, c3g, c4u, c4g):
            fill(ref)

    def assemble(level, _):
        merged = g_all[level, 0]
        for k in range(1, gz_n):
            block = g_all[level, k]
            size, cz = merged.shape[0], block.shape[0]
            face = z_all[k][:, 0:1]
            a, d = block[0:1, 0:1], merged[size - 1 : size, size - 1 : size]
            last, first = merged[size - 1 : size], block[0:1]
            scale = face / (1.0 - face * face * a * d)
            p_row = jnp.concatenate([face * a * last, first], 1) * scale
            q_row = jnp.concatenate([last, face * d * first], 1) * scale
            top = jnp.concatenate([merged, jnp.zeros((size, cz), f32)], 1)
            low = jnp.concatenate([jnp.zeros((cz, size), f32), block], 1)
            top = top + merged[:, size - 1 : size] * p_row
            low = low + block[:, 0:1] * q_row
            merged = jnp.concatenate([top, low], 0)
        sinv[level] = (damping * merged).astype(jnp.bfloat16)
        return 0

    def plane_mask(level, i):
        n0 = owned(level)[0]
        x = bx * n0 - HALOS[level] + i
        return jnp.where((x >= 0) & (x < bx_n * n0), 1.0, 0.0).astype(f32)

    def row_mask(level, first, rows, stride):
        n1 = owned(level)[1]
        y = lax.broadcasted_iota(jnp.int32, (rows, depth), 0) * stride + first
        y = y + iy * n1 - YPAD
        return jnp.where((y >= 0) & (y < gy_n * n1), 1.0, 0.0).astype(f32)

    def region(level, shrink):
        if level < DEEPEST:
            n0, n1 = owned(level)
            h = ROWS[level] - shrink
            return HALOS[level] - h, n0 + 2 * h, YPAD - h, round_up(n1 + 2 * h, 8)
        window = X[level][0].shape
        return 1, window[0] - 2, YPAD, window[2] - 2 * YPAD

    def weights(level, p, c, r0, rows):
        e = e_ref[level]
        if level >= DEEPEST:
            return e
        mask = row_mask(level, r0, rows, 1)
        return jnp.stack([mask * (e * plane_mask(level, p + i)) for i in range(c)])

    def chunks(where):
        p0, planes, r0, rows = where
        c = split_planes(planes, rows)
        return [(p0 + s * c, c, r0, rows) for s in range(planes // c)]

    def around(src, k, p, c, r0, rows):
        at = lambda dp, dr: src[pl.ds(p + dp, c), k, pl.ds(r0 + dr, rows)]
        return (at(-1, 0) + at(1, 0)) + (at(0, -1) + at(0, 1))

    def line_solve(level, fields):
        flat = [v.reshape(-1, depth) for v in fields]
        lhs = jnp.concatenate(flat, 1).astype(jnp.bfloat16)
        out = jnp.dot(lhs, sinv[level], preferred_element_type=f32)
        shape = fields[0].shape
        return [out[:, k * depth : (k + 1) * depth].reshape(shape) for k in range(len(flat))]

    def relax(level, src, dst, where, place=None):
        for p, c, r0, rows in chunks(where):
            w = weights(level, p, c, r0, rows)
            total = [around(src, k, p, c, r0, rows) * w for k in range(gz_n)]
            out = line_solve(level, total)
            for k in range(gz_n):
                value = (1.0 - damping) * src[pl.ds(p, c), k, pl.ds(r0, rows)] + out[k]
                if place is None:
                    dst[pl.ds(p, c), k, pl.ds(r0, rows)] = value
                else:
                    dst[k, pl.ds(place + p - where[0], c)] = value

    def collect(level, where, place=None, offset=0):
        for p, c, r0, rows in chunks(where):
            at = lambda ref, k: ref[pl.ds(p, c), k, pl.ds(r0, rows)]
            total = []
            for k in range(gz_n):
                part = [at(ref, k) for ref in X[level]]
                while len(part) > 1:
                    part = [part[i] + part[i + 1] for i in range(0, len(part), 2)]
                total.append(part[0])
            out = line_solve(level, total)
            for k in range(gz_n):
                u = out[k] if level > DEEPEST else out[k] + at(C[level], k)
                if level == 0:
                    sol_ref[k, pl.ds(place + p - where[0], c)] = u
                    continue
                g = damping * total[k] + (4.0 * (e_ref[level - 1] - e_ref[level])) * u
                if level <= DEEPEST:
                    g = g + at(E[level], k)
                UP[level][pl.ds(p + offset, c), k, pl.ds(r0, rows)] = u
                GP[level][pl.ds(p + offset, c), k, pl.ds(r0, rows)] = g

    def restrict_planes(level, dst, planes, x0, y0, to_plane, to_row, rows):
        src = X[level][2]
        for j in range(planes):
            for k in range(gz_n):
                total = None
                for a in (0, 1):
                    for b in (0, 1):
                        part = src[x0 + 2 * j + a, k, pl.ds(y0 + b, rows, 2), :]
                        total = part if total is None else total + part
                dst[to_plane + j, k, pl.ds(to_row, rows), :] = total * 0.25

    def prolong(level, x0, y0, coarse):
        shift = 1 if level >= DEEPEST else 0
        p0, planes, r0, rows = region(level, 1)
        low, high = p0 - shift, p0 - shift + planes
        first = r0 // 2 * 2
        half = round_up((r0 + rows - first + 1) // 2, 8) if level < DEEPEST else rows // 2
        start = y0 + (first // 2 if level < DEEPEST else 0)
        masks = [
            row_mask(level, first + b, half, 2) if level < DEEPEST else None for b in (0, 1)
        ]
        mixes = {}

        def mixed(src, index, j, k):
            key = (index, j, k)
            if key not in mixes:
                load = lambda dy: src[x0 + j, k, pl.ds(start + dy, half), :]
                quarter = 0.25 * load(0)
                near = load(0) - quarter
                out = []
                for dy in (-1, 1):
                    value = near + 0.25 * load(dy)
                    far = 0.25 * value
                    out.append((value - far, far))
                mixes[key] = out
            return mixes[key]

        for j in range(low // 2, (high - 1) // 2 + 1):
            for a in (0, 1):
                p = 2 * j + a
                if not low <= p < high:
                    continue
                for b in (0, 1):
                    if level < DEEPEST:
                        mask = masks[b] * plane_mask(level, p)
                    for index, (src, dst) in enumerate(coarse):
                        for k in range(gz_n):
                            near = mixed(src, index, j, k)[b][0]
                            value = near + mixed(src, index, j + 2 * a - 1, k)[b][1]
                            if level < DEEPEST:
                                value = value * mask
                            dst[p + shift, k, pl.ds(first + b, half, 2), :] = value

    def correct(level, coarse_u, coarse_g, x0, y0):
        prolong(level, x0, y0, [(coarse_u, C[level]), (coarse_g, E[level])])
        where = region(level, 2)
        target = X[level][2]
        for p, c, r0, rows in chunks(where):
            w = weights(level, p, c, r0, rows)
            for k in range(gz_n):
                at = lambda ref: ref[pl.ds(p, c), k, pl.ds(r0, rows)]
                total = around(C[level], k, p, c, r0, rows) * w
                target[pl.ds(p, c), k, pl.ds(r0, rows)] = at(target) + (total - at(E[level]))

    def spans(own, reach, width, start):
        out = {0: (start - 1, own + 2)}
        near = 2
        for t in range(1, reach + 1):
            far = min(width, t * own + 1)
            if far >= near:
                out[t] = (start - far, far - near + 1)
                out[-t] = (start + own - 1 + near, far - near + 1)
            near = far + 1
        return out

    def exchange(level, meanwhile):
        n0, n1 = owned(level)
        width = ROWS[level]
        window = X[level][0]
        along_x = spans(n0, -(-width // n0), width, HALOS[level])
        along_y = spans(n1, 1, width, YPAD)
        pieces = [(t, dy) for t in along_x for dy in along_y if t or dy]

        def valid(x, y):
            return (x >= 0) & (x < bx_n) & (y >= 0) & (y < gy_n)

        for t, dy in pieces:
            (p, planes), (r, rows) = along_x[t], along_y[dy]
            there = bx + t + bx_n

            @pl.when(valid(bx + t, iy + dy))
            def _():
                copy(
                    window.at[pl.ds(p + t * n0, planes), :, pl.ds(r + dy * n1, rows), :],
                    window.at[pl.ds(p, planes), :, pl.ds(r, rows), :],
                    h_send.at[level],
                    h_recv.at[level],
                    (there // gz_n - gx_n, iy + dy, lax.rem(there, gz_n)),
                ).start()

        def total(sign):
            def count(b, y):
                return sum(
                    gz_n * along_x[t][1] * along_y[dy][1]
                    for t, dy in pieces
                    if in_grid(b + sign * t, y + sign * dy)
                )

            return count

        meanwhile()
        settle(h_recv.at[level], total(-1))
        return lambda: settle(h_send.at[level], total(1))

    def gather_all():
        def line_y(other, slot):
            return copy(own3, gather.at[bx, slot], y_send, y_recv.at[slot], (ix, other, iz))

        def line_x(src, other, slot_x, slot_y):
            return copy(
                src,
                gather.at[slot_x, slot_y],
                x_send,
                x_recv,
                (other // gz_n, iy, lax.rem(other, gz_n)),
            )

        def others(me, count, act):
            for s in range(1, count):
                act(lax.rem(me + s, count))

        others(iy, gy_n, lambda y: line_y(y, iy).start())
        others(bx, bx_n, lambda x: line_x(own3, x, bx, iy).start())
        gather[bx, iy] = own3[...]
        for distance in range(1, gy_n):
            for y in (iy + distance, iy - distance):

                @pl.when((y >= 0) & (y < gy_n))
                def _():
                    line_y(y, y).wait_recv()
                    block = gather.at[bx, y]
                    others(bx, bx_n, lambda x: line_x(block, x, bx, y).start())

        size = own3.shape[0] * own3.shape[1] * own3.shape[2]
        take_rows(x_recv, (bx_n - 1) * gy_n * size)
        n0, n1 = owned(3)
        window = X[3][0]

        def place(b, _):
            for i in range(n0):
                for y in range(gy_n):
                    window[1 + b * n0 + i, :, pl.ds(YPAD + y * n1, n1), :] = gather[b, y, i]
            return 0

        lax.fori_loop(0, bx_n, place, 0)

        def drains():
            take_rows(y_send, (gy_n - 1) * size)
            take_rows(x_send, (bx_n - 1) * gy_n * size)

        return drains

    clear_edges()
    f_load.wait()
    pl.semaphore_wait(barrier, partners)
    send0()
    for c in loads:
        c.wait()
    setups = [setup_copies(other) for other in range(1, gz_n)]
    for group in setups:
        for c in group:
            c.start()
    for group in setups:
        for c in group[:2]:
            c.wait()
    assemble(0, 0)
    for target, move in local0:

        @pl.when(iz == target)
        def _():
            move.wait()

    settle(h_recv.at[0], received0)
    drains = [lambda: settle(h_send.at[0], sent0)]

    def later():
        for group in setups:
            group[2].wait()
        lax.fori_loop(1, levels, assemble, 0)

    for level in range(DEEPEST):
        one, two = X[level][1], X[level][2]
        relax(level, X[level][0], one, region(level, 1))
        relax(level, one, two, region(level, 2))
        n0, n1 = owned(level + 1)
        p, r = HALOS[level], YPAD
        if level < DEEPEST - 1:
            to_plane = HALOS[level + 1] - 1
            window = X[level + 1][0]
            restrict_planes(level, window, n0 + 2, p - 2, r - 2, to_plane, YPAD - 1, n1 + 2)
            drains.append(exchange(level + 1, (later, clear_coarse)[level]))
        else:
            restrict_planes(level, own3, n0, p, r, 0, 0, n1)
            drains.append(gather_all())

    whole3, whole4 = region(3, 0), region(4, 0)
    relax(3, X[3][0], X[3][1], whole3)
    relax(3, X[3][1], X[3][2], whole3)
    restrict_planes(3, X[4][0], whole4[1], 1, YPAD, 1, YPAD, whole4[3])
    relax(4, X[4][0], X[4][1], whole4)
    collect(4, whole4)
    correct(3, c4u, c4g, 1, YPAD)
    relax(3, X[3][2], X[3][3], whole3)
    pad3 = HALOS[2] // 2 + 1
    collect(3, whole3, offset=pad3 - 1)
    n0, n1 = owned(3)
    margin = YPAD // 2
    for y in range(gy_n):

        @pl.when(iy == y)
        def _():
            for j in range(HALOS[2] + 2 * n0):
                for src, dst in ((c3u, cwu), (c3g, cwg)):
                    dst[j, :, pl.ds(margin, n1 + 4 * margin), :] = src[
                        bx * n0 + j, :, pl.ds(y * n1, n1 + 4 * margin), :
                    ]

    for level in (2, 1, 0):
        if level == 2:
            correct(2, cwu, cwg, 1, YPAD)
        else:
            x0 = HALOS[level + 1] - HALOS[level] // 2
            correct(level, UP[level + 1], GP[level + 1], x0, YPAD // 2)
        where = region(level, 3)
        relax(level, X[level][2], X[level][3], where)
        if level:
            collect(level, where)

    def send_out(ref, p, c):
        for other in range(1, gz_n):
            there = lax.rem(iz + other, gz_n)
            block = ref.at[there, pl.ds(iz * nx + p, c)]
            copy(block, block, o_send, o_recv, (ix, iy, there)).start()

    quarter = nx // 4
    own0 = [(HALOS[0] + p, quarter, YPAD, ny) for p in range(0, nx, quarter)]
    for where in own0:
        p = where[0] - HALOS[0]
        collect(0, where, place=iz * nx + p)
        send_out(sol_ref, p, quarter)
    for where in own0:
        p = where[0] - HALOS[0]
        relax(0, X[0][3], res_ref, where, place=iz * nx + p)
        send_out(res_ref, p, quarter)
    for drain in drains:
        drain()
    for sem in (o_send, o_recv):
        take_rows(sem, (gz_n - 1) * 2 * nx * ny)


def zero_rows(ref, i, at, value):
    ref[i, :, pl.ds(at, YPAD), :] = value
    return 0


def store_kernel(pieces, sol_v, res_v, sol_hbm, res_hbm, sem):
    iz = lax.axis_index("gz")
    span = sol_hbm.shape[0] // pieces
    moves = []
    for which, (src, dst) in enumerate(((sol_v, sol_hbm), (res_v, res_hbm))):
        for i in range(pieces):
            at = pl.ds(i * span, span)
            moves.append(
                pltpu.make_async_copy(src.at[iz, at], dst.at[at], sem.at[which, i])
            )
    for move in moves:
        move.start()
    for move in moves:
        move.wait()


def fits(mesh, shape, inverse_shape):
    gx_n, gy_n, gz_n = (mesh.shape[a] for a in ("gx", "gy", "gz"))
    nx, ny = shape[0] // (gx_n * gz_n), shape[1] // gy_n
    return (
        inverse_shape[0] == LEVELS == 5
        and SWEEPS == 2
        and inverse_shape[2] == 128
        and nx % 8 == 0
        and ny % 32 == 0
        and (shape[1] >> 4) % 8 == 0
        and gz_n <= 2
    )


def fused_body(mesh, right_side, z_faces, xy_coupling, block_inverse):
    gx_n, gy_n, gz_n = (mesh.shape[a] for a in ("gx", "gy", "gz"))
    levels, _, depth = block_inverse.shape
    nx, ny = right_side.shape[0] // gz_n, right_side.shape[1]
    windows = []
    for level in range(levels):
        if level < DEEPEST:
            size = ((nx >> level) + 2 * HALOS[level], (ny >> level) + SPARE)
        else:
            size = (
                ((nx * gx_n * gz_n) >> level) + 2,
                ((ny * gy_n) >> level) + 2 * YPAD,
            )
        windows.append((size[0], gz_n, size[1], depth))
    vmem = lambda shape: pltpu.VMEM(shape, jnp.float32)
    full3, full4 = windows[3], windows[4]
    pad3 = HALOS[2] // 2 + 1
    c4 = full4
    c3 = (full3[0] - 2 + 2 * pad3,) + full3[1:]
    cw = (windows[2][0] // 2 + 2, gz_n, (ny >> 3) + 28, depth)
    most = gz_n * (nx + 2 * HALOS[0] + 8) * (ny + 2 * YPAD)
    bx_n = gx_n * gz_n
    dma = pltpu.SemaphoreType.DMA
    own = lambda k: (nx >> k, gz_n, ny >> k, depth)
    scratch = (
        [
            pltpu.VMEM((levels, gz_n * depth, gz_n * depth), jnp.bfloat16),
            vmem((levels, gz_n, depth, depth)),
            vmem((gz_n, 1, depth)),
            vmem((bx_n, gy_n) + own(3)),
            vmem(right_side.shape),
            pltpu.SMEM((levels,), jnp.float32),
        ]
        + [vmem(w) for w in windows[: DEEPEST + 1] for _ in range(4)]
        + [vmem(full4)] * 2
        + [vmem(w) for w in windows[: DEEPEST + 1]] * 2
        + [vmem(windows[1])] * 2
        + [vmem(windows[2])] * 2
        + [vmem(c3), vmem(c3), vmem(c4), vmem(c4), vmem(cw), vmem(cw)]
        + [vmem(own(3)), vmem((most, depth))]
        + [dma((6,))]
        + [dma((gz_n, 3))] * 2
        + [dma((DEEPEST,))] * 2
        + [dma((gy_n,)), dma((5,))]
    )
    in_vmem = pl.BlockSpec(memory_space=pltpu.VMEM)
    in_hbm = pl.BlockSpec(memory_space=pltpu.HBM)
    staged = (gz_n,) + right_side.shape
    hold = lambda x: pltpu.with_memory_space_constraint(x, pltpu.HBM)
    halves = pl.pallas_call(
        functools.partial(cycle_kernel, (gx_n, gy_n, gz_n, nx, ny, depth, levels)),
        out_shape=[pltpu.VMEM(staged, jnp.float32)] * 2,
        in_specs=[
            in_hbm,
            in_hbm,
            in_hbm,
            in_hbm,
        ],
        out_specs=[in_vmem, in_vmem],
        scratch_shapes=scratch,
        compiler_params=pltpu.CompilerParams(
            collective_id=0, has_side_effects=True, vmem_limit_bytes=48 * 1024 * 1024
        ),
    )(hold(right_side), hold(z_faces.reshape(1, -1)), hold(xy_coupling), hold(block_inverse))
    pieces = 4
    return tuple(
        pl.pallas_call(
            functools.partial(store_kernel, pieces),
            out_shape=[jax.ShapeDtypeStruct(right_side.shape, jnp.float32)] * 2,
            in_specs=[in_vmem, in_vmem],
            out_specs=[in_hbm, in_hbm],
            scratch_shapes=[dma((2, pieces))],
        )(*[pltpu.with_memory_space_constraint(x, pltpu.VMEM) for x in halves])
    )


def solution(mesh):
    def call(right_side, z_faces, xy_coupling, block_inverse):
        local = body
        if fits(mesh, right_side.shape, block_inverse.shape):
            local = functools.partial(fused_body, mesh)
        return jax.shard_map(
            local,
            mesh=mesh,
            in_specs=(P("gx", "gy", "gz"), P("gz"), P(), P(None, "gz", None)),
            out_specs=(P("gx", "gy", "gz"), P("gx", "gy", "gz")),
            check_vma=False,
        )(right_side, z_faces, xy_coupling, block_inverse)

    return call
```

```python
import functools

import jax
import jax.numpy as jnp
from jax import lax
from jax.experimental import pallas as pl
from jax.experimental.pallas import tpu as pltpu
from jax.sharding import PartitionSpec as P

LEVELS = 5
SWEEPS = 2


damping = 0.8
highest = lax.Precision.HIGHEST


def extended(cells, sides, width):
    for axis, dim in sides:
        count = lax.axis_size(axis)
        ends = count - 1
        head = lax.slice_in_dim(cells, 0, width, axis=dim)
        tail = lax.slice_in_dim(cells, cells.shape[dim] - width, cells.shape[dim], axis=dim)
        cells = jnp.concatenate(
            [
                lax.ppermute(tail, axis, [(i, (i + 1) % count) for i in range(ends)]),
                cells,
                lax.ppermute(head, axis, [((i + 1) % count, i) for i in range(ends)]),
            ],
            axis=dim,
        )
    return cells


def interface_setup(corner_aa, corner_ab, corner_ba, corner_bb, couplings):
    determinant = corner_aa * corner_bb - corner_ab * corner_ba
    corner_inverse = (
        jnp.stack(
            [jnp.stack([corner_bb, -corner_ab], -1), jnp.stack([-corner_ba, corner_aa], -1)], -2
        )
        / determinant[:, None, None]
    )
    blocks_count = corner_aa.shape[0]
    identity = jnp.eye(blocks_count, dtype=corner_inverse.dtype)
    diagonal_part = jnp.einsum("kab,kl->kalb", corner_inverse, identity, precision=highest).reshape(
        2 * blocks_count, 2 * blocks_count
    )
    link_values = jnp.zeros((2 * blocks_count - 1,), corner_inverse.dtype).at[1::2].set(-couplings)
    schur_matrix = diagonal_part + jnp.diag(link_values, 1) + jnp.diag(link_values, -1)
    return (corner_inverse, diagonal_part, jnp.linalg.cholesky(schur_matrix))


def make_solver(inverse_block, corner_rows, couplings, device_index, down_coupling, up_coupling):
    corner_inverse, diagonal_part, factor = interface_setup(
        corner_rows[:, 0], corner_rows[:, 1], corner_rows[:, 2], corner_rows[:, 3], couplings
    )
    block_len = inverse_block.shape[0]
    forward = lax.linalg.triangular_solve(factor, diagonal_part, left_side=True, lower=True)
    reach = lax.linalg.triangular_solve(
        factor, forward, left_side=True, lower=True, transpose_a=True
    )
    padded_reach = jnp.pad(reach, ((1, 1), (0, 0)))
    slice_rows = lax.dynamic_slice_in_dim(padded_reach, 2 * device_index, 4, 0)
    needed = jnp.stack([slice_rows[0], slice_rows[3]])

    def neighbours(end_values):
        zero_carry = jnp.zeros(end_values.shape, jnp.float32)
        nearby = zero_carry + jnp.dot(
            needed, lax.all_gather(end_values, "gz", axis=0, tiled=True), precision=highest
        )
        return (nearby[0], nearby[1])

    def solve(source):
        first_extent, second_extent, depth = source.shape
        line_count = first_extent * second_extent
        local_part = jnp.einsum("xyj,ij->xyi", source, inverse_block, precision=highest)
        end_values = jnp.stack(
            [
                local_part[:, :, 0].reshape(line_count),
                local_part[:, :, block_len - 1].reshape(line_count),
            ]
        )
        below_last, above_first = neighbours(end_values)
        return (
            local_part
            + (down_coupling * below_last).reshape(first_extent, second_extent, 1)
            * inverse_block[:, 0]
            + (up_coupling * above_first).reshape(first_extent, second_extent, 1)
            * inverse_block[:, block_len - 1]
        )

    return solve


def apply_operator(iterate, lateral_weight, down_faces, up_faces):
    padded = extended(iterate, (("gx", 0), ("gy", 1), ("gz", 2)), 1)
    lateral = (
        padded[:-2, 1:-1, 1:-1]
        + padded[2:, 1:-1, 1:-1]
        + padded[1:-1, :-2, 1:-1]
        + padded[1:-1, 2:, 1:-1]
    )
    return (
        lateral_weight * (4.0 * iterate - lateral)
        + down_faces * (iterate - padded[1:-1, 1:-1, :-2])
        + up_faces * (iterate - padded[1:-1, 1:-1, 2:])
    )


def restrict(field):
    first_extent, second_extent, depth = field.shape
    return field.reshape(first_extent // 2, 2, second_extent // 2, 2, depth).sum(axis=(1, 3)) * 0.25


def prolong(padded):
    first_extent = padded.shape[0] - 2
    second_extent = padded.shape[1] - 2
    depth = padded.shape[2]
    even_rows = 0.75 * padded[1:-1] + 0.25 * padded[:-2]
    odd_rows = 0.75 * padded[1:-1] + 0.25 * padded[2:]
    widened = jnp.stack([even_rows, odd_rows], 1).reshape(
        2 * first_extent, second_extent + 2, depth
    )
    even_rows = 0.75 * widened[:, 1:-1] + 0.25 * widened[:, :-2]
    odd_rows = 0.75 * widened[:, 1:-1] + 0.25 * widened[:, 2:]
    return jnp.stack([even_rows, odd_rows], 2).reshape(2 * first_extent, 2 * second_extent, depth)


def body(right_side, z_faces, xy_coupling, block_inverse):
    device_index = lax.axis_index("gz")
    levels_count = block_inverse.shape[0]
    last_cell = block_inverse.shape[1] - 1
    corner = jnp.stack(
        [
            block_inverse[:, 0, 0],
            block_inverse[:, 0, last_cell],
            block_inverse[:, last_cell, 0],
            block_inverse[:, last_cell, last_cell],
        ],
        -1,
    )[None]
    corners, firsts = (
        lax.all_gather(corner, "gz", axis=0, tiled=True),
        lax.all_gather(z_faces[:1], "gz", axis=0, tiled=True),
    )
    couplings = firsts[1:]
    edge_faces = jnp.concatenate([firsts, jnp.ones((1,), jnp.float32)])
    top_face = lax.dynamic_slice_in_dim(edge_faces, device_index + 1, 1, 0)
    up_faces = jnp.concatenate([z_faces[1:], top_face])
    solvers = [
        make_solver(
            block_inverse[level],
            corners[:, level],
            couplings,
            device_index,
            z_faces[0],
            top_face[0],
        )
        for level in range(levels_count)
    ]

    def operator(iterate, level):
        return apply_operator(iterate, xy_coupling[level], z_faces, up_faces)

    def multigrid_cycle(source, level):
        iterate = damping * solvers[level](source)
        iterate = iterate + damping * solvers[level](source - operator(iterate, level))
        if level == LEVELS - 1:
            return iterate
        coarse = multigrid_cycle(restrict(source - operator(iterate, level)), level + 1)
        widened = extended(coarse, (("gx", 0), ("gy", 1)), 1)
        iterate = iterate + prolong(widened)
        for sweep in range(SWEEPS):
            iterate = iterate + damping * solvers[level](source - operator(iterate, level))
        return iterate

    solution = multigrid_cycle(right_side, 0)
    return (solution, right_side - operator(solution, 0))


MESH = pl.DeviceIdType.MESH
HALOS = (4, 6, 6)
ROWS = (4, 5, 6)
YPAD = 8
SPARE = 32
DEEPEST = 3
NEAR = 2


def block_range(offset, own, halo, extent):
    start = offset * own - halo
    low = max(0, start)
    high = min(extent, (offset + 1) * own + halo)
    return low, high - low, low - start


def round_up(value, unit):
    return -(-value // unit) * unit


def difference(outer, inner):
    (a, b), (c, d) = outer
    (e, f), (g, h) = inner
    if e >= f or g >= h:
        return [outer]
    parts = [((a, e), (c, d)), ((f, b), (c, d)), ((e, f), (c, g)), ((e, f), (h, d))]
    return [(x, y) for x, y in parts if x[0] < x[1] and y[0] < y[1]]


def needed(t, dy, own, size, halo):
    (n0, n1), (s0, s1) = own, size
    x = max(0, t * n0 - halo), min(s0, (t + 1) * n0 + halo)
    y = max(0, dy * n1 - halo), min(s1, (dy + 1) * n1 + halo)
    return x, y


def both_parts(t, dy, own, size, halo):
    near = needed(t, dy, own, size, NEAR)
    inner = [near] if near[0][0] < near[0][1] and near[1][0] < near[1][1] else []
    outer = difference(needed(t, dy, own, size, halo), near)
    return inner, outer


def area(parts):
    return sum((x[1] - x[0]) * (y[1] - y[0]) for x, y in parts)


def split_planes(count, rows):
    return max(c for c in range(1, count + 1) if count % c == 0 and c * rows <= 448)


def cycle_kernel(geometry, f_hbm, z_hbm, e_hbm, g_hbm, sol_ref, res_ref, *scratch):
    gx_n, gy_n, gz_n, nx, ny, depth, levels = geometry
    refs = iter(scratch)
    take = lambda count: [next(refs) for _ in range(count)]
    sinv, g_all, z_all, gather, f_v, e_ref = take(6)
    X = [take(4) for _ in range(DEEPEST + 1)]
    X.append(take(2))
    C = take(DEEPEST + 1)
    E = take(DEEPEST + 1)
    (U1, G1, U2, G2, c3u, c3g, c4u, c4g, cwu, cwg) = take(10)
    UP, GP = [None, U1, U2, c3u, c4u], [None, G1, G2, c3g, c4g]
    own3, pool = take(2)
    N = take(DEEPEST)
    (in_sem, g_send, g_recv, h_send, h_recv, y_recv, p_sem) = take(7)
    y_send, x_send, x_recv, o_send, o_recv = [p_sem.at[i] for i in range(5)]

    ix, iy, iz = lax.axis_index("gx"), lax.axis_index("gy"), lax.axis_index("gz")
    bx = ix * gz_n + iz
    bx_n = gx_n * gz_n
    f32 = jnp.float32

    def owned(level):
        return nx >> level, ny >> level

    def copy(src, dst, send, recv, device):
        return pltpu.make_async_remote_copy(
            src_ref=src,
            dst_ref=dst,
            send_sem=send,
            recv_sem=recv,
            device_id=device,
            device_id_type=MESH,
        )

    def inside(x, y):
        return (x >= 0) & (x < gx_n) & (y >= 0) & (y < gy_n)

    parts = 4
    span = f_v.shape[0] // parts
    for i in range(parts):
        at = pl.ds(i * span, span)
        pltpu.make_async_copy(f_hbm.at[at], f_v.at[at], in_sem.at[0]).start()
    f_load = pltpu.make_async_copy(f_hbm, f_v, in_sem.at[0])
    rest = pl.ds(1, levels - 1)
    loads = [
        pltpu.make_async_copy(z_hbm, z_all.at[iz], in_sem.at[1]),
        pltpu.make_async_copy(g_hbm.at[0], g_all.at[0, iz], in_sem.at[2]),
        pltpu.make_async_copy(g_hbm.at[rest], g_all.at[rest, iz], in_sem.at[3]),
        pltpu.make_async_copy(e_hbm, e_ref, in_sem.at[4]),
    ]
    for c in loads:
        c.start()

    reach_all = max(
        gz_n - 1 - (-HALOS[0] // nx), *[-(-HALOS[k] // owned(k)[0]) for k in (1, 2)]
    )
    barrier = pltpu.get_barrier_semaphore()
    partners = jnp.int32(0)
    for dx in range(1 - bx_n, bx_n):
        for dy in range(1 - gy_n, gy_n):
            close = abs(dx) <= reach_all and abs(dy) <= 1
            if (dx == 0 and dy == 0) or not (close or dx == 0 or dy == 0):
                continue
            x, y = bx + dx, iy + dy
            ok = (x >= 0) & (x < bx_n) & (y >= 0) & (y < gy_n)

            @pl.when(ok)
            def _():
                pl.semaphore_signal(
                    barrier,
                    inc=1,
                    device_id=(x // gz_n, y, lax.rem(x, gz_n)),
                    device_id_type=MESH,
                )

            partners = partners + jnp.where(ok, 1, 0).astype(jnp.int32)

    def setup_copies(other):
        here = (ix, iy, lax.rem(iz + other, gz_n))
        out = []
        for i, block in enumerate((z_all.at[iz], g_all.at[0, iz], g_all.at[rest, iz])):
            out.append(copy(block, block, g_send.at[other, i], g_recv.at[other, i], here))
        return out

    def runs(count, key):
        out = []
        for i in range(count):
            if out and key(i) == out[-1][2]:
                out[-1][1] = i
            else:
                out.append([i, i, key(i)])
        return [(low, high) for low, high, _ in out]

    def take_rows(sem, rows):
        block = pool.at[pl.ds(0, rows)]
        pltpu.make_async_copy(block, block, sem).wait()

    def settle(sem, total):
        table = [[total(b, y) for y in range(gy_n)] for b in range(bx_n)]
        for low, high in runs(bx_n, lambda b: table[b]):
            for first, last in runs(gy_n, lambda y: [row[y] for row in table]):

                @pl.when((bx >= low) & (bx <= high) & (iy >= first) & (iy <= last))
                def _():
                    take_rows(sem, table[low][first])

    near0, far0 = N[0], X[0][0]
    plan0 = []
    reach = -(-ROWS[0] // nx)
    for t in range(-reach, gz_n + reach):
        for dy in (-1, 0, 1):
            parts0 = both_parts(t, dy, (nx, ny), (nx * gz_n, ny), ROWS[0])
            plan0.append((t, t // gz_n, t % gz_n, dy, parts0))

    def target0(window, part, t, dy, source_z):
        (x0, x1), (y0, y1) = part
        p, r = x0 - t * nx + HALOS[0], y0 - dy * ny + YPAD
        return window.at[pl.ds(p, x1 - x0), source_z, pl.ds(r, y1 - y0), :]

    local0 = []
    for t, dgx, target, dy, parts0 in plan0:
        if dgx == 0 and dy == 0:
            for which, window in enumerate((near0, far0)):
                for part in parts0[which]:
                    (x0, x1), (y0, y1) = part
                    move = pltpu.make_async_copy(
                        f_hbm.at[pl.ds(x0, x1 - x0), pl.ds(y0, y1 - y0), :],
                        target0(window, part, t, dy, target),
                        in_sem.at[5 + which],
                    )
                    local0.append((target, which, move))

    for target, _, move in local0:

        @pl.when(iz == target)
        def _():
            move.start()

    def local_done(which):
        for target, other, move in local0:
            if other == which:

                @pl.when(iz == target)
                def _():
                    move.wait()

    def send0(which):
        for t, dgx, target, dy, parts0 in plan0:
            ok = inside(ix + dgx, iy + dy)
            if dgx == 0 and dy == 0:
                ok = ok & (iz != target)

            @pl.when(ok)
            def _():
                for part in parts0[which]:
                    (x0, x1), (y0, y1) = part
                    copy(
                        f_v.at[pl.ds(x0, x1 - x0), pl.ds(y0, y1 - y0), :],
                        target0((near0, far0)[which], part, t, dy, iz),
                        h_send.at[0],
                        h_recv.at[0, which],
                        (ix + dgx, iy + dy, target),
                    ).start()

    def in_grid(b, y):
        return 0 <= b < bx_n and 0 <= y < gy_n

    def sent0(b, y):
        total = 0
        for t, dgx, target, dy, parts0 in plan0:
            there = (b // gz_n + dgx) * gz_n + target
            if in_grid(there, y + dy) and (there, dy) != (b, 0):
                total += area(parts0[0]) + area(parts0[1])
        return total

    def received0(which):
        def count(b, y):
            total = 0
            for t, dgx, target, dy, parts0 in plan0:
                for source_z in range(gz_n):
                    there = (b // gz_n - dgx) * gz_n + source_z
                    ok = target == b % gz_n and in_grid(there, y - dy)
                    if ok and (there, dy) != (b, 0):
                        total += area(parts0[which])
            return total

        return count

    def clear_edges():
        for level, window in [(k, w) for k in range(DEEPEST) for w in (N[k], X[k][0])]:
            planes, zb, rows, lanes = window.shape
            halo = HALOS[level]
            n0, n1 = owned(level)
            reach = -(-halo // n0)
            for t in range(1, reach + 1):
                low = max(0, halo - t * n0)
                high = halo - (t - 1) * n0
                plane = jnp.zeros((high - low, zb, n1 + 2 * YPAD, lanes), f32)

                @pl.when(bx - t < 0)
                def _():
                    window[low:high, :, pl.ds(0, n1 + 2 * YPAD)] = plane

                low2, high2 = planes - high, planes - low

                @pl.when(bx + t >= bx_n)
                def _():
                    window[low2:high2, :, pl.ds(0, n1 + 2 * YPAD)] = plane

            edge = jnp.zeros((zb, YPAD, lanes), f32)

            @pl.when(iy == 0)
            def _():
                lax.fori_loop(0, planes, lambda i, c: zero_rows(window, i, 0, edge), 0)

            @pl.when(iy == gy_n - 1)
            def _():
                lax.fori_loop(
                    0, planes, lambda i, c: zero_rows(window, i, YPAD + n1, edge), 0
                )

    def fill(ref):
        zero = jnp.zeros(ref.shape[1:], f32)

        def step(i, _):
            ref[i] = zero
            return 0

        lax.fori_loop(0, ref.shape[0], step, 0)

    def clear_coarse():
        for ref in (*X[3][:3], C[3], X[4][0], c3u, c3g, c4u, c4g):
            fill(ref)

    def assemble(level, _):
        merged = g_all[level, 0]
        for k in range(1, gz_n):
            block = g_all[level, k]
            size, cz = merged.shape[0], block.shape[0]
            face = z_all[k][:, 0:1]
            a, d = block[0:1, 0:1], merged[size - 1 : size, size - 1 : size]
            last, first = merged[size - 1 : size], block[0:1]
            scale = face / (1.0 - face * face * a * d)
            p_row = jnp.concatenate([face * a * last, first], 1) * scale
            q_row = jnp.concatenate([last, face * d * first], 1) * scale
            top = jnp.concatenate([merged, jnp.zeros((size, cz), f32)], 1)
            low = jnp.concatenate([jnp.zeros((cz, size), f32), block], 1)
            top = top + merged[:, size - 1 : size] * p_row
            low = low + block[:, 0:1] * q_row
            merged = jnp.concatenate([top, low], 0)
        sinv[level] = (damping * merged).astype(jnp.bfloat16)
        return 0

    def plane_mask(level, i):
        n0 = owned(level)[0]
        x = bx * n0 - HALOS[level] + i
        return jnp.where((x >= 0) & (x < bx_n * n0), 1.0, 0.0).astype(f32)

    def row_mask(level, first, rows, stride):
        n1 = owned(level)[1]
        y = lax.broadcasted_iota(jnp.int32, (rows, depth), 0) * stride + first
        y = y + iy * n1 - YPAD
        return jnp.where((y >= 0) & (y < gy_n * n1), 1.0, 0.0).astype(f32)

    def region(level, shrink=0):
        if level < DEEPEST:
            return nearby(level, ROWS[level] - shrink)
        window = X[level][0].shape
        return 1, window[0] - 2, YPAD, window[2] - 2 * YPAD

    def nearby(level, h):
        n0, n1 = owned(level)
        return HALOS[level] - h, n0 + 2 * h, YPAD - h, round_up(n1 + 2 * h, 8)

    def weights(level, p, c, r0, rows):
        e = e_ref[level]
        if level >= DEEPEST:
            return e
        mask = row_mask(level, r0, rows, 1)
        return jnp.stack([mask * (e * plane_mask(level, p + i)) for i in range(c)])

    def chunks(where):
        p0, planes, r0, rows = where
        c = split_planes(planes, rows)
        return [(p0 + s * c, c, r0, rows) for s in range(planes // c)]

    def around(src, k, p, c, r0, rows):
        at = lambda dp, dr: src[pl.ds(p + dp, c), k, pl.ds(r0 + dr, rows)]
        return (at(-1, 0) + at(1, 0)) + (at(0, -1) + at(0, 1))

    def line_solve(level, fields):
        flat = [v.reshape(-1, depth) for v in fields]
        lhs = jnp.concatenate(flat, 1).astype(jnp.bfloat16)
        out = jnp.dot(lhs, sinv[level], preferred_element_type=f32)
        shape = fields[0].shape
        return [out[:, k * depth : (k + 1) * depth].reshape(shape) for k in range(len(flat))]

    def relax(level, src, dst, where, place=None):
        for p, c, r0, rows in chunks(where):
            w = weights(level, p, c, r0, rows)
            total = [around(src, k, p, c, r0, rows) * w for k in range(gz_n)]
            out = line_solve(level, total)
            for k in range(gz_n):
                value = (1.0 - damping) * src[pl.ds(p, c), k, pl.ds(r0, rows)] + out[k]
                if place is None:
                    dst[pl.ds(p, c), k, pl.ds(r0, rows)] = value
                else:
                    dst[k, pl.ds(place + p - where[0], c)] = value

    def collect(level, where, place=None, offset=0):
        for p, c, r0, rows in chunks(where):
            at = lambda ref, k: ref[pl.ds(p, c), k, pl.ds(r0, rows)]
            total = []
            for k in range(gz_n):
                part = [at(ref, k) for ref in X[level]]
                while len(part) > 1:
                    part = [part[i] + part[i + 1] for i in range(0, len(part), 2)]
                total.append(part[0])
            out = line_solve(level, total)
            for k in range(gz_n):
                u = out[k] if level > DEEPEST else out[k] + at(C[level], k)
                if level == 0:
                    sol_ref[k, pl.ds(place + p - where[0], c)] = u
                    continue
                g = damping * total[k] + (4.0 * (e_ref[level - 1] - e_ref[level])) * u
                if level <= DEEPEST:
                    g = g + at(E[level], k)
                UP[level][pl.ds(p + offset, c), k, pl.ds(r0, rows)] = u
                GP[level][pl.ds(p + offset, c), k, pl.ds(r0, rows)] = g

    def restrict_planes(level, dst, planes, x0, y0, to_plane, to_row, rows):
        src = X[level][2]
        for j in range(planes):
            for k in range(gz_n):
                total = None
                for a in (0, 1):
                    for b in (0, 1):
                        part = src[x0 + 2 * j + a, k, pl.ds(y0 + b, rows, 2), :]
                        total = part if total is None else total + part
                dst[to_plane + j, k, pl.ds(to_row, rows), :] = total * 0.25

    def prolong(level, x0, y0, coarse):
        shift = 1 if level >= DEEPEST else 0
        p0, planes, r0, rows = region(level, 1)
        low, high = p0 - shift, p0 - shift + planes
        first = r0 // 2 * 2
        half = round_up((r0 + rows - first + 1) // 2, 8) if level < DEEPEST else rows // 2
        start = y0 + (first // 2 if level < DEEPEST else 0)
        masks = [
            row_mask(level, first + b, half, 2) if level < DEEPEST else None for b in (0, 1)
        ]
        mixes = {}

        def mixed(src, index, j, k):
            key = (index, j, k)
            if key not in mixes:
                load = lambda dy: src[x0 + j, k, pl.ds(start + dy, half), :]
                quarter = 0.25 * load(0)
                near = load(0) - quarter
                out = []
                for dy in (-1, 1):
                    value = near + 0.25 * load(dy)
                    far = 0.25 * value
                    out.append((value - far, far))
                mixes[key] = out
            return mixes[key]

        for j in range(low // 2, (high - 1) // 2 + 1):
            for a in (0, 1):
                p = 2 * j + a
                if not low <= p < high:
                    continue
                for b in (0, 1):
                    if level < DEEPEST:
                        mask = masks[b] * plane_mask(level, p)
                    for index, (src, dst) in enumerate(coarse):
                        for k in range(gz_n):
                            near = mixed(src, index, j, k)[b][0]
                            value = near + mixed(src, index, j + 2 * a - 1, k)[b][1]
                            if level < DEEPEST:
                                value = value * mask
                            dst[p + shift, k, pl.ds(first + b, half, 2), :] = value

    def correct(level, coarse_u, coarse_g, x0, y0):
        prolong(level, x0, y0, [(coarse_u, C[level]), (coarse_g, E[level])])
        where = region(level, 2)
        target = X[level][2]
        for p, c, r0, rows in chunks(where):
            w = weights(level, p, c, r0, rows)
            for k in range(gz_n):
                at = lambda ref: ref[pl.ds(p, c), k, pl.ds(r0, rows)]
                total = around(C[level], k, p, c, r0, rows) * w
                target[pl.ds(p, c), k, pl.ds(r0, rows)] = at(target) + (total - at(E[level]))

    def exchange(level):
        n0, n1 = owned(level)
        width = ROWS[level]
        halo = HALOS[level]
        reach = -(-width // n0)
        pieces = [
            (t, dy, both_parts(t, dy, (n0, n1), (n0, n1), width))
            for t in range(-reach, reach + 1)
            for dy in (-1, 0, 1)
            if t or dy
        ]

        for which, window in enumerate((N[level], X[level][0])):
            for t, dy, parts in pieces:
                there = bx + t + bx_n
                x, y = bx + t, iy + dy

                @pl.when((x >= 0) & (x < bx_n) & (y >= 0) & (y < gy_n))
                def _():
                    for (x0, x1), (y0, y1) in parts[which]:
                        p, r = x0 - t * n0 + halo, y0 - dy * n1 + YPAD
                        copy(
                            N[level].at[
                                pl.ds(halo + x0, x1 - x0), :, pl.ds(YPAD + y0, y1 - y0), :
                            ],
                            window.at[pl.ds(p, x1 - x0), :, pl.ds(r, y1 - y0), :],
                            h_send.at[level],
                            h_recv.at[level, which],
                            (there // gz_n - gx_n, y, lax.rem(there, gz_n)),
                        ).start()

        def total(sign, wanted):
            def count(b, y):
                return sum(
                    gz_n * area(parts[which])
                    for t, dy, parts in pieces
                    for which in wanted
                    if in_grid(b + sign * t, y + sign * dy)
                )

            return count

        arrive = lambda which: settle(h_recv.at[level, which], total(-1, (which,)))
        return arrive, lambda: settle(h_send.at[level], total(1, (0, 1)))

    def widen(level, arrive):
        n0, n1 = owned(level)
        rows = pl.ds(YPAD - NEAR, n1 + 2 * NEAR)
        for p in range(HALOS[level] - NEAR, HALOS[level] + n0 + NEAR):
            X[level][0][p, :, rows] = N[level][p, :, rows]
        arrive(1)
        relax(level, X[level][0], X[level][1], region(level, 1))
        relax(level, X[level][1], X[level][2], region(level, 2))

    def gather_all(meanwhile):
        def line_y(other, slot):
            return copy(own3, gather.at[bx, slot], y_send, y_recv.at[slot], (ix, other, iz))

        def line_x(src, other, slot_x, slot_y):
            return copy(
                src,
                gather.at[slot_x, slot_y],
                x_send,
                x_recv,
                (other // gz_n, iy, lax.rem(other, gz_n)),
            )

        def others(me, count, act):
            for s in range(1, count):
                act(lax.rem(me + s, count))

        others(iy, gy_n, lambda y: line_y(y, iy).start())
        others(bx, bx_n, lambda x: line_x(own3, x, bx, iy).start())
        gather[bx, iy] = own3[...]
        meanwhile()
        for distance in range(1, gy_n):
            for y in (iy + distance, iy - distance):

                @pl.when((y >= 0) & (y < gy_n))
                def _():
                    line_y(y, y).wait_recv()
                    block = gather.at[bx, y]
                    others(bx, bx_n, lambda x: line_x(block, x, bx, y).start())

        size = own3.shape[0] * own3.shape[1] * own3.shape[2]
        take_rows(x_recv, (bx_n - 1) * gy_n * size)
        n0, n1 = owned(3)
        window = X[3][0]

        def place(b, _):
            for i in range(n0):
                for y in range(gy_n):
                    window[1 + b * n0 + i, :, pl.ds(YPAD + y * n1, n1), :] = gather[b, y, i]
            return 0

        lax.fori_loop(0, bx_n, place, 0)

        def drains():
            take_rows(y_send, (gy_n - 1) * size)
            take_rows(x_send, (bx_n - 1) * gy_n * size)

        return drains

    f_load.wait()
    pl.semaphore_wait(barrier, partners)
    send0(0)
    for c in loads:
        c.wait()
    setups = [setup_copies(other) for other in range(1, gz_n)]
    for group in setups:
        for c in group[:2]:
            c.start()
    send0(1)
    for group in setups:
        group[2].start()
    clear_edges()
    for group in setups:
        for c in group[:2]:
            c.wait()
    assemble(0, 0)
    local_done(0)

    def arrive0(which):
        if which:
            local_done(1)
        settle(h_recv.at[0, which], received0(which))

    def later():
        for group in setups:
            group[2].wait()
        lax.fori_loop(1, levels, assemble, 0)

    arrive = arrive0
    drains = [lambda: settle(h_send.at[0], sent0)]
    for level in range(DEEPEST):
        arrive(0)
        one, two = X[level][1], X[level][2]
        relax(level, N[level], one, nearby(level, 1))
        relax(level, one, two, nearby(level, 0))
        n0, n1 = owned(level + 1)
        p, r = HALOS[level], YPAD
        if level < DEEPEST - 1:
            restrict_planes(level, N[level + 1], n0, p, r, HALOS[level + 1], YPAD, n1)
            following, drain = exchange(level + 1)
            drains.append(drain)
            (later, clear_coarse)[level]()
            widen(level, arrive)
            arrive = following
        else:
            restrict_planes(level, own3, n0, p, r, 0, 0, n1)
            drains.append(gather_all(lambda: widen(level, arrive)))

    whole3, whole4 = region(3, 0), region(4, 0)
    relax(3, X[3][0], X[3][1], whole3)
    relax(3, X[3][1], X[3][2], whole3)
    restrict_planes(3, X[4][0], whole4[1], 1, YPAD, 1, YPAD, whole4[3])
    relax(4, X[4][0], X[4][1], whole4)
    collect(4, whole4)
    correct(3, c4u, c4g, 1, YPAD)
    relax(3, X[3][2], X[3][3], whole3)
    pad3 = HALOS[2] // 2 + 1
    collect(3, whole3, offset=pad3 - 1)
    n0, n1 = owned(3)
    margin = YPAD // 2
    for y in range(gy_n):

        @pl.when(iy == y)
        def _():
            for j in range(HALOS[2] + 2 * n0):
                for src, dst in ((c3u, cwu), (c3g, cwg)):
                    dst[j, :, pl.ds(margin, n1 + 4 * margin), :] = src[
                        bx * n0 + j, :, pl.ds(y * n1, n1 + 4 * margin), :
                    ]

    for level in (2, 1, 0):
        if level == 2:
            correct(2, cwu, cwg, 1, YPAD)
        else:
            x0 = HALOS[level + 1] - HALOS[level] // 2
            correct(level, UP[level + 1], GP[level + 1], x0, YPAD // 2)
        where = region(level, 3)
        relax(level, X[level][2], X[level][3], where)
        if level:
            collect(level, where)

    def send_out(ref, p, c):
        for other in range(1, gz_n):
            there = lax.rem(iz + other, gz_n)
            block = ref.at[there, pl.ds(iz * nx + p, c)]
            copy(block, block, o_send, o_recv, (ix, iy, there)).start()

    own0 = nearby(0, 0)
    collect(0, own0, place=iz * nx)
    send_out(sol_ref, 0, nx)
    relax(0, X[0][3], res_ref, own0, place=iz * nx)
    send_out(res_ref, 0, nx)
    for drain in drains:
        drain()
    for sem in (o_send, o_recv):
        take_rows(sem, (gz_n - 1) * 2 * nx * ny)


def zero_rows(ref, i, at, value):
    ref[i, :, pl.ds(at, YPAD), :] = value
    return 0


def store_kernel(pieces, sol_v, res_v, sol_hbm, res_hbm, sem):
    iz = lax.axis_index("gz")
    span = sol_hbm.shape[0] // pieces
    moves = []
    for which, (src, dst) in enumerate(((sol_v, sol_hbm), (res_v, res_hbm))):
        for i in range(pieces):
            at = pl.ds(i * span, span)
            moves.append(
                pltpu.make_async_copy(src.at[iz, at], dst.at[at], sem.at[which, i])
            )
    for move in moves:
        move.start()
    for move in moves:
        move.wait()


def fits(mesh, shape, inverse_shape):
    gx_n, gy_n, gz_n = (mesh.shape[a] for a in ("gx", "gy", "gz"))
    nx, ny = shape[0] // (gx_n * gz_n), shape[1] // gy_n
    return (
        inverse_shape[0] == LEVELS == 5
        and SWEEPS == 2
        and inverse_shape[2] == 128
        and nx % 8 == 0
        and ny % 32 == 0
        and (shape[1] >> 4) % 8 == 0
        and gz_n <= 2
    )


def fused_body(mesh, right_side, z_faces, xy_coupling, block_inverse):
    gx_n, gy_n, gz_n = (mesh.shape[a] for a in ("gx", "gy", "gz"))
    levels, _, depth = block_inverse.shape
    nx, ny = right_side.shape[0] // gz_n, right_side.shape[1]
    windows = []
    for level in range(levels):
        if level < DEEPEST:
            size = ((nx >> level) + 2 * HALOS[level], (ny >> level) + SPARE)
        else:
            size = (
                ((nx * gx_n * gz_n) >> level) + 2,
                ((ny * gy_n) >> level) + 2 * YPAD,
            )
        windows.append((size[0], gz_n, size[1], depth))
    vmem = lambda shape: pltpu.VMEM(shape, jnp.float32)
    full3, full4 = windows[3], windows[4]
    pad3 = HALOS[2] // 2 + 1
    c4 = full4
    c3 = (full3[0] - 2 + 2 * pad3,) + full3[1:]
    cw = (windows[2][0] // 2 + 2, gz_n, (ny >> 3) + 28, depth)
    most = gz_n * (nx + 2 * HALOS[0] + 8) * (ny + 2 * YPAD)
    bx_n = gx_n * gz_n
    dma = pltpu.SemaphoreType.DMA
    own = lambda k: (nx >> k, gz_n, ny >> k, depth)
    scratch = (
        [
            pltpu.VMEM((levels, gz_n * depth, gz_n * depth), jnp.bfloat16),
            vmem((levels, gz_n, depth, depth)),
            vmem((gz_n, 1, depth)),
            vmem((bx_n, gy_n) + own(3)),
            vmem(right_side.shape),
            pltpu.SMEM((levels,), jnp.float32),
        ]
        + [vmem(w) for w in windows[: DEEPEST + 1] for _ in range(4)]
        + [vmem(full4)] * 2
        + [vmem(w) for w in windows[: DEEPEST + 1]] * 2
        + [vmem(windows[1])] * 2
        + [vmem(windows[2])] * 2
        + [vmem(c3), vmem(c3), vmem(c4), vmem(c4), vmem(cw), vmem(cw)]
        + [vmem(own(3)), vmem((most, depth))]
        + [vmem(w) for w in windows[:DEEPEST]]
        + [dma((7,))]
        + [dma((gz_n, 3))] * 2
        + [dma((DEEPEST,)), dma((DEEPEST, 2))]
        + [dma((gy_n,)), dma((5,))]
    )
    in_vmem = pl.BlockSpec(memory_space=pltpu.VMEM)
    in_hbm = pl.BlockSpec(memory_space=pltpu.HBM)
    staged = (gz_n,) + right_side.shape
    hold = lambda x: pltpu.with_memory_space_constraint(x, pltpu.HBM)
    halves = pl.pallas_call(
        functools.partial(cycle_kernel, (gx_n, gy_n, gz_n, nx, ny, depth, levels)),
        out_shape=[pltpu.VMEM(staged, jnp.float32)] * 2,
        in_specs=[
            in_hbm,
            in_hbm,
            in_hbm,
            in_hbm,
        ],
        out_specs=[in_vmem, in_vmem],
        scratch_shapes=scratch,
        compiler_params=pltpu.CompilerParams(
            collective_id=0, has_side_effects=True, vmem_limit_bytes=48 * 1024 * 1024
        ),
    )(hold(right_side), hold(z_faces.reshape(1, -1)), hold(xy_coupling), hold(block_inverse))
    pieces = 4
    return tuple(
        pl.pallas_call(
            functools.partial(store_kernel, pieces),
            out_shape=[jax.ShapeDtypeStruct(right_side.shape, jnp.float32)] * 2,
            in_specs=[in_vmem, in_vmem],
            out_specs=[in_hbm, in_hbm],
            scratch_shapes=[dma((2, pieces))],
        )(*[pltpu.with_memory_space_constraint(x, pltpu.VMEM) for x in halves])
    )


def solution(mesh):
    def call(right_side, z_faces, xy_coupling, block_inverse):
        local = body
        if fits(mesh, right_side.shape, block_inverse.shape):
            local = functools.partial(fused_body, mesh)
        return jax.shard_map(
            local,
            mesh=mesh,
            in_specs=(P("gx", "gy", "gz"), P("gz"), P(), P(None, "gz", None)),
            out_specs=(P("gx", "gy", "gz"), P("gx", "gy", "gz")),
            check_vma=False,
        )(right_side, z_faces, xy_coupling, block_inverse)

    return call
```

```python
import functools

import jax
import jax.numpy as jnp
from jax import lax
from jax.experimental import pallas as pl
from jax.experimental.pallas import tpu as pltpu
from jax.sharding import PartitionSpec as P

LEVELS = 5
SWEEPS = 2


damping = 0.8
highest = lax.Precision.HIGHEST


def extended(cells, sides, width):
    for axis, dim in sides:
        count = lax.axis_size(axis)
        ends = count - 1
        head = lax.slice_in_dim(cells, 0, width, axis=dim)
        tail = lax.slice_in_dim(cells, cells.shape[dim] - width, cells.shape[dim], axis=dim)
        cells = jnp.concatenate(
            [
                lax.ppermute(tail, axis, [(i, (i + 1) % count) for i in range(ends)]),
                cells,
                lax.ppermute(head, axis, [((i + 1) % count, i) for i in range(ends)]),
            ],
            axis=dim,
        )
    return cells


def interface_setup(corner_aa, corner_ab, corner_ba, corner_bb, couplings):
    determinant = corner_aa * corner_bb - corner_ab * corner_ba
    corner_inverse = (
        jnp.stack(
            [jnp.stack([corner_bb, -corner_ab], -1), jnp.stack([-corner_ba, corner_aa], -1)], -2
        )
        / determinant[:, None, None]
    )
    blocks_count = corner_aa.shape[0]
    identity = jnp.eye(blocks_count, dtype=corner_inverse.dtype)
    diagonal_part = jnp.einsum("kab,kl->kalb", corner_inverse, identity, precision=highest).reshape(
        2 * blocks_count, 2 * blocks_count
    )
    link_values = jnp.zeros((2 * blocks_count - 1,), corner_inverse.dtype).at[1::2].set(-couplings)
    schur_matrix = diagonal_part + jnp.diag(link_values, 1) + jnp.diag(link_values, -1)
    return (corner_inverse, diagonal_part, jnp.linalg.cholesky(schur_matrix))


def make_solver(inverse_block, corner_rows, couplings, device_index, down_coupling, up_coupling):
    corner_inverse, diagonal_part, factor = interface_setup(
        corner_rows[:, 0], corner_rows[:, 1], corner_rows[:, 2], corner_rows[:, 3], couplings
    )
    block_len = inverse_block.shape[0]
    forward = lax.linalg.triangular_solve(factor, diagonal_part, left_side=True, lower=True)
    reach = lax.linalg.triangular_solve(
        factor, forward, left_side=True, lower=True, transpose_a=True
    )
    padded_reach = jnp.pad(reach, ((1, 1), (0, 0)))
    slice_rows = lax.dynamic_slice_in_dim(padded_reach, 2 * device_index, 4, 0)
    needed = jnp.stack([slice_rows[0], slice_rows[3]])

    def neighbours(end_values):
        zero_carry = jnp.zeros(end_values.shape, jnp.float32)
        nearby = zero_carry + jnp.dot(
            needed, lax.all_gather(end_values, "gz", axis=0, tiled=True), precision=highest
        )
        return (nearby[0], nearby[1])

    def solve(source):
        first_extent, second_extent, depth = source.shape
        line_count = first_extent * second_extent
        local_part = jnp.einsum("xyj,ij->xyi", source, inverse_block, precision=highest)
        end_values = jnp.stack(
            [
                local_part[:, :, 0].reshape(line_count),
                local_part[:, :, block_len - 1].reshape(line_count),
            ]
        )
        below_last, above_first = neighbours(end_values)
        return (
            local_part
            + (down_coupling * below_last).reshape(first_extent, second_extent, 1)
            * inverse_block[:, 0]
            + (up_coupling * above_first).reshape(first_extent, second_extent, 1)
            * inverse_block[:, block_len - 1]
        )

    return solve


def apply_operator(iterate, lateral_weight, down_faces, up_faces):
    padded = extended(iterate, (("gx", 0), ("gy", 1), ("gz", 2)), 1)
    lateral = (
        padded[:-2, 1:-1, 1:-1]
        + padded[2:, 1:-1, 1:-1]
        + padded[1:-1, :-2, 1:-1]
        + padded[1:-1, 2:, 1:-1]
    )
    return (
        lateral_weight * (4.0 * iterate - lateral)
        + down_faces * (iterate - padded[1:-1, 1:-1, :-2])
        + up_faces * (iterate - padded[1:-1, 1:-1, 2:])
    )


def restrict(field):
    first_extent, second_extent, depth = field.shape
    return field.reshape(first_extent // 2, 2, second_extent // 2, 2, depth).sum(axis=(1, 3)) * 0.25


def prolong(padded):
    first_extent = padded.shape[0] - 2
    second_extent = padded.shape[1] - 2
    depth = padded.shape[2]
    even_rows = 0.75 * padded[1:-1] + 0.25 * padded[:-2]
    odd_rows = 0.75 * padded[1:-1] + 0.25 * padded[2:]
    widened = jnp.stack([even_rows, odd_rows], 1).reshape(
        2 * first_extent, second_extent + 2, depth
    )
    even_rows = 0.75 * widened[:, 1:-1] + 0.25 * widened[:, :-2]
    odd_rows = 0.75 * widened[:, 1:-1] + 0.25 * widened[:, 2:]
    return jnp.stack([even_rows, odd_rows], 2).reshape(2 * first_extent, 2 * second_extent, depth)


def body(right_side, z_faces, xy_coupling, block_inverse):
    device_index = lax.axis_index("gz")
    levels_count = block_inverse.shape[0]
    last_cell = block_inverse.shape[1] - 1
    corner = jnp.stack(
        [
            block_inverse[:, 0, 0],
            block_inverse[:, 0, last_cell],
            block_inverse[:, last_cell, 0],
            block_inverse[:, last_cell, last_cell],
        ],
        -1,
    )[None]
    corners, firsts = (
        lax.all_gather(corner, "gz", axis=0, tiled=True),
        lax.all_gather(z_faces[:1], "gz", axis=0, tiled=True),
    )
    couplings = firsts[1:]
    edge_faces = jnp.concatenate([firsts, jnp.ones((1,), jnp.float32)])
    top_face = lax.dynamic_slice_in_dim(edge_faces, device_index + 1, 1, 0)
    up_faces = jnp.concatenate([z_faces[1:], top_face])
    solvers = [
        make_solver(
            block_inverse[level],
            corners[:, level],
            couplings,
            device_index,
            z_faces[0],
            top_face[0],
        )
        for level in range(levels_count)
    ]

    def operator(iterate, level):
        return apply_operator(iterate, xy_coupling[level], z_faces, up_faces)

    def multigrid_cycle(source, level):
        iterate = damping * solvers[level](source)
        iterate = iterate + damping * solvers[level](source - operator(iterate, level))
        if level == LEVELS - 1:
            return iterate
        coarse = multigrid_cycle(restrict(source - operator(iterate, level)), level + 1)
        widened = extended(coarse, (("gx", 0), ("gy", 1)), 1)
        iterate = iterate + prolong(widened)
        for sweep in range(SWEEPS):
            iterate = iterate + damping * solvers[level](source - operator(iterate, level))
        return iterate

    solution = multigrid_cycle(right_side, 0)
    return (solution, right_side - operator(solution, 0))


MESH = pl.DeviceIdType.MESH
HALOS = (4, 6, 6)
ROWS = (4, 5, 6)
YPAD = 8
SPARE = 32
DEEPEST = 3
NEAR = 2


def block_range(offset, own, halo, extent):
    start = offset * own - halo
    low = max(0, start)
    high = min(extent, (offset + 1) * own + halo)
    return low, high - low, low - start


def round_up(value, unit):
    return -(-value // unit) * unit


def difference(outer, inner):
    (a, b), (c, d) = outer
    (e, f), (g, h) = inner
    if e >= f or g >= h:
        return [outer]
    parts = [((a, e), (c, d)), ((f, b), (c, d)), ((e, f), (c, g)), ((e, f), (h, d))]
    return [(x, y) for x, y in parts if x[0] < x[1] and y[0] < y[1]]


def needed(t, dy, own, size, halos):
    (n0, n1), (s0, s1), (left, right, side) = own, size, halos
    x = max(0, t * n0 - left), min(s0, (t + 1) * n0 + right)
    y = max(0, dy * n1 - side), min(s1, (dy + 1) * n1 + side)
    return x, y


def vacant(part):
    return any(low >= high for low, high in part)


def both_parts(t, dy, own, size, near, far):
    whole = needed(t, dy, own, size, far)
    inner = needed(t, dy, own, size, near) if near else ((0, 0), (0, 0))
    common = tuple((max(a, c), min(b, d)) for (a, b), (c, d) in zip(whole, inner))
    outer = [] if vacant(whole) else difference(whole, common)
    return [] if vacant(inner) else [inner], outer


def area(parts):
    return sum((x[1] - x[0]) * (y[1] - y[0]) for x, y in parts)


def split_planes(count, rows):
    return max(c for c in range(1, count + 1) if count % c == 0 and c * rows <= 448)


def cycle_kernel(geometry, f_hbm, z_hbm, e_hbm, g_hbm, sol_ref, res_ref, *scratch):
    gx_n, gy_n, gz_n, nx, ny, depth, levels = geometry
    refs = iter(scratch)
    take = lambda count: [next(refs) for _ in range(count)]
    sinv, g_all, z_all, gather, f_v, e_ref = take(6)
    X = [take(3) for _ in range(DEEPEST + 1)]
    X.append(take(1))
    C = take(DEEPEST + 1)
    E = take(DEEPEST + 1)
    (U1, G1, U2, G2, c3u, c3g, c4u, c4g, cwu, cwg) = take(10)
    UP, GP = [None, U1, U2, c3u, c4u], [None, G1, G2, c3g, c4g]
    own3, pool = take(2)
    T = take(DEEPEST + 1)
    N = take(DEEPEST)
    (in_sem, g_send, g_recv, h_send, h_recv, y_recv, p_sem) = take(7)
    r_send, r_recv = take(2)
    y_send, x_send, x_recv, o_send, o_recv = [p_sem.at[i] for i in range(5)]

    ix, iy, iz = lax.axis_index("gx"), lax.axis_index("gy"), lax.axis_index("gz")
    bx = ix * gz_n + iz
    bx_n = gx_n * gz_n
    f32 = jnp.float32

    whole = gz_n * depth
    keep = 1.0 - damping

    def owned(level):
        return nx >> level, ny >> level

    def copy(src, dst, send, recv, device):
        return pltpu.make_async_remote_copy(
            src_ref=src,
            dst_ref=dst,
            send_sem=send,
            recv_sem=recv,
            device_id=device,
            device_id_type=MESH,
        )

    def inside(x, y):
        return (x >= 0) & (x < gx_n) & (y >= 0) & (y < gy_n)

    parts = 4
    span = f_v.shape[0] // parts
    for i in range(parts):
        at = pl.ds(i * span, span)
        pltpu.make_async_copy(f_hbm.at[at], f_v.at[at], in_sem.at[0]).start()
    f_load = pltpu.make_async_copy(f_hbm, f_v, in_sem.at[0])
    rest = pl.ds(1, levels - 1)
    loads = [
        pltpu.make_async_copy(z_hbm, z_all.at[iz], in_sem.at[1]),
        pltpu.make_async_copy(g_hbm.at[0], g_all.at[0, iz], in_sem.at[2]),
        pltpu.make_async_copy(g_hbm.at[rest], g_all.at[rest, iz], in_sem.at[3]),
        pltpu.make_async_copy(e_hbm, e_ref, in_sem.at[4]),
    ]
    for c in loads:
        c.start()

    reach_all = max(
        gz_n - 1 - (-HALOS[0] // nx), *[-(-HALOS[k] // owned(k)[0]) for k in (1, 2)]
    )
    barrier = pltpu.get_barrier_semaphore()
    partners = jnp.int32(0)
    for dx in range(1 - bx_n, bx_n):
        for dy in range(1 - gy_n, gy_n):
            close = abs(dx) <= reach_all and abs(dy) <= 1
            if (dx == 0 and dy == 0) or not close:
                continue
            x, y = bx + dx, iy + dy
            ok = (x >= 0) & (x < bx_n) & (y >= 0) & (y < gy_n)

            @pl.when(ok)
            def _():
                pl.semaphore_signal(
                    barrier,
                    inc=1,
                    device_id=(x // gz_n, y, lax.rem(x, gz_n)),
                    device_id_type=MESH,
                )

            partners = partners + jnp.where(ok, 1, 0).astype(jnp.int32)

    def setup_copies(other):
        here = (ix, iy, lax.rem(iz + other, gz_n))
        out = []
        for i, block in enumerate((z_all.at[iz], g_all.at[0, iz], g_all.at[rest, iz])):
            out.append(copy(block, block, g_send.at[other, i], g_recv.at[other, i], here))
        return out

    def runs(count, key):
        out = []
        for i in range(count):
            if out and key(i) == out[-1][2]:
                out[-1][1] = i
            else:
                out.append([i, i, key(i)])
        return [(low, high) for low, high, _ in out]

    def take_rows(sem, rows):
        block = pool.at[pl.ds(0, rows)]
        pltpu.make_async_copy(block, block, sem).wait()

    def settle(sem, total):
        table = [[total(b, y) for y in range(gy_n)] for b in range(bx_n)]
        for low, high in runs(bx_n, lambda b: table[b]):
            for first, last in runs(gy_n, lambda y: [row[y] for row in table]):

                @pl.when((bx >= low) & (bx <= high) & (iy >= first) & (iy <= last))
                def _():
                    take_rows(sem, table[low][first])

    near0, far0 = N[0], X[0][0]
    plan0 = []
    reach = -(-ROWS[0] // nx)
    for t in range(-reach, gz_n + reach):
        for dy in (-1, 0, 1):
            near_halo, far_halo = (NEAR,) * 3, (ROWS[0],) * 3
            parts0 = both_parts(t, dy, (nx, ny), (nx * gz_n, ny), near_halo, far_halo)
            plan0.append((t, t // gz_n, t % gz_n, dy, parts0))
    plan0.sort(key=lambda entry: -abs(entry[1]) - abs(entry[3]))

    def target0(window, part, t, dy, source_z):
        (x0, x1), (y0, y1) = part
        p, r = x0 - t * nx + HALOS[0], y0 - dy * ny + YPAD
        return window.at[pl.ds(p, x1 - x0), source_z, pl.ds(r, y1 - y0), :]

    local0 = []
    for t, dgx, target, dy, parts0 in plan0:
        if dgx == 0 and dy == 0:
            for which, window in enumerate((near0, far0)):
                for part in parts0[which]:
                    (x0, x1), (y0, y1) = part
                    move = pltpu.make_async_copy(
                        f_hbm.at[pl.ds(x0, x1 - x0), pl.ds(y0, y1 - y0), :],
                        target0(window, part, t, dy, target),
                        in_sem.at[5 + which],
                    )
                    local0.append((target, which, move))

    for target, _, move in local0:

        @pl.when(iz == target)
        def _():
            move.start()

    def local_done(which):
        for target, other, move in local0:
            if other == which:

                @pl.when(iz == target)
                def _():
                    move.wait()

    def send0(which):
        for t, dgx, target, dy, parts0 in plan0:
            ok = inside(ix + dgx, iy + dy)
            if dgx == 0 and dy == 0:
                ok = ok & (iz != target)

            @pl.when(ok)
            def _():
                for part in parts0[which]:
                    (x0, x1), (y0, y1) = part
                    copy(
                        f_v.at[pl.ds(x0, x1 - x0), pl.ds(y0, y1 - y0), :],
                        target0((near0, far0)[which], part, t, dy, iz),
                        h_send.at[0],
                        h_recv.at[0, which],
                        (ix + dgx, iy + dy, target),
                    ).start()

    def in_grid(b, y):
        return 0 <= b < bx_n and 0 <= y < gy_n

    def sent0(b, y):
        total = 0
        for t, dgx, target, dy, parts0 in plan0:
            there = (b // gz_n + dgx) * gz_n + target
            if in_grid(there, y + dy) and (there, dy) != (b, 0):
                total += area(parts0[0]) + area(parts0[1])
        return total

    def received0(which):
        def count(b, y):
            total = 0
            for t, dgx, target, dy, parts0 in plan0:
                for source_z in range(gz_n):
                    there = (b // gz_n - dgx) * gz_n + source_z
                    ok = target == b % gz_n and in_grid(there, y - dy)
                    if ok and (there, dy) != (b, 0):
                        total += area(parts0[which])
            return total

        return count

    def clear_edges():
        for level, window in [(k, w) for k in range(DEEPEST) for w in (N[k], X[k][0])]:
            planes, zb, rows, lanes = window.shape
            halo = HALOS[level]
            n0, n1 = owned(level)
            reach = -(-halo // n0)
            for t in range(1, reach + 1):
                low = max(0, halo - t * n0)
                high = halo - (t - 1) * n0
                plane = jnp.zeros((high - low, zb, n1 + 2 * YPAD, lanes), f32)

                @pl.when(bx - t < 0)
                def _():
                    window[low:high, :, pl.ds(0, n1 + 2 * YPAD)] = plane

                low2, high2 = planes - high, planes - low

                @pl.when(bx + t >= bx_n)
                def _():
                    window[low2:high2, :, pl.ds(0, n1 + 2 * YPAD)] = plane

            edge = jnp.zeros((zb, YPAD, lanes), f32)

            @pl.when(iy == 0)
            def _():
                lax.fori_loop(0, planes, lambda i, c: zero_rows(window, i, 0, edge), 0)

            @pl.when(iy == gy_n - 1)
            def _():
                lax.fori_loop(
                    0, planes, lambda i, c: zero_rows(window, i, YPAD + n1, edge), 0
                )

    def fill_border(ref, side):
        planes, zb, rows, lanes = ref.shape
        plane = jnp.zeros((side, zb, rows, lanes), f32)
        edge = jnp.zeros((zb, YPAD, lanes), f32)
        ref[0:side] = plane
        ref[planes - side : planes] = plane

        def step(i, _):
            ref[i, :, pl.ds(0, YPAD)] = edge
            ref[i, :, pl.ds(rows - YPAD, YPAD)] = edge
            return 0

        lax.fori_loop(side, planes - side, step, 0, unroll=4)

    def clear_coarse():
        side = HALOS[2] // 2 + 1
        for ref in (X[3][0], X[3][2], T[3], C[3], X[4][0], c4u, c4g):
            fill_border(ref, 1)
        for ref in (c3u, c3g):
            fill_border(ref, side)

    def assemble(level, _):
        merged = g_all[level, 0]
        for k in range(1, gz_n):
            block = g_all[level, k]
            size, cz = merged.shape[0], block.shape[0]
            face = z_all[k][:, 0:1]
            a, d = block[0:1, 0:1], merged[size - 1 : size, size - 1 : size]
            last, first = merged[size - 1 : size], block[0:1]
            scale = face / (1.0 - face * face * a * d)
            p_row = jnp.concatenate([face * a * last, first], 1) * scale
            q_row = jnp.concatenate([last, face * d * first], 1) * scale
            top = jnp.concatenate([merged, jnp.zeros((size, cz), f32)], 1)
            low = jnp.concatenate([jnp.zeros((cz, size), f32), block], 1)
            top = top + merged[:, size - 1 : size] * p_row
            low = low + block[:, 0:1] * q_row
            merged = jnp.concatenate([top, low], 0)
        solve = (damping * merged).astype(jnp.bfloat16)
        sinv[level, pl.ds(0, whole), :] = solve
        twice = jnp.dot(solve, solve, preferred_element_type=f32)
        sinv[level, pl.ds(whole, whole), :] = twice.astype(jnp.bfloat16)
        return 0

    def plane_mask(level, i):
        n0 = owned(level)[0]
        x = bx * n0 - HALOS[level] + i
        return jnp.where((x >= 0) & (x < bx_n * n0), 1.0, 0.0).astype(f32)

    def row_mask(level, first, rows, stride):
        n1 = owned(level)[1]
        y = lax.broadcasted_iota(jnp.int32, (rows, depth), 0) * stride + first
        y = y + iy * n1 - YPAD
        return jnp.where((y >= 0) & (y < gy_n * n1), 1.0, 0.0).astype(f32)

    def region(level, shrink=0):
        if level < DEEPEST:
            return nearby(level, ROWS[level] - shrink)
        window = X[level][0].shape
        return 1, window[0] - 2, YPAD, window[2] - 2 * YPAD

    def nearby(level, h, extra=0):
        n0, n1 = owned(level)
        first = HALOS[level] - h - extra
        return first, n0 + 2 * h + extra, YPAD - h, round_up(n1 + 2 * h, 8)

    def weights(level, p, c, r0, rows):
        e = e_ref[level]
        if level >= DEEPEST:
            return e
        mask = row_mask(level, r0, rows, 1)
        return jnp.stack([mask * (e * plane_mask(level, p + i)) for i in range(c)])

    def chunks(where):
        p0, planes, r0, rows = where
        c = split_planes(planes, rows)
        return [(p0 + s * c, c, r0, rows) for s in range(planes // c)]

    def around(src, k, p, c, r0, rows):
        at = lambda dp, dr: src[pl.ds(p + dp, c), k, pl.ds(r0 + dr, rows)]
        return (at(-1, 0) + at(1, 0)) + (at(0, -1) + at(0, 1))

    def product(level, first, *groups):
        flat = [v.reshape(-1, depth) for fields in groups for v in fields]
        lhs = jnp.concatenate(flat, 1).astype(jnp.bfloat16)
        rhs = sinv[level, pl.ds(first * whole, len(groups) * whole), :]
        out = jnp.dot(lhs, rhs, preferred_element_type=f32)
        shape = groups[0][0].shape
        return [out[:, k * depth : (k + 1) * depth].reshape(shape) for k in range(gz_n)]

    def relax(level, src, dst, where):
        for p, c, r0, rows in chunks(where):
            w = weights(level, p, c, r0, rows)
            total = [around(src, k, p, c, r0, rows) * w for k in range(gz_n)]
            out = product(level, 0, total)
            for k in range(gz_n):
                value = keep * src[pl.ds(p, c), k, pl.ds(r0, rows)] + out[k]
                dst[pl.ds(p, c), k, pl.ds(r0, rows)] = value

    def spread(level, src, where):
        for p, c, r0, rows in chunks(where):
            w = weights(level, p, c, r0, rows)
            for k in range(gz_n):
                T[level][pl.ds(p, c), k, pl.ds(r0, rows)] = around(src, k, p, c, r0, rows) * w

    def relax_twice(level, src, where, once, put):
        for p, c, r0, rows in chunks(where):
            w = weights(level, p, c, r0, rows)
            at = lambda ref, k: ref[pl.ds(p, c), k, pl.ds(r0, rows)]
            one = [at(T[level], k) for k in range(gz_n)]
            two = [around(T[level], k, p, c, r0, rows) * w for k in range(gz_n)]
            if once is None:
                out = product(level, 0, [2.0 * keep * v for v in one], two)
            else:
                first, second = product(level, 0, one), product(level, 1, two)
                out = [second[k] + 2.0 * keep * first[k] for k in range(gz_n)]
            for k in range(gz_n):
                value = at(src, k)
                if once is not None:
                    once[pl.ds(p, c), k, pl.ds(r0, rows)] = keep * value + first[k]
                put(k, p, c, r0, rows, keep * keep * value + out[k])

    def into(ref):
        def put(k, p, c, r0, rows, value):
            ref[pl.ds(p, c), k, pl.ds(r0, rows)] = value

        return put

    def sums(level, p, c, r0, rows):
        at = lambda ref, k: ref[pl.ds(p, c), k, pl.ds(r0, rows)]
        last = X[level][-1]
        total = []
        for k in range(gz_n):
            value = (1.0 + keep) * at(last, k)
            if level <= DEEPEST:
                value = value + (at(X[level][0], k) + at(X[level][1], k))
            total.append(value)
        return total

    def finish(level, where, offset=0):
        last = X[level][-1]
        for p, c, r0, rows in chunks(where):
            w = weights(level, p, c, r0, rows)
            at = lambda ref, k: ref[pl.ds(p, c), k, pl.ds(r0, rows)]
            total = sums(level, p, c, r0, rows)
            side = [around(last, k, p, c, r0, rows) * w for k in range(gz_n)]
            rest = product(level, 0, side)
            u = product(level, 0, total, side)
            for k in range(gz_n):
                if level <= DEEPEST:
                    u[k] = u[k] + at(C[level], k)
                g = damping * (total[k] + rest[k])
                g = g + (4.0 * (e_ref[level - 1] - e_ref[level])) * u[k]
                if level <= DEEPEST:
                    g = g + at(E[level], k)
                UP[level][pl.ds(p + offset, c), k, pl.ds(r0, rows)] = u[k]
                GP[level][pl.ds(p + offset, c), k, pl.ds(r0, rows)] = g

    def finest(where, place):
        for p, c, r0, rows in chunks(where):
            at = lambda ref, k: ref[pl.ds(p, c), k, pl.ds(r0, rows)]
            total = sums(0, p, c, r0, rows)
            u = product(0, 0, total, [at(T[0], k) for k in range(gz_n)])
            for k in range(gz_n):
                sol_ref[k, pl.ds(place + p - where[0], c)] = u[k] + at(C[0], k)

    def restrict_planes(level, dst, planes, x0, y0, to_plane, to_row, rows):
        src = X[level][2]
        for j in range(planes):
            for k in range(gz_n):
                total = None
                for a in (0, 1):
                    for b in (0, 1):
                        part = src[x0 + 2 * j + a, k, pl.ds(y0 + b, rows, 2), :]
                        total = part if total is None else total + part
                dst[to_plane + j, k, pl.ds(to_row, rows), :] = total * 0.25

    def prolong(level, x0, y0, coarse):
        shift = 1 if level >= DEEPEST else 0
        p0, planes, r0, rows = region(level, 1)
        low, high = p0 - shift, p0 - shift + planes
        first = r0 // 2 * 2
        half = round_up((r0 + rows - first + 1) // 2, 8) if level < DEEPEST else rows // 2
        start = y0 + (first // 2 if level < DEEPEST else 0)
        masks = [
            row_mask(level, first + b, half, 2) if level < DEEPEST else None for b in (0, 1)
        ]
        mixes = {}

        def mixed(src, index, j, k):
            key = (index, j, k)
            if key not in mixes:
                load = lambda dy: src[x0 + j, k, pl.ds(start + dy, half), :]
                quarter = 0.25 * load(0)
                near = load(0) - quarter
                out = []
                for dy in (-1, 1):
                    value = near + 0.25 * load(dy)
                    far = 0.25 * value
                    out.append((value - far, far))
                mixes[key] = out
            return mixes[key]

        for j in range(low // 2, (high - 1) // 2 + 1):
            for a in (0, 1):
                p = 2 * j + a
                if not low <= p < high:
                    continue
                for b in (0, 1):
                    if level < DEEPEST:
                        mask = masks[b] * plane_mask(level, p)
                    for index, (src, dst) in enumerate(coarse):
                        for k in range(gz_n):
                            near = mixed(src, index, j, k)[b][0]
                            value = near + mixed(src, index, j + 2 * a - 1, k)[b][1]
                            if level < DEEPEST:
                                value = value * mask
                            dst[p + shift, k, pl.ds(first + b, half, 2), :] = value

    def correct(level, coarse_u, coarse_g, x0, y0):
        prolong(level, x0, y0, [(coarse_u, C[level]), (coarse_g, E[level])])
        where = region(level, 2)
        target = X[level][2]
        for p, c, r0, rows in chunks(where):
            w = weights(level, p, c, r0, rows)
            for k in range(gz_n):
                at = lambda ref: ref[pl.ds(p, c), k, pl.ds(r0, rows)]
                total = around(C[level], k, p, c, r0, rows) * w
                target[pl.ds(p, c), k, pl.ds(r0, rows)] = at(target) + (total - at(E[level]))

    def near_halos(level, core):
        if level < DEEPEST - 1:
            return (NEAR,) * 3
        if core < gz_n - 1:
            return None
        return NEAR + owned(level)[0] * core, NEAR, NEAR

    def far_halos(level, core):
        width = ROWS[level]
        return (0 if core else width), (width if core else 0), width

    def relay(level):
        n0, n1 = owned(level)
        width, halo = ROWS[level], HALOS[level]
        rows = pl.ds(YPAD - width, n1 + 2 * width)
        window = X[level][0]
        def move(core):
            src, dst = ((halo + n0 - width, halo - width), (halo, halo + n0))[core]
            return copy(
                window.at[pl.ds(src, width), :, rows, :],
                window.at[pl.ds(dst, width), :, rows, :],
                r_send.at[level - 1],
                r_recv.at[level - 1],
                (ix, iy, 1 - core),
            )

        return move

    def exchange(level):
        n0, n1 = owned(level)
        width = ROWS[level]
        halo = HALOS[level]
        reach = -(-width // n0)
        pieces = []
        for t in range(-reach, reach + 1):
            for dy in (-1, 0, 1):
                if t or dy:
                    parts = [
                        both_parts(
                            t,
                            dy,
                            (n0, n1),
                            (n0, n1),
                            near_halos(level, core),
                            far_halos(level, core),
                        )
                        for core in range(gz_n)
                    ]
                    pieces.append((t, dy, parts))
        pieces.sort(key=lambda piece: -abs(piece[0]) - abs(piece[1]))

        def start(which):
            window = (N[level], X[level][0])[which]
            for t, dy, parts in pieces:
                there = bx + t + bx_n
                core = lax.rem(there, gz_n)
                x, y = bx + t, iy + dy
                alike = all(part == parts[0] for part in parts)
                for target in range(1 if alike else gz_n):
                    ok = (x >= 0) & (x < bx_n) & (y >= 0) & (y < gy_n)
                    if not alike:
                        ok = ok & (core == target)
                    if not parts[target][which]:
                        continue

                    @pl.when(ok)
                    def _():
                        for (x0, x1), (y0, y1) in parts[target][which]:
                            p, r = x0 - t * n0 + halo, y0 - dy * n1 + YPAD
                            copy(
                                N[level].at[
                                    pl.ds(halo + x0, x1 - x0),
                                    :,
                                    pl.ds(YPAD + y0, y1 - y0),
                                    :,
                                ],
                                window.at[pl.ds(p, x1 - x0), :, pl.ds(r, y1 - y0), :],
                                h_send.at[level],
                                h_recv.at[level, which],
                                (there // gz_n - gx_n, y, core),
                            ).start()

        def total(sign, wanted):
            def count(b, y):
                rows = 0
                for t, dy, parts in pieces:
                    if in_grid(b + sign * t, y + sign * dy):
                        core = (b + t) % gz_n if sign > 0 else b % gz_n
                        rows += sum(gz_n * area(parts[core][which]) for which in wanted)
                return rows

            return count

        arrive = lambda which: settle(h_recv.at[level, which], total(-1, (which,)))
        return start, arrive, lambda: settle(h_send.at[level], total(1, (0, 1)))

    def widen(level, arrive):
        n0, n1 = owned(level)
        for core in range(gz_n):
            near = near_halos(level, core) or (0, 0, 0)
            far = far_halos(level, core) if level else near
            left, right, side = (min(a, b) for a, b in zip(near, far))
            rows = pl.ds(YPAD - side, n1 + 2 * side)

            @pl.when(iz == core)
            def _():
                for p in range(HALOS[level] - left, HALOS[level] + n0 + right):
                    X[level][0][p, :, rows] = N[level][p, :, rows]

        arrive(1)
        if level:
            for core in range(gz_n):

                @pl.when(iz == core)
                def _():
                    relay(level)(core).start()

            relay(level)(0).wait_recv()
        relax(level, X[level][0], X[level][1], region(level, 1))
        relax(level, X[level][1], X[level][2], region(level, 2))
        if level:
            relay(level)(0).wait_send()

    def gather_all(meanwhile):
        leader = gz_n - 1
        leading = iz == leader

        def line_y(other, slot):
            return copy(own3, gather.at[ix, slot], y_send, y_recv.at[slot], (ix, other, leader))

        def share(src, slot):
            for core in range(gz_n):
                for s in range(1, gx_n):
                    other = (lax.rem(ix + s, gx_n), iy, core)
                    copy(src, gather.at[ix, slot], x_send, x_recv, other).start()
            for core in range(leader):
                copy(src, gather.at[ix, slot], x_send, x_recv, (ix, iy, core)).start()

        @pl.when(leading)
        def _():
            for s in range(1, gy_n):
                line_y(lax.rem(iy + s, gy_n), iy).start()
            share(own3, iy)
            gather[ix, iy] = own3[...]
            for distance in range(1, gy_n):
                for y in (iy + distance, iy - distance):

                    @pl.when((y >= 0) & (y < gy_n))
                    def _():
                        line_y(y, y).wait_recv()
                        share(gather.at[ix, y], y)

        meanwhile()
        size = own3.shape[0] * own3.shape[1] * own3.shape[2]

        @pl.when(leading)
        def _():
            take_rows(x_recv, (gx_n - 1) * gy_n * size)

        @pl.when(iz < leader)
        def _():
            take_rows(x_recv, gx_n * gy_n * size)

        n0, n1 = owned(3)
        window = X[3][0]

        def place(b, _):
            for i in range(gz_n * n0):
                for y in range(gy_n):
                    at = 1 + b * gz_n * n0 + i
                    window[at, :, pl.ds(YPAD + y * n1, n1), :] = gather[b, y, i]
            return 0

        lax.fori_loop(0, gx_n, place, 0)

        def drains():
            @pl.when(leading)
            def _():
                take_rows(y_send, (gy_n - 1) * size)
                for _ in range(gy_n):
                    take_rows(x_send, (gx_n * gz_n - 1) * size)

        return drains

    f_load.wait()
    pl.semaphore_wait(barrier, partners)
    send0(0)
    for c in loads:
        c.wait()
    setups = [setup_copies(other) for other in range(1, gz_n)]
    for group in setups:
        for c in group[:2]:
            c.start()
    clear_edges()
    send0(1)
    for group in setups:
        for c in group[:2]:
            c.wait()
    assemble(0, 0)
    local_done(0)

    def arrive0(which):
        if which:
            local_done(1)
        settle(h_recv.at[0, which], received0(which))

    def later():
        for group in setups:
            group[2].wait()
        lax.fori_loop(1, levels, assemble, 0)

    arrive = arrive0
    drains = [lambda: settle(h_send.at[0], sent0)]
    for level in range(DEEPEST):
        arrive(0)
        extra = owned(level)[0] * (gz_n - 1) if level == DEEPEST - 1 else 0
        spread(level, N[level], nearby(level, 1, extra))
        relax_twice(level, N[level], nearby(level, 0, extra), None, into(X[level][2]))
        n0, n1 = owned(level + 1)
        p, r = HALOS[level], YPAD
        if level < DEEPEST - 1:
            restrict_planes(level, N[level + 1], n0, p, r, HALOS[level + 1], YPAD, n1)
            start, following, drain = exchange(level + 1)
            drains.append(drain)
            start(0)
            start(1)
            if level == 0:
                for group in setups:
                    group[2].start()
                widen(level, arrive)
                later()
            else:
                clear_coarse()
                widen(level, arrive)
            arrive = following
        else:
            restrict_planes(level, own3, gz_n * n0, p - extra, r, 0, 0, n1)
            drains.append(gather_all(lambda: widen(level, arrive)))

    whole3, whole4 = region(3, 0), region(4, 0)
    spread(3, X[3][0], whole3)
    relax_twice(3, X[3][0], whole3, X[3][1], into(X[3][2]))
    restrict_planes(3, X[4][0], whole4[1], 1, YPAD, 1, YPAD, whole4[3])
    finish(4, whole4)
    correct(3, c4u, c4g, 1, YPAD)
    pad3 = HALOS[2] // 2 + 1
    finish(3, whole3, offset=pad3 - 1)
    n0, n1 = owned(3)
    margin = YPAD // 2
    for y in range(gy_n):

        @pl.when(iy == y)
        def _():
            for j in range(HALOS[2] + 2 * n0):
                for src, dst in ((c3u, cwu), (c3g, cwg)):
                    dst[j, :, pl.ds(margin, n1 + 4 * margin), :] = src[
                        bx * n0 + j, :, pl.ds(y * n1, n1 + 4 * margin), :
                    ]

    for level in (2, 1, 0):
        if level == 2:
            correct(2, cwu, cwg, 1, YPAD)
        else:
            x0 = HALOS[level + 1] - HALOS[level] // 2
            correct(level, UP[level + 1], GP[level + 1], x0, YPAD // 2)
        if level:
            finish(level, region(level, 3))
        else:
            spread(0, X[0][2], region(0, 3))

    def send_out(ref, p, c):
        for other in range(1, gz_n):
            there = lax.rem(iz + other, gz_n)
            block = ref.at[there, pl.ds(iz * nx + p, c)]
            copy(block, block, o_send, o_recv, (ix, iy, there)).start()

    own0 = nearby(0, 0)
    finest(own0, iz * nx)
    send_out(sol_ref, 0, nx)

    def store(k, p, c, r0, rows, value):
        res_ref[k, pl.ds(iz * nx + p - own0[0], c)] = value

    relax_twice(0, X[0][2], own0, None, store)
    send_out(res_ref, 0, nx)
    for drain in drains:
        drain()
    for sem in (o_send, o_recv):
        take_rows(sem, (gz_n - 1) * 2 * nx * ny)


def zero_rows(ref, i, at, value):
    ref[i, :, pl.ds(at, YPAD), :] = value
    return 0


def store_kernel(pieces, sol_v, res_v, sol_hbm, res_hbm, sem):
    iz = lax.axis_index("gz")
    span = sol_hbm.shape[0] // pieces
    moves = []
    for which, (src, dst) in enumerate(((sol_v, sol_hbm), (res_v, res_hbm))):
        for i in range(pieces):
            at = pl.ds(i * span, span)
            moves.append(
                pltpu.make_async_copy(src.at[iz, at], dst.at[at], sem.at[which, i])
            )
    for move in moves:
        move.start()
    for move in moves:
        move.wait()


def fits(mesh, shape, inverse_shape):
    gx_n, gy_n, gz_n = (mesh.shape[a] for a in ("gx", "gy", "gz"))
    nx, ny = shape[0] // (gx_n * gz_n), shape[1] // gy_n
    return (
        inverse_shape[0] == LEVELS == 5
        and SWEEPS == 2
        and inverse_shape[2] == 128
        and nx % 8 == 0
        and ny % 32 == 0
        and (shape[1] >> 4) % 8 == 0
        and gz_n == 2 and gy_n <= 4
    )


def fused_body(mesh, right_side, z_faces, xy_coupling, block_inverse):
    gx_n, gy_n, gz_n = (mesh.shape[a] for a in ("gx", "gy", "gz"))
    levels, _, depth = block_inverse.shape
    nx, ny = right_side.shape[0] // gz_n, right_side.shape[1]
    windows = []
    for level in range(levels):
        if level < DEEPEST:
            size = ((nx >> level) + 2 * HALOS[level], (ny >> level) + SPARE)
        else:
            size = (
                ((nx * gx_n * gz_n) >> level) + 2,
                ((ny * gy_n) >> level) + 2 * YPAD,
            )
        windows.append((size[0], gz_n, size[1], depth))
    vmem = lambda shape: pltpu.VMEM(shape, jnp.float32)
    full3, full4 = windows[3], windows[4]
    pad3 = HALOS[2] // 2 + 1
    c4 = full4
    c3 = (full3[0] - 2 + 2 * pad3,) + full3[1:]
    cw = (windows[2][0] // 2 + 2, gz_n, (ny >> 3) + 28, depth)
    most = gz_n * (nx + 2 * HALOS[0] + 8) * (ny + 2 * YPAD)
    dma = pltpu.SemaphoreType.DMA
    chip3 = (gz_n * (nx >> 3), gz_n, ny >> 3, depth)
    scratch = (
        [
            pltpu.VMEM((levels, 2 * gz_n * depth, gz_n * depth), jnp.bfloat16),
            vmem((levels, gz_n, depth, depth)),
            vmem((gz_n, 1, depth)),
            vmem((gx_n, gy_n) + chip3),
            vmem(right_side.shape),
            pltpu.SMEM((levels,), jnp.float32),
        ]
        + [vmem(w) for w in windows[: DEEPEST + 1] for _ in range(3)]
        + [vmem(full4)]
        + [vmem(w) for w in windows[: DEEPEST + 1]] * 2
        + [vmem(windows[1])] * 2
        + [vmem(windows[2])] * 2
        + [vmem(c3), vmem(c3), vmem(c4), vmem(c4), vmem(cw), vmem(cw)]
        + [vmem(chip3), vmem((most, depth))]
        + [vmem(w) for w in windows[: DEEPEST + 1]]
        + [vmem(w) for w in windows[:DEEPEST]]
        + [dma((7,))]
        + [dma((gz_n, 3))] * 2
        + [dma((DEEPEST,)), dma((DEEPEST, 2))]
        + [dma((gy_n,)), dma((5,))]
        + [dma((DEEPEST - 1,))] * 2
    )
    in_vmem = pl.BlockSpec(memory_space=pltpu.VMEM)
    in_hbm = pl.BlockSpec(memory_space=pltpu.HBM)
    staged = (gz_n,) + right_side.shape
    hold = lambda x: pltpu.with_memory_space_constraint(x, pltpu.HBM)
    halves = pl.pallas_call(
        functools.partial(cycle_kernel, (gx_n, gy_n, gz_n, nx, ny, depth, levels)),
        out_shape=[pltpu.VMEM(staged, jnp.float32)] * 2,
        in_specs=[
            in_hbm,
            in_hbm,
            in_hbm,
            in_hbm,
        ],
        out_specs=[in_vmem, in_vmem],
        scratch_shapes=scratch,
        compiler_params=pltpu.CompilerParams(
            collective_id=0, has_side_effects=True, vmem_limit_bytes=48 * 1024 * 1024
        ),
    )(hold(right_side), hold(z_faces.reshape(1, -1)), hold(xy_coupling), hold(block_inverse))
    pieces = 4
    return tuple(
        pl.pallas_call(
            functools.partial(store_kernel, pieces),
            out_shape=[jax.ShapeDtypeStruct(right_side.shape, jnp.float32)] * 2,
            in_specs=[in_vmem, in_vmem],
            out_specs=[in_hbm, in_hbm],
            scratch_shapes=[dma((2, pieces))],
        )(*[pltpu.with_memory_space_constraint(x, pltpu.VMEM) for x in halves])
    )


def solution(mesh):
    def call(right_side, z_faces, xy_coupling, block_inverse):
        local = body
        if fits(mesh, right_side.shape, block_inverse.shape):
            local = functools.partial(fused_body, mesh)
        return jax.shard_map(
            local,
            mesh=mesh,
            in_specs=(P("gx", "gy", "gz"), P("gz"), P(), P(None, "gz", None)),
            out_specs=(P("gx", "gy", "gz"), P("gx", "gy", "gz")),
            check_vma=False,
        )(right_side, z_faces, xy_coupling, block_inverse)

    return call
```

```python
import functools

import jax
import jax.numpy as jnp
from jax import lax
from jax.experimental import pallas as pl
from jax.experimental.pallas import tpu as pltpu
from jax.sharding import PartitionSpec as P

LEVELS = 5
SWEEPS = 2


damping = 0.8
highest = lax.Precision.HIGHEST


def extended(cells, sides, width):
    for axis, dim in sides:
        count = lax.axis_size(axis)
        ends = count - 1
        head = lax.slice_in_dim(cells, 0, width, axis=dim)
        tail = lax.slice_in_dim(cells, cells.shape[dim] - width, cells.shape[dim], axis=dim)
        cells = jnp.concatenate(
            [
                lax.ppermute(tail, axis, [(i, (i + 1) % count) for i in range(ends)]),
                cells,
                lax.ppermute(head, axis, [((i + 1) % count, i) for i in range(ends)]),
            ],
            axis=dim,
        )
    return cells


def interface_setup(corner_aa, corner_ab, corner_ba, corner_bb, couplings):
    determinant = corner_aa * corner_bb - corner_ab * corner_ba
    corner_inverse = (
        jnp.stack(
            [jnp.stack([corner_bb, -corner_ab], -1), jnp.stack([-corner_ba, corner_aa], -1)], -2
        )
        / determinant[:, None, None]
    )
    blocks_count = corner_aa.shape[0]
    identity = jnp.eye(blocks_count, dtype=corner_inverse.dtype)
    diagonal_part = jnp.einsum("kab,kl->kalb", corner_inverse, identity, precision=highest).reshape(
        2 * blocks_count, 2 * blocks_count
    )
    link_values = jnp.zeros((2 * blocks_count - 1,), corner_inverse.dtype).at[1::2].set(-couplings)
    schur_matrix = diagonal_part + jnp.diag(link_values, 1) + jnp.diag(link_values, -1)
    return (corner_inverse, diagonal_part, jnp.linalg.cholesky(schur_matrix))


def make_solver(inverse_block, corner_rows, couplings, device_index, down_coupling, up_coupling):
    corner_inverse, diagonal_part, factor = interface_setup(
        corner_rows[:, 0], corner_rows[:, 1], corner_rows[:, 2], corner_rows[:, 3], couplings
    )
    block_len = inverse_block.shape[0]
    forward = lax.linalg.triangular_solve(factor, diagonal_part, left_side=True, lower=True)
    reach = lax.linalg.triangular_solve(
        factor, forward, left_side=True, lower=True, transpose_a=True
    )
    padded_reach = jnp.pad(reach, ((1, 1), (0, 0)))
    slice_rows = lax.dynamic_slice_in_dim(padded_reach, 2 * device_index, 4, 0)
    needed = jnp.stack([slice_rows[0], slice_rows[3]])

    def neighbours(end_values):
        zero_carry = jnp.zeros(end_values.shape, jnp.float32)
        nearby = zero_carry + jnp.dot(
            needed, lax.all_gather(end_values, "gz", axis=0, tiled=True), precision=highest
        )
        return (nearby[0], nearby[1])

    def solve(source):
        first_extent, second_extent, depth = source.shape
        line_count = first_extent * second_extent
        local_part = jnp.einsum("xyj,ij->xyi", source, inverse_block, precision=highest)
        end_values = jnp.stack(
            [
                local_part[:, :, 0].reshape(line_count),
                local_part[:, :, block_len - 1].reshape(line_count),
            ]
        )
        below_last, above_first = neighbours(end_values)
        return (
            local_part
            + (down_coupling * below_last).reshape(first_extent, second_extent, 1)
            * inverse_block[:, 0]
            + (up_coupling * above_first).reshape(first_extent, second_extent, 1)
            * inverse_block[:, block_len - 1]
        )

    return solve


def apply_operator(iterate, lateral_weight, down_faces, up_faces):
    padded = extended(iterate, (("gx", 0), ("gy", 1), ("gz", 2)), 1)
    lateral = (
        padded[:-2, 1:-1, 1:-1]
        + padded[2:, 1:-1, 1:-1]
        + padded[1:-1, :-2, 1:-1]
        + padded[1:-1, 2:, 1:-1]
    )
    return (
        lateral_weight * (4.0 * iterate - lateral)
        + down_faces * (iterate - padded[1:-1, 1:-1, :-2])
        + up_faces * (iterate - padded[1:-1, 1:-1, 2:])
    )


def restrict(field):
    first_extent, second_extent, depth = field.shape
    return field.reshape(first_extent // 2, 2, second_extent // 2, 2, depth).sum(axis=(1, 3)) * 0.25


def prolong(padded):
    first_extent = padded.shape[0] - 2
    second_extent = padded.shape[1] - 2
    depth = padded.shape[2]
    even_rows = 0.75 * padded[1:-1] + 0.25 * padded[:-2]
    odd_rows = 0.75 * padded[1:-1] + 0.25 * padded[2:]
    widened = jnp.stack([even_rows, odd_rows], 1).reshape(
        2 * first_extent, second_extent + 2, depth
    )
    even_rows = 0.75 * widened[:, 1:-1] + 0.25 * widened[:, :-2]
    odd_rows = 0.75 * widened[:, 1:-1] + 0.25 * widened[:, 2:]
    return jnp.stack([even_rows, odd_rows], 2).reshape(2 * first_extent, 2 * second_extent, depth)


def body(right_side, z_faces, xy_coupling, block_inverse):
    device_index = lax.axis_index("gz")
    levels_count = block_inverse.shape[0]
    last_cell = block_inverse.shape[1] - 1
    corner = jnp.stack(
        [
            block_inverse[:, 0, 0],
            block_inverse[:, 0, last_cell],
            block_inverse[:, last_cell, 0],
            block_inverse[:, last_cell, last_cell],
        ],
        -1,
    )[None]
    corners, firsts = (
        lax.all_gather(corner, "gz", axis=0, tiled=True),
        lax.all_gather(z_faces[:1], "gz", axis=0, tiled=True),
    )
    couplings = firsts[1:]
    edge_faces = jnp.concatenate([firsts, jnp.ones((1,), jnp.float32)])
    top_face = lax.dynamic_slice_in_dim(edge_faces, device_index + 1, 1, 0)
    up_faces = jnp.concatenate([z_faces[1:], top_face])
    solvers = [
        make_solver(
            block_inverse[level],
            corners[:, level],
            couplings,
            device_index,
            z_faces[0],
            top_face[0],
        )
        for level in range(levels_count)
    ]

    def operator(iterate, level):
        return apply_operator(iterate, xy_coupling[level], z_faces, up_faces)

    def multigrid_cycle(source, level):
        iterate = damping * solvers[level](source)
        iterate = iterate + damping * solvers[level](source - operator(iterate, level))
        if level == LEVELS - 1:
            return iterate
        coarse = multigrid_cycle(restrict(source - operator(iterate, level)), level + 1)
        widened = extended(coarse, (("gx", 0), ("gy", 1)), 1)
        iterate = iterate + prolong(widened)
        for sweep in range(SWEEPS):
            iterate = iterate + damping * solvers[level](source - operator(iterate, level))
        return iterate

    solution = multigrid_cycle(right_side, 0)
    return (solution, right_side - operator(solution, 0))


MESH = pl.DeviceIdType.MESH
HALOS = (4, 6, 6)
ROWS = (4, 5, 6)
YPAD = 8
SPARE = 32
DEEPEST = 3
NEAR = 2


def block_range(offset, own, halo, extent):
    start = offset * own - halo
    low = max(0, start)
    high = min(extent, (offset + 1) * own + halo)
    return low, high - low, low - start


def round_up(value, unit):
    return -(-value // unit) * unit


def difference(outer, inner):
    (a, b), (c, d) = outer
    (e, f), (g, h) = inner
    if e >= f or g >= h:
        return [outer]
    parts = [((a, e), (c, d)), ((f, b), (c, d)), ((e, f), (c, g)), ((e, f), (h, d))]
    return [(x, y) for x, y in parts if x[0] < x[1] and y[0] < y[1]]


def needed(t, dy, own, size, halos):
    (n0, n1), (s0, s1), (left, right, side) = own, size, halos
    x = max(0, t * n0 - left), min(s0, (t + 1) * n0 + right)
    y = max(0, dy * n1 - side), min(s1, (dy + 1) * n1 + side)
    return x, y


def vacant(part):
    return any(low >= high for low, high in part)


def both_parts(t, dy, own, size, near, far):
    whole = needed(t, dy, own, size, far)
    inner = needed(t, dy, own, size, near) if near else ((0, 0), (0, 0))
    common = tuple((max(a, c), min(b, d)) for (a, b), (c, d) in zip(whole, inner))
    outer = [] if vacant(whole) else difference(whole, common)
    return [] if vacant(inner) else [inner], outer


def area(parts):
    return sum((x[1] - x[0]) * (y[1] - y[0]) for x, y in parts)


def split_planes(count, rows):
    return max(c for c in range(1, count + 1) if count % c == 0 and c * rows <= 448)


def cycle_kernel(geometry, f_hbm, z_hbm, e_hbm, g_hbm, sol_ref, res_ref, *scratch):
    gx_n, gy_n, gz_n, nx, ny, depth, levels = geometry
    refs = iter(scratch)
    take = lambda count: [next(refs) for _ in range(count)]
    sinv, g_all, z_all, gather, f_v, e_ref = take(6)
    X = [take(3) for _ in range(DEEPEST + 1)]
    X.append(take(1))
    C = take(DEEPEST + 1)
    E = take(DEEPEST + 1)
    (U1, G1, U2, G2, c3u, c3g, c4u, c4g, cwu, cwg) = take(10)
    UP, GP = [None, U1, U2, c3u, c4u], [None, G1, G2, c3g, c4g]
    own3, pool = take(2)
    T = take(DEEPEST + 1)
    N = take(DEEPEST)
    (in_sem, g_send, g_recv, h_send, h_recv, y_recv, p_sem) = take(7)
    r_send, r_recv = take(2)
    y_send, x_send, x_recv, o_send, o_recv = [p_sem.at[i] for i in range(5)]

    ix, iy, iz = lax.axis_index("gx"), lax.axis_index("gy"), lax.axis_index("gz")
    bx = ix * gz_n + iz
    bx_n = gx_n * gz_n
    f32 = jnp.float32

    whole = gz_n * depth
    keep = 1.0 - damping

    def owned(level):
        return nx >> level, ny >> level

    def copy(src, dst, send, recv, device):
        return pltpu.make_async_remote_copy(
            src_ref=src,
            dst_ref=dst,
            send_sem=send,
            recv_sem=recv,
            device_id=device,
            device_id_type=MESH,
        )

    def inside(x, y):
        return (x >= 0) & (x < gx_n) & (y >= 0) & (y < gy_n)

    parts = 8
    span = f_v.shape[0] // parts
    for i in range(parts):
        at = pl.ds(i * span, span)
        pltpu.make_async_copy(f_hbm.at[at], f_v.at[at], in_sem.at[0]).start()
    f_load = pltpu.make_async_copy(f_hbm, f_v, in_sem.at[0])
    rest = pl.ds(1, levels - 1)
    loads = [
        pltpu.make_async_copy(z_hbm, z_all.at[iz], in_sem.at[1]),
        pltpu.make_async_copy(g_hbm.at[0], g_all.at[0, iz], in_sem.at[2]),
        pltpu.make_async_copy(g_hbm.at[rest], g_all.at[rest, iz], in_sem.at[3]),
        pltpu.make_async_copy(e_hbm, e_ref, in_sem.at[4]),
    ]
    reach_all = max(
        gz_n - 1 - (-HALOS[0] // nx), *[-(-HALOS[k] // owned(k)[0]) for k in (1, 2)]
    )
    barrier = pltpu.get_barrier_semaphore()
    partners = jnp.int32(0)
    for dx in range(1 - bx_n, bx_n):
        for dy in range(1 - gy_n, gy_n):
            close = abs(dx) <= reach_all and abs(dy) <= 1
            if (dx == 0 and dy == 0) or not close:
                continue
            x, y = bx + dx, iy + dy
            ok = (x >= 0) & (x < bx_n) & (y >= 0) & (y < gy_n)

            @pl.when(ok)
            def _():
                pl.semaphore_signal(
                    barrier,
                    inc=1,
                    device_id=(x // gz_n, y, lax.rem(x, gz_n)),
                    device_id_type=MESH,
                )

            partners = partners + jnp.where(ok, 1, 0).astype(jnp.int32)

    def setup_copies(other):
        here = (ix, iy, lax.rem(iz + other, gz_n))
        out = []
        for i, block in enumerate((z_all.at[iz], g_all.at[0, iz], g_all.at[rest, iz])):
            out.append(copy(block, block, g_send.at[other, i], g_recv.at[other, i], here))
        return out

    def runs(count, key):
        out = []
        for i in range(count):
            if out and key(i) == out[-1][2]:
                out[-1][1] = i
            else:
                out.append([i, i, key(i)])
        return [(low, high) for low, high, _ in out]

    def take_rows(sem, rows):
        block = pool.at[pl.ds(0, rows)]
        pltpu.make_async_copy(block, block, sem).wait()

    def settle(sem, total):
        table = [[total(b, y) for y in range(gy_n)] for b in range(bx_n)]
        for low, high in runs(bx_n, lambda b: table[b]):
            for first, last in runs(gy_n, lambda y: [row[y] for row in table]):

                @pl.when((bx >= low) & (bx <= high) & (iy >= first) & (iy <= last))
                def _():
                    take_rows(sem, table[low][first])

    near0, far0 = N[0], X[0][0]
    plan0 = []
    reach = -(-ROWS[0] // nx)
    for t in range(-reach, gz_n + reach):
        for dy in (-1, 0, 1):
            near_halo, far_halo = (NEAR,) * 3, (ROWS[0],) * 3
            parts0 = both_parts(t, dy, (nx, ny), (nx * gz_n, ny), near_halo, far_halo)
            plan0.append((t, t // gz_n, t % gz_n, dy, parts0))
    plan0.sort(key=lambda entry: -abs(entry[1]) - abs(entry[3]))

    def target0(window, part, t, dy, source_z):
        (x0, x1), (y0, y1) = part
        p, r = x0 - t * nx + HALOS[0], y0 - dy * ny + YPAD
        return window.at[pl.ds(p, x1 - x0), source_z, pl.ds(r, y1 - y0), :]

    local0 = []
    for t, dgx, target, dy, parts0 in plan0:
        if dgx == 0 and dy == 0:
            for which, window in enumerate((near0, far0)):
                for part in parts0[which]:
                    (x0, x1), (y0, y1) = part
                    move = pltpu.make_async_copy(
                        f_hbm.at[pl.ds(x0, x1 - x0), pl.ds(y0, y1 - y0), :],
                        target0(window, part, t, dy, target),
                        in_sem.at[5 + which],
                    )
                    local0.append((target, which, move))

    for target, _, move in local0:

        @pl.when(iz == target)
        def _():
            move.start()

    def local_done(which):
        for target, other, move in local0:
            if other == which:

                @pl.when(iz == target)
                def _():
                    move.wait()

    def send0(which):
        for t, dgx, target, dy, parts0 in plan0:
            ok = inside(ix + dgx, iy + dy)
            if dgx == 0 and dy == 0:
                ok = ok & (iz != target)

            @pl.when(ok)
            def _():
                for part in parts0[which]:
                    (x0, x1), (y0, y1) = part
                    copy(
                        f_v.at[pl.ds(x0, x1 - x0), pl.ds(y0, y1 - y0), :],
                        target0((near0, far0)[which], part, t, dy, iz),
                        h_send.at[0],
                        h_recv.at[0, which],
                        (ix + dgx, iy + dy, target),
                    ).start()

    def in_grid(b, y):
        return 0 <= b < bx_n and 0 <= y < gy_n

    def sent0(b, y):
        total = 0
        for t, dgx, target, dy, parts0 in plan0:
            there = (b // gz_n + dgx) * gz_n + target
            if in_grid(there, y + dy) and (there, dy) != (b, 0):
                total += area(parts0[0]) + area(parts0[1])
        return total

    def received0(which):
        def count(b, y):
            total = 0
            for t, dgx, target, dy, parts0 in plan0:
                for source_z in range(gz_n):
                    there = (b // gz_n - dgx) * gz_n + source_z
                    ok = target == b % gz_n and in_grid(there, y - dy)
                    if ok and (there, dy) != (b, 0):
                        total += area(parts0[which])
            return total

        return count

    def clear_edges():
        for level, window in [(k, w) for k in range(DEEPEST) for w in (N[k], X[k][0])]:
            planes, zb, rows, lanes = window.shape
            halo = HALOS[level]
            n0, n1 = owned(level)
            reach = -(-halo // n0)
            for t in range(1, reach + 1):
                low = max(0, halo - t * n0)
                high = halo - (t - 1) * n0
                plane = jnp.zeros((high - low, zb, n1 + 2 * YPAD, lanes), f32)

                @pl.when(bx - t < 0)
                def _():
                    window[low:high, :, pl.ds(0, n1 + 2 * YPAD)] = plane

                low2, high2 = planes - high, planes - low

                @pl.when(bx + t >= bx_n)
                def _():
                    window[low2:high2, :, pl.ds(0, n1 + 2 * YPAD)] = plane

            edge = jnp.zeros((zb, YPAD, lanes), f32)

            @pl.when(iy == 0)
            def _():
                lax.fori_loop(0, planes, lambda i, c: zero_rows(window, i, 0, edge), 0)

            @pl.when(iy == gy_n - 1)
            def _():
                lax.fori_loop(
                    0, planes, lambda i, c: zero_rows(window, i, YPAD + n1, edge), 0
                )

    def fill_border(ref, side):
        planes, zb, rows, lanes = ref.shape
        plane = jnp.zeros((side, zb, rows, lanes), f32)
        edge = jnp.zeros((zb, YPAD, lanes), f32)
        ref[0:side] = plane
        ref[planes - side : planes] = plane

        def step(i, _):
            ref[i, :, pl.ds(0, YPAD)] = edge
            ref[i, :, pl.ds(rows - YPAD, YPAD)] = edge
            return 0

        lax.fori_loop(side, planes - side, step, 0, unroll=4)

    def clear_coarse():
        side = HALOS[2] // 2 + 1
        for ref in (X[3][0], X[3][2], T[3], C[3], X[4][0], c4u, c4g):
            fill_border(ref, 1)
        for ref in (c3u, c3g):
            fill_border(ref, side)

    def assemble(level, _):
        merged = g_all[level, 0]
        for k in range(1, gz_n):
            block = g_all[level, k]
            size, cz = merged.shape[0], block.shape[0]
            face = z_all[k][:, 0:1]
            a, d = block[0:1, 0:1], merged[size - 1 : size, size - 1 : size]
            last, first = merged[size - 1 : size], block[0:1]
            scale = face / (1.0 - face * face * a * d)
            p_row = jnp.concatenate([face * a * last, first], 1) * scale
            q_row = jnp.concatenate([last, face * d * first], 1) * scale
            top = jnp.concatenate([merged, jnp.zeros((size, cz), f32)], 1)
            low = jnp.concatenate([jnp.zeros((cz, size), f32), block], 1)
            top = top + merged[:, size - 1 : size] * p_row
            low = low + block[:, 0:1] * q_row
            merged = jnp.concatenate([top, low], 0)
        solve = (damping * merged).astype(jnp.bfloat16)
        sinv[level, pl.ds(0, whole), :] = solve
        twice = jnp.dot(solve, solve, preferred_element_type=f32)
        sinv[level, pl.ds(whole, whole), :] = twice.astype(jnp.bfloat16)
        return 0

    def plane_mask(level, i):
        n0 = owned(level)[0]
        x = bx * n0 - HALOS[level] + i
        return jnp.where((x >= 0) & (x < bx_n * n0), 1.0, 0.0).astype(f32)

    def masked(level, p, value):
        if 0 <= p - HALOS[level] < owned(level)[0]:
            return value
        return value * plane_mask(level, p)

    def row_mask(level, first, rows, stride):
        n1 = owned(level)[1]
        y = lax.broadcasted_iota(jnp.int32, (rows, depth), 0) * stride + first
        y = y + iy * n1 - YPAD
        return jnp.where((y >= 0) & (y < gy_n * n1), 1.0, 0.0).astype(f32)

    def region(level, shrink=0):
        if level < DEEPEST:
            return nearby(level, ROWS[level] - shrink)
        window = X[level][0].shape
        return 1, window[0] - 2, YPAD, window[2] - 2 * YPAD

    def nearby(level, h, extra=0):
        n0, n1 = owned(level)
        first = HALOS[level] - h - extra
        return first, n0 + 2 * h + extra, YPAD - h, round_up(n1 + 2 * h, 8)

    def weights(level, p, c, r0, rows):
        e = e_ref[level]
        if level >= DEEPEST:
            return e
        mask = row_mask(level, r0, rows, 1) * e
        return jnp.stack([masked(level, p + i, mask) for i in range(c)])

    def chunks(where):
        p0, planes, r0, rows = where
        c = split_planes(planes, rows)
        return [(p0 + s * c, c, r0, rows) for s in range(planes // c)]

    def around(src, k, p, c, r0, rows):
        at = lambda dp, dr: src[pl.ds(p + dp, c), k, pl.ds(r0 + dr, rows)]
        return (at(-1, 0) + at(1, 0)) + (at(0, -1) + at(0, 1))

    def product(level, first, *groups):
        flat = [v.reshape(-1, depth) for fields in groups for v in fields]
        lhs = jnp.concatenate(flat, 1).astype(jnp.bfloat16)
        rhs = sinv[level, pl.ds(first * whole, len(groups) * whole), :]
        out = jnp.dot(lhs, rhs, preferred_element_type=f32)
        shape = groups[0][0].shape
        return [out[:, k * depth : (k + 1) * depth].reshape(shape) for k in range(gz_n)]

    def relax(level, src, dst, where):
        for p, c, r0, rows in chunks(where):
            w = weights(level, p, c, r0, rows)
            total = [around(src, k, p, c, r0, rows) * w for k in range(gz_n)]
            out = product(level, 0, total)
            for k in range(gz_n):
                value = keep * src[pl.ds(p, c), k, pl.ds(r0, rows)] + out[k]
                dst[pl.ds(p, c), k, pl.ds(r0, rows)] = value

    def spread(level, src, where):
        for p, c, r0, rows in chunks(where):
            w = weights(level, p, c, r0, rows)
            for k in range(gz_n):
                T[level][pl.ds(p, c), k, pl.ds(r0, rows)] = around(src, k, p, c, r0, rows) * w

    def relax_twice(level, src, where, once, put):
        for p, c, r0, rows in chunks(where):
            w = weights(level, p, c, r0, rows)
            at = lambda ref, k: ref[pl.ds(p, c), k, pl.ds(r0, rows)]
            one = [at(T[level], k) for k in range(gz_n)]
            two = [around(T[level], k, p, c, r0, rows) * w for k in range(gz_n)]
            if once is None:
                out = product(level, 0, [2.0 * keep * v for v in one], two)
            else:
                first, second = product(level, 0, one), product(level, 1, two)
                out = [second[k] + 2.0 * keep * first[k] for k in range(gz_n)]
            for k in range(gz_n):
                value = at(src, k)
                if once is not None:
                    once[pl.ds(p, c), k, pl.ds(r0, rows)] = keep * value + first[k]
                put(k, p, c, r0, rows, keep * keep * value + out[k])

    def into(ref):
        def put(k, p, c, r0, rows, value):
            ref[pl.ds(p, c), k, pl.ds(r0, rows)] = value

        return put

    def sums(level, p, c, r0, rows):
        at = lambda ref, k: ref[pl.ds(p, c), k, pl.ds(r0, rows)]
        last = X[level][-1]
        total = []
        for k in range(gz_n):
            value = (1.0 + keep) * at(last, k)
            if level <= DEEPEST:
                value = value + (at(X[level][0], k) + at(X[level][1], k))
            total.append(value)
        return total

    def finish(level, where, offset=0):
        last = X[level][-1]
        for p, c, r0, rows in chunks(where):
            w = weights(level, p, c, r0, rows)
            at = lambda ref, k: ref[pl.ds(p, c), k, pl.ds(r0, rows)]
            total = sums(level, p, c, r0, rows)
            side = [around(last, k, p, c, r0, rows) * w for k in range(gz_n)]
            rest = product(level, 0, side)
            u = product(level, 0, total, side)
            for k in range(gz_n):
                if level <= DEEPEST:
                    u[k] = u[k] + at(C[level], k)
                g = damping * (total[k] + rest[k])
                g = g + (4.0 * (e_ref[level - 1] - e_ref[level])) * u[k]
                if level <= DEEPEST:
                    g = g + at(E[level], k)
                UP[level][pl.ds(p + offset, c), k, pl.ds(r0, rows)] = u[k]
                GP[level][pl.ds(p + offset, c), k, pl.ds(r0, rows)] = g

    def finest(where, place):
        for p, c, r0, rows in chunks(where):
            at = lambda ref, k: ref[pl.ds(p, c), k, pl.ds(r0, rows)]
            total = sums(0, p, c, r0, rows)
            u = product(0, 0, total, [at(T[0], k) for k in range(gz_n)])
            for k in range(gz_n):
                sol_ref[k, pl.ds(place + p - where[0], c)] = u[k] + at(C[0], k)

    def restrict_planes(level, dst, planes, x0, y0, to_plane, to_row, rows):
        src = X[level][2]
        for j in range(planes):
            for k in range(gz_n):
                total = None
                for a in (0, 1):
                    for b in (0, 1):
                        part = src[x0 + 2 * j + a, k, pl.ds(y0 + b, rows, 2), :]
                        total = part if total is None else total + part
                dst[to_plane + j, k, pl.ds(to_row, rows), :] = total * 0.25

    def prolong(level, x0, y0, coarse):
        shift = 1 if level >= DEEPEST else 0
        p0, planes, r0, rows = region(level, 1)
        low, high = p0 - shift, p0 - shift + planes
        first = r0 // 2 * 2
        half = round_up((r0 + rows - first + 1) // 2, 8) if level < DEEPEST else rows // 2
        start = y0 + (first // 2 if level < DEEPEST else 0)
        masks = [
            row_mask(level, first + b, half, 2) if level < DEEPEST else None for b in (0, 1)
        ]
        def mixed(src, j, k):
            load = lambda dy: src[x0 + j, k, pl.ds(start + dy, half), :]
            quarter = 0.25 * load(0)
            near = load(0) - quarter
            out = []
            for dy in (-1, 1):
                value = near + 0.25 * load(dy)
                far = 0.25 * value
                out.append((value - far, far))
            return out

        first_j, last_j = low // 2, (high - 1) // 2
        for src, dst in coarse:
            for k in range(gz_n):
                behind, here = mixed(src, first_j - 1, k), mixed(src, first_j, k)
                for j in range(first_j, last_j + 1):
                    ahead = mixed(src, j + 1, k)
                    for a, beside in ((0, behind), (1, ahead)):
                        p = 2 * j + a
                        if not low <= p < high:
                            continue
                        for b in (0, 1):
                            value = here[b][0] + beside[b][1]
                            if level < DEEPEST:
                                value = masked(level, p, value * masks[b])
                            dst[p + shift, k, pl.ds(first + b, half, 2), :] = value
                    behind, here = here, ahead

    def correct(level, coarse_u, coarse_g, x0, y0):
        prolong(level, x0, y0, [(coarse_u, C[level]), (coarse_g, E[level])])
        where = region(level, 2)
        target = X[level][2]
        for p, c, r0, rows in chunks(where):
            w = weights(level, p, c, r0, rows)
            for k in range(gz_n):
                at = lambda ref: ref[pl.ds(p, c), k, pl.ds(r0, rows)]
                total = around(C[level], k, p, c, r0, rows) * w
                target[pl.ds(p, c), k, pl.ds(r0, rows)] = at(target) + (total - at(E[level]))

    def near_halos(level, core):
        if level < DEEPEST - 1:
            return (NEAR,) * 3
        if core < gz_n - 1:
            return None
        return NEAR + owned(level)[0] * core, NEAR, NEAR

    def far_halos(level, core):
        width = ROWS[level]
        return (0 if core else width), (width if core else 0), width

    def relay(level):
        n0, n1 = owned(level)
        width, halo = ROWS[level], HALOS[level]
        rows = pl.ds(YPAD - width, n1 + 2 * width)
        window = X[level][0]
        def move(core):
            src, dst = ((halo + n0 - width, halo - width), (halo, halo + n0))[core]
            return copy(
                window.at[pl.ds(src, width), :, rows, :],
                window.at[pl.ds(dst, width), :, rows, :],
                r_send.at[level - 1],
                r_recv.at[level - 1],
                (ix, iy, 1 - core),
            )

        return move

    def exchange(level):
        n0, n1 = owned(level)
        width = ROWS[level]
        halo = HALOS[level]
        reach = -(-width // n0)
        pieces = []
        for t in range(-reach, reach + 1):
            for dy in (-1, 0, 1):
                if t or dy:
                    parts = [
                        both_parts(
                            t,
                            dy,
                            (n0, n1),
                            (n0, n1),
                            near_halos(level, core),
                            far_halos(level, core),
                        )
                        for core in range(gz_n)
                    ]
                    pieces.append((t, dy, parts))
        pieces.sort(key=lambda piece: -abs(piece[0]) - abs(piece[1]))

        def start(which):
            window = (N[level], X[level][0])[which]
            for t, dy, parts in pieces:
                there = bx + t + bx_n
                core = lax.rem(there, gz_n)
                x, y = bx + t, iy + dy
                alike = all(part == parts[0] for part in parts)
                for target in range(1 if alike else gz_n):
                    ok = (x >= 0) & (x < bx_n) & (y >= 0) & (y < gy_n)
                    if not alike:
                        ok = ok & (core == target)
                    if not parts[target][which]:
                        continue

                    @pl.when(ok)
                    def _():
                        for (x0, x1), (y0, y1) in parts[target][which]:
                            p, r = x0 - t * n0 + halo, y0 - dy * n1 + YPAD
                            copy(
                                N[level].at[
                                    pl.ds(halo + x0, x1 - x0),
                                    :,
                                    pl.ds(YPAD + y0, y1 - y0),
                                    :,
                                ],
                                window.at[pl.ds(p, x1 - x0), :, pl.ds(r, y1 - y0), :],
                                h_send.at[level],
                                h_recv.at[level, which],
                                (there // gz_n - gx_n, y, core),
                            ).start()

        def total(sign, wanted):
            def count(b, y):
                rows = 0
                for t, dy, parts in pieces:
                    if in_grid(b + sign * t, y + sign * dy):
                        core = (b + t) % gz_n if sign > 0 else b % gz_n
                        rows += sum(gz_n * area(parts[core][which]) for which in wanted)
                return rows

            return count

        arrive = lambda which: settle(h_recv.at[level, which], total(-1, (which,)))
        return start, arrive, lambda: settle(h_send.at[level], total(1, (0, 1)))

    def gather_halo(level, arrive):
        n0, n1 = owned(level)
        for core in range(gz_n):
            near = near_halos(level, core) or (0, 0, 0)
            far = far_halos(level, core) if level else near
            left, right, side = (min(a, b) for a, b in zip(near, far))
            rows = pl.ds(YPAD - side, n1 + 2 * side)

            @pl.when(iz == core)
            def _():
                for p in range(HALOS[level] - left, HALOS[level] + n0 + right):
                    X[level][0][p, :, rows] = N[level][p, :, rows]

        arrive(1)
        if level:
            for core in range(gz_n):

                @pl.when(iz == core)
                def _():
                    relay(level)(core).start()

    def presmooth(level):
        if level:
            relay(level)(0).wait_recv()
        relax(level, X[level][0], X[level][1], region(level, 1))
        relax(level, X[level][1], X[level][2], region(level, 2))

    def gather_all(early, late):
        leader = gz_n - 1
        leading = iz == leader

        def line_y(other, slot):
            return copy(own3, gather.at[ix, slot], y_send, y_recv.at[slot], (ix, other, leader))

        def share(src, slot):
            for core in range(gz_n):
                for s in range(1, gx_n):
                    other = (lax.rem(ix + s, gx_n), iy, core)
                    copy(src, gather.at[ix, slot], x_send, x_recv, other).start()
            for core in range(leader):
                copy(src, gather.at[ix, slot], x_send, x_recv, (ix, iy, core)).start()

        @pl.when(leading)
        def _():
            for s in range(1, gy_n):
                line_y(lax.rem(iy + s, gy_n), iy).start()
            share(own3, iy)
            gather[ix, iy] = own3[...]

        early()

        @pl.when(leading)
        def _():
            for distance in range(1, gy_n):
                for y in (iy + distance, iy - distance):

                    @pl.when((y >= 0) & (y < gy_n))
                    def _():
                        line_y(y, y).wait_recv()
                        share(gather.at[ix, y], y)

        late()
        size = own3.shape[0] * own3.shape[1] * own3.shape[2]

        @pl.when(leading)
        def _():
            take_rows(x_recv, (gx_n - 1) * gy_n * size)

        @pl.when(iz < leader)
        def _():
            take_rows(x_recv, gx_n * gy_n * size)

        n0, n1 = owned(3)
        window = X[3][0]

        def place(b, _):
            for i in range(gz_n * n0):
                for y in range(gy_n):
                    at = 1 + b * gz_n * n0 + i
                    window[at, :, pl.ds(YPAD + y * n1, n1), :] = gather[b, y, i]
            return 0

        lax.fori_loop(0, gx_n, place, 0)

        def drains():
            @pl.when(leading)
            def _():
                take_rows(y_send, (gy_n - 1) * size)
                for _ in range(gy_n):
                    take_rows(x_send, (gx_n * gz_n - 1) * size)

        return drains

    for c in loads:
        c.start()
    f_load.wait()
    pl.semaphore_wait(barrier, partners)
    send0(0)
    for c in loads:
        c.wait()
    setups = [setup_copies(other) for other in range(1, gz_n)]
    for group in setups:
        for c in group[:2]:
            c.start()
    clear_edges()
    for group in setups:
        for c in group[:2]:
            c.wait()
    assemble(0, 0)
    send0(1)
    for group in setups:
        group[2].start()
    local_done(0)

    def arrive0(which):
        if which:
            local_done(1)
        settle(h_recv.at[0, which], received0(which))

    def later():
        for group in setups:
            group[2].wait()
        assemble(1, 0)

    arrive = arrive0
    drains = [lambda: settle(h_send.at[0], sent0)]
    for level in range(DEEPEST):
        arrive(0)
        extra = owned(level)[0] * (gz_n - 1) if level == DEEPEST - 1 else 0
        spread(level, N[level], nearby(level, 1, extra))
        relax_twice(level, N[level], nearby(level, 0, extra), None, into(X[level][2]))
        n0, n1 = owned(level + 1)
        p, r = HALOS[level], YPAD
        if level < DEEPEST - 1:
            restrict_planes(level, N[level + 1], n0, p, r, HALOS[level + 1], YPAD, n1)
            start, following, drain = exchange(level + 1)
            drains.append(drain)
            start(0)
            if level == 0:
                later()
                gather_halo(level, arrive)
                presmooth(level)
                start(1)
            else:
                lax.fori_loop(2, levels, assemble, 0)
                clear_coarse()
                start(1)

                @pl.when(iz < gz_n - 1)
                def _():
                    gather_halo(level, arrive)

                before = arrive
            arrive = following
        else:
            restrict_planes(level, own3, gz_n * n0, p - extra, r, 0, 0, n1)

            def early():
                @pl.when(iz == gz_n - 1)
                def _():
                    gather_halo(level - 1, before)

                presmooth(level - 1)

            def late():
                gather_halo(level, arrive)
                presmooth(level)

            drains.append(gather_all(early, late))

    whole3, whole4 = region(3, 0), region(4, 0)
    spread(3, X[3][0], whole3)
    relax_twice(3, X[3][0], whole3, X[3][1], into(X[3][2]))
    restrict_planes(3, X[4][0], whole4[1], 1, YPAD, 1, YPAD, whole4[3])
    finish(4, whole4)
    correct(3, c4u, c4g, 1, YPAD)
    pad3 = HALOS[2] // 2 + 1
    finish(3, whole3, offset=pad3 - 1)
    n0, n1 = owned(3)
    margin = YPAD // 2
    for y in range(gy_n):

        @pl.when(iy == y)
        def _():
            for j in range(HALOS[2] + 2 * n0):
                for src, dst in ((c3u, cwu), (c3g, cwg)):
                    dst[j, :, pl.ds(margin, n1 + 4 * margin), :] = src[
                        bx * n0 + j, :, pl.ds(y * n1, n1 + 4 * margin), :
                    ]

    for level in (2, 1, 0):
        if level == 2:
            correct(2, cwu, cwg, 1, YPAD)
        else:
            x0 = HALOS[level + 1] - HALOS[level] // 2
            correct(level, UP[level + 1], GP[level + 1], x0, YPAD // 2)
        if level:
            finish(level, region(level, 3))
        else:
            spread(0, X[0][2], region(0, 3))

    def send_out(ref, p, c):
        for other in range(1, gz_n):
            there = lax.rem(iz + other, gz_n)
            block = ref.at[there, pl.ds(iz * nx + p, c)]
            copy(block, block, o_send, o_recv, (ix, iy, there)).start()

    own0 = nearby(0, 0)
    finest(own0, iz * nx)
    send_out(sol_ref, 0, nx)

    def store(k, p, c, r0, rows, value):
        res_ref[k, pl.ds(iz * nx + p - own0[0], c)] = value

    relax_twice(0, X[0][2], own0, None, store)
    send_out(res_ref, 0, nx)
    for drain in drains:
        drain()
    for level in range(1, DEEPEST):
        relay(level)(0).wait_send()
    for sem in (o_send, o_recv):
        take_rows(sem, (gz_n - 1) * 2 * nx * ny)


def zero_rows(ref, i, at, value):
    ref[i, :, pl.ds(at, YPAD), :] = value
    return 0


def store_kernel(pieces, sol_v, res_v, sol_hbm, res_hbm, sem):
    iz = lax.axis_index("gz")
    span = sol_hbm.shape[0] // pieces
    moves = []
    for which, (src, dst) in enumerate(((sol_v, sol_hbm), (res_v, res_hbm))):
        for i in range(pieces):
            at = pl.ds(i * span, span)
            moves.append(
                pltpu.make_async_copy(src.at[iz, at], dst.at[at], sem.at[which, i])
            )
    for move in moves:
        move.start()
    for move in moves:
        move.wait()


def fits(mesh, shape, inverse_shape):
    gx_n, gy_n, gz_n = (mesh.shape[a] for a in ("gx", "gy", "gz"))
    nx, ny = shape[0] // (gx_n * gz_n), shape[1] // gy_n
    return (
        inverse_shape[0] == LEVELS == 5
        and SWEEPS == 2
        and inverse_shape[2] == 128
        and nx % 8 == 0
        and ny % 32 == 0
        and (shape[1] >> 4) % 8 == 0
        and gz_n == 2 and gy_n <= 4
    )


def fused_body(mesh, right_side, z_faces, xy_coupling, block_inverse):
    gx_n, gy_n, gz_n = (mesh.shape[a] for a in ("gx", "gy", "gz"))
    levels, _, depth = block_inverse.shape
    nx, ny = right_side.shape[0] // gz_n, right_side.shape[1]
    windows = []
    for level in range(levels):
        if level < DEEPEST:
            size = ((nx >> level) + 2 * HALOS[level], (ny >> level) + SPARE)
        else:
            size = (
                ((nx * gx_n * gz_n) >> level) + 2,
                ((ny * gy_n) >> level) + 2 * YPAD,
            )
        windows.append((size[0], gz_n, size[1], depth))
    vmem = lambda shape: pltpu.VMEM(shape, jnp.float32)
    full3, full4 = windows[3], windows[4]
    pad3 = HALOS[2] // 2 + 1
    c4 = full4
    c3 = (full3[0] - 2 + 2 * pad3,) + full3[1:]
    cw = (windows[2][0] // 2 + 2, gz_n, (ny >> 3) + 28, depth)
    most = gz_n * (nx + 2 * HALOS[0] + 8) * (ny + 2 * YPAD)
    dma = pltpu.SemaphoreType.DMA
    chip3 = (gz_n * (nx >> 3), gz_n, ny >> 3, depth)
    scratch = (
        [
            pltpu.VMEM((levels, 2 * gz_n * depth, gz_n * depth), jnp.bfloat16),
            vmem((levels, gz_n, depth, depth)),
            vmem((gz_n, 1, depth)),
            vmem((gx_n, gy_n) + chip3),
            vmem(right_side.shape),
            pltpu.SMEM((levels,), jnp.float32),
        ]
        + [vmem(w) for w in windows[: DEEPEST + 1] for _ in range(3)]
        + [vmem(full4)]
        + [vmem(w) for w in windows[: DEEPEST + 1]] * 2
        + [vmem(windows[1])] * 2
        + [vmem(windows[2])] * 2
        + [vmem(c3), vmem(c3), vmem(c4), vmem(c4), vmem(cw), vmem(cw)]
        + [vmem(chip3), vmem((most, depth))]
        + [vmem(w) for w in windows[: DEEPEST + 1]]
        + [vmem(w) for w in windows[:DEEPEST]]
        + [dma((7,))]
        + [dma((gz_n, 3))] * 2
        + [dma((DEEPEST,)), dma((DEEPEST, 2))]
        + [dma((gy_n,)), dma((5,))]
        + [dma((DEEPEST - 1,))] * 2
    )
    in_vmem = pl.BlockSpec(memory_space=pltpu.VMEM)
    in_hbm = pl.BlockSpec(memory_space=pltpu.HBM)
    staged = (gz_n,) + right_side.shape
    hold = lambda x: pltpu.with_memory_space_constraint(x, pltpu.HBM)
    halves = pl.pallas_call(
        functools.partial(cycle_kernel, (gx_n, gy_n, gz_n, nx, ny, depth, levels)),
        out_shape=[pltpu.VMEM(staged, jnp.float32)] * 2,
        in_specs=[
            in_hbm,
            in_hbm,
            in_hbm,
            in_hbm,
        ],
        out_specs=[in_vmem, in_vmem],
        scratch_shapes=scratch,
        compiler_params=pltpu.CompilerParams(
            collective_id=0, has_side_effects=True, vmem_limit_bytes=48 * 1024 * 1024
        ),
    )(hold(right_side), hold(z_faces.reshape(1, -1)), hold(xy_coupling), hold(block_inverse))
    pieces = 2
    return tuple(
        pl.pallas_call(
            functools.partial(store_kernel, pieces),
            out_shape=[jax.ShapeDtypeStruct(right_side.shape, jnp.float32)] * 2,
            in_specs=[in_vmem, in_vmem],
            out_specs=[in_hbm, in_hbm],
            scratch_shapes=[dma((2, pieces))],
        )(*[pltpu.with_memory_space_constraint(x, pltpu.VMEM) for x in halves])
    )


def solution(mesh):
    def call(right_side, z_faces, xy_coupling, block_inverse):
        local = body
        if fits(mesh, right_side.shape, block_inverse.shape):
            local = functools.partial(fused_body, mesh)
        return jax.shard_map(
            local,
            mesh=mesh,
            in_specs=(P("gx", "gy", "gz"), P("gz"), P(), P(None, "gz", None)),
            out_specs=(P("gx", "gy", "gz"), P("gx", "gy", "gz")),
            check_vma=False,
        )(right_side, z_faces, xy_coupling, block_inverse)

    return call
```

```python
import functools

import jax
import jax.numpy as jnp
from jax import lax
from jax.experimental import pallas as pl
from jax.experimental.pallas import tpu as pltpu
from jax.sharding import PartitionSpec as P

LEVELS = 5
SWEEPS = 2


damping = 0.8
highest = lax.Precision.HIGHEST


def extended(cells, sides, width):
    for axis, dim in sides:
        count = lax.axis_size(axis)
        ends = count - 1
        head = lax.slice_in_dim(cells, 0, width, axis=dim)
        tail = lax.slice_in_dim(cells, cells.shape[dim] - width, cells.shape[dim], axis=dim)
        cells = jnp.concatenate(
            [
                lax.ppermute(tail, axis, [(i, (i + 1) % count) for i in range(ends)]),
                cells,
                lax.ppermute(head, axis, [((i + 1) % count, i) for i in range(ends)]),
            ],
            axis=dim,
        )
    return cells


def interface_setup(corner_aa, corner_ab, corner_ba, corner_bb, couplings):
    determinant = corner_aa * corner_bb - corner_ab * corner_ba
    corner_inverse = (
        jnp.stack(
            [jnp.stack([corner_bb, -corner_ab], -1), jnp.stack([-corner_ba, corner_aa], -1)], -2
        )
        / determinant[:, None, None]
    )
    blocks_count = corner_aa.shape[0]
    identity = jnp.eye(blocks_count, dtype=corner_inverse.dtype)
    diagonal_part = jnp.einsum("kab,kl->kalb", corner_inverse, identity, precision=highest).reshape(
        2 * blocks_count, 2 * blocks_count
    )
    link_values = jnp.zeros((2 * blocks_count - 1,), corner_inverse.dtype).at[1::2].set(-couplings)
    schur_matrix = diagonal_part + jnp.diag(link_values, 1) + jnp.diag(link_values, -1)
    return (corner_inverse, diagonal_part, jnp.linalg.cholesky(schur_matrix))


def make_solver(inverse_block, corner_rows, couplings, device_index, down_coupling, up_coupling):
    corner_inverse, diagonal_part, factor = interface_setup(
        corner_rows[:, 0], corner_rows[:, 1], corner_rows[:, 2], corner_rows[:, 3], couplings
    )
    block_len = inverse_block.shape[0]
    forward = lax.linalg.triangular_solve(factor, diagonal_part, left_side=True, lower=True)
    reach = lax.linalg.triangular_solve(
        factor, forward, left_side=True, lower=True, transpose_a=True
    )
    padded_reach = jnp.pad(reach, ((1, 1), (0, 0)))
    slice_rows = lax.dynamic_slice_in_dim(padded_reach, 2 * device_index, 4, 0)
    needed = jnp.stack([slice_rows[0], slice_rows[3]])

    def neighbours(end_values):
        zero_carry = jnp.zeros(end_values.shape, jnp.float32)
        nearby = zero_carry + jnp.dot(
            needed, lax.all_gather(end_values, "gz", axis=0, tiled=True), precision=highest
        )
        return (nearby[0], nearby[1])

    def solve(source):
        first_extent, second_extent, depth = source.shape
        line_count = first_extent * second_extent
        local_part = jnp.einsum("xyj,ij->xyi", source, inverse_block, precision=highest)
        end_values = jnp.stack(
            [
                local_part[:, :, 0].reshape(line_count),
                local_part[:, :, block_len - 1].reshape(line_count),
            ]
        )
        below_last, above_first = neighbours(end_values)
        return (
            local_part
            + (down_coupling * below_last).reshape(first_extent, second_extent, 1)
            * inverse_block[:, 0]
            + (up_coupling * above_first).reshape(first_extent, second_extent, 1)
            * inverse_block[:, block_len - 1]
        )

    return solve


def apply_operator(iterate, lateral_weight, down_faces, up_faces):
    padded = extended(iterate, (("gx", 0), ("gy", 1), ("gz", 2)), 1)
    lateral = (
        padded[:-2, 1:-1, 1:-1]
        + padded[2:, 1:-1, 1:-1]
        + padded[1:-1, :-2, 1:-1]
        + padded[1:-1, 2:, 1:-1]
    )
    return (
        lateral_weight * (4.0 * iterate - lateral)
        + down_faces * (iterate - padded[1:-1, 1:-1, :-2])
        + up_faces * (iterate - padded[1:-1, 1:-1, 2:])
    )


def restrict(field):
    first_extent, second_extent, depth = field.shape
    return field.reshape(first_extent // 2, 2, second_extent // 2, 2, depth).sum(axis=(1, 3)) * 0.25


def prolong(padded):
    first_extent = padded.shape[0] - 2
    second_extent = padded.shape[1] - 2
    depth = padded.shape[2]
    even_rows = 0.75 * padded[1:-1] + 0.25 * padded[:-2]
    odd_rows = 0.75 * padded[1:-1] + 0.25 * padded[2:]
    widened = jnp.stack([even_rows, odd_rows], 1).reshape(
        2 * first_extent, second_extent + 2, depth
    )
    even_rows = 0.75 * widened[:, 1:-1] + 0.25 * widened[:, :-2]
    odd_rows = 0.75 * widened[:, 1:-1] + 0.25 * widened[:, 2:]
    return jnp.stack([even_rows, odd_rows], 2).reshape(2 * first_extent, 2 * second_extent, depth)


def body(right_side, z_faces, xy_coupling, block_inverse):
    device_index = lax.axis_index("gz")
    levels_count = block_inverse.shape[0]
    last_cell = block_inverse.shape[1] - 1
    corner = jnp.stack(
        [
            block_inverse[:, 0, 0],
            block_inverse[:, 0, last_cell],
            block_inverse[:, last_cell, 0],
            block_inverse[:, last_cell, last_cell],
        ],
        -1,
    )[None]
    corners, firsts = (
        lax.all_gather(corner, "gz", axis=0, tiled=True),
        lax.all_gather(z_faces[:1], "gz", axis=0, tiled=True),
    )
    couplings = firsts[1:]
    edge_faces = jnp.concatenate([firsts, jnp.ones((1,), jnp.float32)])
    top_face = lax.dynamic_slice_in_dim(edge_faces, device_index + 1, 1, 0)
    up_faces = jnp.concatenate([z_faces[1:], top_face])
    solvers = [
        make_solver(
            block_inverse[level],
            corners[:, level],
            couplings,
            device_index,
            z_faces[0],
            top_face[0],
        )
        for level in range(levels_count)
    ]

    def operator(iterate, level):
        return apply_operator(iterate, xy_coupling[level], z_faces, up_faces)

    def multigrid_cycle(source, level):
        iterate = damping * solvers[level](source)
        iterate = iterate + damping * solvers[level](source - operator(iterate, level))
        if level == LEVELS - 1:
            return iterate
        coarse = multigrid_cycle(restrict(source - operator(iterate, level)), level + 1)
        widened = extended(coarse, (("gx", 0), ("gy", 1)), 1)
        iterate = iterate + prolong(widened)
        for sweep in range(SWEEPS):
            iterate = iterate + damping * solvers[level](source - operator(iterate, level))
        return iterate

    solution = multigrid_cycle(right_side, 0)
    return (solution, right_side - operator(solution, 0))


MESH = pl.DeviceIdType.MESH
HALOS = (4, 6, 6)
ROWS = (4, 5, 6)
YPAD = 8
SPARE = 32
DEEPEST = 3
NEAR = 2


def block_range(offset, own, halo, extent):
    start = offset * own - halo
    low = max(0, start)
    high = min(extent, (offset + 1) * own + halo)
    return low, high - low, low - start


def round_up(value, unit):
    return -(-value // unit) * unit


def difference(outer, inner):
    (a, b), (c, d) = outer
    (e, f), (g, h) = inner
    if e >= f or g >= h:
        return [outer]
    parts = [((a, e), (c, d)), ((f, b), (c, d)), ((e, f), (c, g)), ((e, f), (h, d))]
    return [(x, y) for x, y in parts if x[0] < x[1] and y[0] < y[1]]


def needed(t, dy, own, size, halos):
    (n0, n1), (s0, s1), (left, right, side) = own, size, halos
    x = max(0, t * n0 - left), min(s0, (t + 1) * n0 + right)
    y = max(0, dy * n1 - side), min(s1, (dy + 1) * n1 + side)
    return x, y


def vacant(part):
    return any(low >= high for low, high in part)


def both_parts(t, dy, own, size, near, far):
    whole = needed(t, dy, own, size, far)
    inner = needed(t, dy, own, size, near) if near else ((0, 0), (0, 0))
    common = tuple((max(a, c), min(b, d)) for (a, b), (c, d) in zip(whole, inner))
    outer = [] if vacant(whole) else difference(whole, common)
    return [] if vacant(inner) else [inner], outer


def area(parts):
    return sum((x[1] - x[0]) * (y[1] - y[0]) for x, y in parts)


def split_planes(count, rows):
    return max(c for c in range(1, count + 1) if count % c == 0 and c * rows <= 520)


def cycle_kernel(geometry, f_hbm, z_hbm, e_hbm, g_hbm, sol_ref, res_ref, *scratch):
    gx_n, gy_n, gz_n, nx, ny, depth, levels = geometry
    refs = iter(scratch)
    take = lambda count: [next(refs) for _ in range(count)]
    sinv, g_all, z_all, gather, f_v, e_ref = take(6)
    X = [take(3) for _ in range(DEEPEST + 1)]
    X.append(take(1))
    C = take(DEEPEST + 1)
    E = take(DEEPEST + 1)
    (U1, G1, U2, G2, c3u, c3g, c4u, c4g, cwu, cwg) = take(10)
    UP, GP = [None, U1, U2, c3u, c4u], [None, G1, G2, c3g, c4g]
    own3, pool = take(2)
    T = take(DEEPEST + 1)
    N = take(DEEPEST)
    (in_sem, g_send, g_recv, h_send, h_recv, y_recv, p_sem) = take(7)
    r_send, r_recv = take(2)
    y_send, x_send, x_recv, o_send, o_recv = [p_sem.at[i] for i in range(5)]

    ix, iy, iz = lax.axis_index("gx"), lax.axis_index("gy"), lax.axis_index("gz")
    bx = ix * gz_n + iz
    bx_n = gx_n * gz_n
    f32 = jnp.float32

    whole = gz_n * depth
    keep = 1.0 - damping

    def owned(level):
        return nx >> level, ny >> level

    def copy(src, dst, send, recv, device):
        return pltpu.make_async_remote_copy(
            src_ref=src,
            dst_ref=dst,
            send_sem=send,
            recv_sem=recv,
            device_id=device,
            device_id_type=MESH,
        )

    def inside(x, y):
        return (x >= 0) & (x < gx_n) & (y >= 0) & (y < gy_n)

    parts = 8
    span = f_v.shape[0] // parts
    for i in range(parts):
        at = pl.ds(i * span, span)
        pltpu.make_async_copy(f_hbm.at[at], f_v.at[at], in_sem.at[0]).start()
    f_load = pltpu.make_async_copy(f_hbm, f_v, in_sem.at[0])
    rest = pl.ds(1, levels - 1)
    loads = [
        pltpu.make_async_copy(z_hbm, z_all.at[iz], in_sem.at[1]),
        pltpu.make_async_copy(g_hbm.at[0], g_all.at[0, iz], in_sem.at[2]),
        pltpu.make_async_copy(g_hbm.at[rest], g_all.at[rest, iz], in_sem.at[3]),
        pltpu.make_async_copy(e_hbm, e_ref, in_sem.at[4]),
    ]
    reach_all = max(
        gz_n - 1 - (-HALOS[0] // nx), *[-(-HALOS[k] // owned(k)[0]) for k in (1, 2)]
    )
    barrier = pltpu.get_barrier_semaphore()
    partners = jnp.int32(0)
    offsets = [
        (dx, dy)
        for dx in range(-reach_all, reach_all + 1)
        for dy in (-1, 0, 1)
        if dx or dy
    ]
    offsets.sort(key=lambda offset: -abs(offset[0]) - 2 * abs(offset[1]))
    for dx, dy in offsets:
        x, y = bx + dx, iy + dy
        ok = (x >= 0) & (x < bx_n) & (y >= 0) & (y < gy_n)

        @pl.when(ok)
        def _():
            pl.semaphore_signal(
                barrier,
                inc=1,
                device_id=(x // gz_n, y, lax.rem(x, gz_n)),
                device_id_type=MESH,
            )

        partners = partners + jnp.where(ok, 1, 0).astype(jnp.int32)

    def setup_copies(other):
        here = (ix, iy, lax.rem(iz + other, gz_n))
        out = []
        for i, block in enumerate((z_all.at[iz], g_all.at[0, iz], g_all.at[rest, iz])):
            out.append(copy(block, block, g_send.at[i], g_recv.at[i], here))
        return out

    def runs(count, key):
        out = []
        for i in range(count):
            if out and key(i) == out[-1][2]:
                out[-1][1] = i
            else:
                out.append([i, i, key(i)])
        return [(low, high) for low, high, _ in out]

    def take_rows(sem, rows):
        block = pool.at[pl.ds(0, rows)]
        pltpu.make_async_copy(block, block, sem).wait()

    def settle(sem, total):
        table = [[total(b, y) for y in range(gy_n)] for b in range(bx_n)]
        for low, high in runs(bx_n, lambda b: table[b]):
            for first, last in runs(gy_n, lambda y: [row[y] for row in table]):

                @pl.when((bx >= low) & (bx <= high) & (iy >= first) & (iy <= last))
                def _():
                    take_rows(sem, table[low][first])

    near0, far0 = N[0], X[0][0]
    plan0 = []
    reach = -(-ROWS[0] // nx)
    for t in range(-reach, gz_n + reach):
        for dy in (-1, 0, 1):
            near_halo, far_halo = (NEAR,) * 3, (ROWS[0],) * 3
            parts0 = both_parts(t, dy, (nx, ny), (nx * gz_n, ny), near_halo, far_halo)
            plan0.append((t, t // gz_n, t % gz_n, dy, parts0))
    plan0.sort(key=lambda entry: -abs(entry[1]) - abs(entry[3]))

    def target0(window, part, t, dy, source_z):
        (x0, x1), (y0, y1) = part
        p, r = x0 - t * nx + HALOS[0], y0 - dy * ny + YPAD
        return window.at[pl.ds(p, x1 - x0), source_z, pl.ds(r, y1 - y0), :]

    local0 = []
    for t, dgx, target, dy, parts0 in plan0:
        if dgx == 0 and dy == 0:
            for which, window in enumerate((near0, far0)):
                for part in parts0[which]:
                    (x0, x1), (y0, y1) = part
                    move = pltpu.make_async_copy(
                        f_hbm.at[pl.ds(x0, x1 - x0), pl.ds(y0, y1 - y0), :],
                        target0(window, part, t, dy, target),
                        in_sem.at[5 + which],
                    )
                    local0.append((target, which, move))

    for target, _, move in local0:

        @pl.when(iz == target)
        def _():
            move.start()

    def local_done(which):
        for target, other, move in local0:
            if other == which:

                @pl.when(iz == target)
                def _():
                    move.wait()

    def send0(which):
        for t, dgx, target, dy, parts0 in plan0:
            ok = inside(ix + dgx, iy + dy)
            if dgx == 0 and dy == 0:
                ok = ok & (iz != target)

            @pl.when(ok)
            def _():
                for part in parts0[which]:
                    (x0, x1), (y0, y1) = part
                    copy(
                        f_v.at[pl.ds(x0, x1 - x0), pl.ds(y0, y1 - y0), :],
                        target0((near0, far0)[which], part, t, dy, iz),
                        h_send.at[0],
                        h_recv.at[0, which],
                        (ix + dgx, iy + dy, target),
                    ).start()

    def in_grid(b, y):
        return 0 <= b < bx_n and 0 <= y < gy_n

    def sent0(b, y):
        total = 0
        for t, dgx, target, dy, parts0 in plan0:
            there = (b // gz_n + dgx) * gz_n + target
            if in_grid(there, y + dy) and (there, dy) != (b, 0):
                total += area(parts0[0]) + area(parts0[1])
        return total

    def received0(which):
        def count(b, y):
            total = 0
            for t, dgx, target, dy, parts0 in plan0:
                for source_z in range(gz_n):
                    there = (b // gz_n - dgx) * gz_n + source_z
                    ok = target == b % gz_n and in_grid(there, y - dy)
                    if ok and (there, dy) != (b, 0):
                        total += area(parts0[which])
            return total

        return count

    def clear_edges():
        for level, window in [(k, w) for k in range(DEEPEST) for w in (N[k], X[k][0])]:
            planes, zb, rows, lanes = window.shape
            halo = HALOS[level]
            n0, n1 = owned(level)
            reach = -(-halo // n0)
            for t in range(1, reach + 1):
                low = max(0, halo - t * n0)
                high = halo - (t - 1) * n0
                plane = jnp.zeros((high - low, zb, n1 + 2 * YPAD, lanes), f32)

                @pl.when(bx - t < 0)
                def _():
                    window[low:high, :, pl.ds(0, n1 + 2 * YPAD)] = plane

                low2, high2 = planes - high, planes - low

                @pl.when(bx + t >= bx_n)
                def _():
                    window[low2:high2, :, pl.ds(0, n1 + 2 * YPAD)] = plane

            edge = jnp.zeros((zb, YPAD, lanes), f32)

            @pl.when(iy == 0)
            def _():
                lax.fori_loop(0, planes, lambda i, c: zero_rows(window, i, 0, edge), 0)

            @pl.when(iy == gy_n - 1)
            def _():
                lax.fori_loop(
                    0, planes, lambda i, c: zero_rows(window, i, YPAD + n1, edge), 0
                )

    def fill_border(ref, side):
        planes, zb, rows, lanes = ref.shape
        plane = jnp.zeros((side, zb, rows, lanes), f32)
        edge = jnp.zeros((zb, YPAD, lanes), f32)
        ref[0:side] = plane
        ref[planes - side : planes] = plane

        def step(i, _):
            ref[i, :, pl.ds(0, YPAD)] = edge
            ref[i, :, pl.ds(rows - YPAD, YPAD)] = edge
            return 0

        lax.fori_loop(side, planes - side, step, 0, unroll=4)

    def clear_coarse():
        side = HALOS[2] // 2 + 1
        for ref in (X[3][0], X[3][2], T[3], C[3], X[4][0], c4u, c4g):
            fill_border(ref, 1)
        for ref in (c3u, c3g):
            fill_border(ref, side)

    def assemble(level, _):
        merged = g_all[level, 0]
        for k in range(1, gz_n):
            block = g_all[level, k]
            size, cz = merged.shape[0], block.shape[0]
            face = z_all[k][:, 0:1]
            a, d = block[0:1, 0:1], merged[size - 1 : size, size - 1 : size]
            last, first = merged[size - 1 : size], block[0:1]
            scale = face / (1.0 - face * face * a * d)
            p_row = jnp.concatenate([face * a * last, first], 1) * scale
            q_row = jnp.concatenate([last, face * d * first], 1) * scale
            top = jnp.concatenate([merged, jnp.zeros((size, cz), f32)], 1)
            low = jnp.concatenate([jnp.zeros((cz, size), f32), block], 1)
            top = top + merged[:, size - 1 : size] * p_row
            low = low + block[:, 0:1] * q_row
            merged = jnp.concatenate([top, low], 0)
        solve = (damping * merged).astype(jnp.bfloat16)
        sinv[level, pl.ds(0, whole), :] = solve
        twice = jnp.dot(solve, solve, preferred_element_type=f32)
        sinv[level, pl.ds(whole, whole), :] = twice.astype(jnp.bfloat16)
        return 0

    def plane_mask(level, i):
        n0 = owned(level)[0]
        x = bx * n0 - HALOS[level] + i
        return jnp.where((x >= 0) & (x < bx_n * n0), 1.0, 0.0).astype(f32)

    def masked(level, p, value):
        if 0 <= p - HALOS[level] < owned(level)[0]:
            return value
        return value * plane_mask(level, p)

    def row_mask(level, first, rows, stride):
        n1 = owned(level)[1]
        y = lax.broadcasted_iota(jnp.int32, (rows, depth), 0) * stride + first
        y = y + iy * n1 - YPAD
        return jnp.where((y >= 0) & (y < gy_n * n1), 1.0, 0.0).astype(f32)

    def region(level, shrink=0):
        if level < DEEPEST:
            return nearby(level, ROWS[level] - shrink)
        window = X[level][0].shape
        return 1, window[0] - 2, YPAD, window[2] - 2 * YPAD

    def nearby(level, h, extra=0):
        n0, n1 = owned(level)
        first = HALOS[level] - h - extra
        return first, n0 + 2 * h + extra, YPAD - h, round_up(n1 + 2 * h, 8)

    def weights(level, p, c, r0, rows):
        e = e_ref[level]
        if level >= DEEPEST:
            return e
        mask = row_mask(level, r0, rows, 1) * e
        return jnp.stack([masked(level, p + i, mask) for i in range(c)])

    def chunks(where):
        p0, planes, r0, rows = where
        c = split_planes(planes, rows)
        return [(p0 + s * c, c, r0, rows) for s in range(planes // c)]

    def around(src, k, p, c, r0, rows):
        at = lambda dp, dr: src[pl.ds(p + dp, c), k, pl.ds(r0 + dr, rows)]
        return (at(-1, 0) + at(1, 0)) + (at(0, -1) + at(0, 1))

    def product(level, first, *groups):
        flat = [v.reshape(-1, depth) for fields in groups for v in fields]
        lhs = jnp.concatenate(flat, 1).astype(jnp.bfloat16)
        rhs = sinv[level, pl.ds(first * whole, len(groups) * whole), :]
        out = jnp.dot(lhs, rhs, preferred_element_type=f32)
        shape = groups[0][0].shape
        return [out[:, k * depth : (k + 1) * depth].reshape(shape) for k in range(gz_n)]

    def relax(level, src, dst, where):
        for p, c, r0, rows in chunks(where):
            w = weights(level, p, c, r0, rows)
            total = [around(src, k, p, c, r0, rows) * w for k in range(gz_n)]
            out = product(level, 0, total)
            for k in range(gz_n):
                value = keep * src[pl.ds(p, c), k, pl.ds(r0, rows)] + out[k]
                dst[pl.ds(p, c), k, pl.ds(r0, rows)] = value

    def spread(level, src, where):
        for p, c, r0, rows in chunks(where):
            w = weights(level, p, c, r0, rows)
            for k in range(gz_n):
                T[level][pl.ds(p, c), k, pl.ds(r0, rows)] = around(src, k, p, c, r0, rows) * w

    def relax_twice(level, src, where, once, put):
        for p, c, r0, rows in chunks(where):
            w = weights(level, p, c, r0, rows)
            at = lambda ref, k: ref[pl.ds(p, c), k, pl.ds(r0, rows)]
            one = [at(T[level], k) for k in range(gz_n)]
            two = [around(T[level], k, p, c, r0, rows) * w for k in range(gz_n)]
            if once is None:
                out = product(level, 0, [2.0 * keep * v for v in one], two)
            else:
                first, second = product(level, 0, one), product(level, 1, two)
                out = [second[k] + 2.0 * keep * first[k] for k in range(gz_n)]
            for k in range(gz_n):
                value = at(src, k)
                if once is not None:
                    once[pl.ds(p, c), k, pl.ds(r0, rows)] = keep * value + first[k]
                put(k, p, c, r0, rows, keep * keep * value + out[k])

    def into(ref):
        def put(k, p, c, r0, rows, value):
            ref[pl.ds(p, c), k, pl.ds(r0, rows)] = value

        return put

    def sums(level, p, c, r0, rows):
        at = lambda ref, k: ref[pl.ds(p, c), k, pl.ds(r0, rows)]
        last = X[level][-1]
        total = []
        for k in range(gz_n):
            value = (1.0 + keep) * at(last, k)
            if level <= DEEPEST:
                value = value + (at(X[level][0], k) + at(X[level][1], k))
            total.append(value)
        return total

    def finish(level, where, offset=0):
        last = X[level][-1]
        for p, c, r0, rows in chunks(where):
            w = weights(level, p, c, r0, rows)
            at = lambda ref, k: ref[pl.ds(p, c), k, pl.ds(r0, rows)]
            total = sums(level, p, c, r0, rows)
            side = [around(last, k, p, c, r0, rows) * w for k in range(gz_n)]
            rest = product(level, 0, side)
            u = product(level, 0, total, side)
            for k in range(gz_n):
                if level <= DEEPEST:
                    u[k] = u[k] + at(C[level], k)
                g = damping * (total[k] + rest[k])
                g = g + (4.0 * (e_ref[level - 1] - e_ref[level])) * u[k]
                if level <= DEEPEST:
                    g = g + at(E[level], k)
                UP[level][pl.ds(p + offset, c), k, pl.ds(r0, rows)] = u[k]
                GP[level][pl.ds(p + offset, c), k, pl.ds(r0, rows)] = g

    def finest(where, place):
        for p, c, r0, rows in chunks(where):
            at = lambda ref, k: ref[pl.ds(p, c), k, pl.ds(r0, rows)]
            total = sums(0, p, c, r0, rows)
            u = product(0, 0, total, [at(T[0], k) for k in range(gz_n)])
            for k in range(gz_n):
                sol_ref[k, pl.ds(place + p - where[0], c)] = u[k] + at(C[0], k)

    def restrict_planes(level, dst, planes, x0, y0, to_plane, to_row, rows):
        src = X[level][2]
        for j in range(planes):
            for k in range(gz_n):
                total = None
                for a in (0, 1):
                    for b in (0, 1):
                        part = src[x0 + 2 * j + a, k, pl.ds(y0 + b, rows, 2), :]
                        total = part if total is None else total + part
                dst[to_plane + j, k, pl.ds(to_row, rows), :] = total * 0.25

    def prolong(level, x0, y0, coarse):
        shift = 1 if level >= DEEPEST else 0
        p0, planes, r0, rows = region(level, 1)
        low, high = p0 - shift, p0 - shift + planes
        first = r0 // 2 * 2
        half = round_up((r0 + rows - first + 1) // 2, 8) if level < DEEPEST else rows // 2
        start = y0 + (first // 2 if level < DEEPEST else 0)
        masks = [
            row_mask(level, first + b, half, 2) if level < DEEPEST else None for b in (0, 1)
        ]
        def mixed(src, j, k):
            load = lambda dy: src[x0 + j, k, pl.ds(start + dy, half), :]
            quarter = 0.25 * load(0)
            near = load(0) - quarter
            out = []
            for dy in (-1, 1):
                value = near + 0.25 * load(dy)
                far = 0.25 * value
                out.append((value - far, far))
            return out

        first_j, last_j = low // 2, (high - 1) // 2
        for src, dst in coarse:
            for k in range(gz_n):
                behind, here = mixed(src, first_j - 1, k), mixed(src, first_j, k)
                for j in range(first_j, last_j + 1):
                    ahead = mixed(src, j + 1, k)
                    for a, beside in ((0, behind), (1, ahead)):
                        p = 2 * j + a
                        if not low <= p < high:
                            continue
                        for b in (0, 1):
                            value = here[b][0] + beside[b][1]
                            if level < DEEPEST:
                                value = masked(level, p, value * masks[b])
                            dst[p + shift, k, pl.ds(first + b, half, 2), :] = value
                    behind, here = here, ahead

    def correct(level, coarse_u, coarse_g, x0, y0):
        prolong(level, x0, y0, [(coarse_u, C[level]), (coarse_g, E[level])])
        where = region(level, 2)
        target = X[level][2]
        for p, c, r0, rows in chunks(where):
            w = weights(level, p, c, r0, rows)
            for k in range(gz_n):
                at = lambda ref: ref[pl.ds(p, c), k, pl.ds(r0, rows)]
                total = around(C[level], k, p, c, r0, rows) * w
                target[pl.ds(p, c), k, pl.ds(r0, rows)] = at(target) + (total - at(E[level]))

    def near_halos(level, core):
        if level < DEEPEST - 1:
            return (NEAR,) * 3
        if core < gz_n - 1:
            return None
        return NEAR + owned(level)[0] * core, NEAR, NEAR

    def far_halos(level, core):
        width = ROWS[level]
        return (0 if core else width), (width if core else 0), width

    def relay(level):
        n0, n1 = owned(level)
        width, halo = ROWS[level], HALOS[level]
        rows = pl.ds(YPAD - width, n1 + 2 * width)
        window = X[level][0]
        def move(core):
            src, dst = ((halo + n0 - width, halo - width), (halo, halo + n0))[core]
            return copy(
                window.at[pl.ds(src, width), :, rows, :],
                window.at[pl.ds(dst, width), :, rows, :],
                r_send.at[level - 1],
                r_recv.at[level - 1],
                (ix, iy, 1 - core),
            )

        return move

    def exchange(level):
        n0, n1 = owned(level)
        width = ROWS[level]
        halo = HALOS[level]
        reach = -(-width // n0)
        pieces = []
        for t in range(-reach, reach + 1):
            for dy in (-1, 0, 1):
                if t or dy:
                    parts = [
                        both_parts(
                            t,
                            dy,
                            (n0, n1),
                            (n0, n1),
                            near_halos(level, core),
                            far_halos(level, core),
                        )
                        for core in range(gz_n)
                    ]
                    pieces.append((t, dy, parts))
        pieces.sort(key=lambda piece: -abs(piece[0]) - abs(piece[1]))

        def start(which):
            window = (N[level], X[level][0])[which]
            for t, dy, parts in pieces:
                there = bx + t + bx_n
                core = lax.rem(there, gz_n)
                x, y = bx + t, iy + dy
                alike = all(part == parts[0] for part in parts)
                for target in range(1 if alike else gz_n):
                    ok = (x >= 0) & (x < bx_n) & (y >= 0) & (y < gy_n)
                    if not alike:
                        ok = ok & (core == target)
                    if not parts[target][which]:
                        continue

                    @pl.when(ok)
                    def _():
                        for (x0, x1), (y0, y1) in parts[target][which]:
                            p, r = x0 - t * n0 + halo, y0 - dy * n1 + YPAD
                            copy(
                                N[level].at[
                                    pl.ds(halo + x0, x1 - x0),
                                    :,
                                    pl.ds(YPAD + y0, y1 - y0),
                                    :,
                                ],
                                window.at[pl.ds(p, x1 - x0), :, pl.ds(r, y1 - y0), :],
                                h_send.at[level],
                                h_recv.at[level, which],
                                (there // gz_n - gx_n, y, core),
                            ).start()

        def total(sign, wanted):
            def count(b, y):
                rows = 0
                for t, dy, parts in pieces:
                    if in_grid(b + sign * t, y + sign * dy):
                        core = (b + t) % gz_n if sign > 0 else b % gz_n
                        rows += sum(gz_n * area(parts[core][which]) for which in wanted)
                return rows

            return count

        arrive = lambda which: settle(h_recv.at[level, which], total(-1, (which,)))
        return start, arrive, lambda: settle(h_send.at[level], total(1, (0, 1)))

    def gather_halo(level, arrive):
        n0, n1 = owned(level)
        for core in range(gz_n):
            near = near_halos(level, core) or (0, 0, 0)
            far = far_halos(level, core) if level else near
            left, right, side = (min(a, b) for a, b in zip(near, far))
            rows = pl.ds(YPAD - side, n1 + 2 * side)

            @pl.when(iz == core)
            def _():
                for p in range(HALOS[level] - left, HALOS[level] + n0 + right):
                    X[level][0][p, :, rows] = N[level][p, :, rows]

        arrive(1)
        if level:
            for core in range(gz_n):

                @pl.when(iz == core)
                def _():
                    relay(level)(core).start()

    def presmooth(level):
        if level:
            relay(level)(0).wait_recv()
        relax(level, X[level][0], X[level][1], region(level, 1))
        relax(level, X[level][1], X[level][2], region(level, 2))

    def gather_all(late):
        leader = gz_n - 1
        leading = iz == leader

        def line_y(other, slot):
            return copy(own3, gather.at[ix, slot], y_send, y_recv.at[slot], (ix, other, leader))

        def share(src, slot):
            for core in range(gz_n):
                for s in range(1, gx_n):
                    other = (lax.rem(ix + s, gx_n), iy, core)
                    copy(src, gather.at[ix, slot], x_send, x_recv, other).start()
            for core in range(leader):
                copy(src, gather.at[ix, slot], x_send, x_recv, (ix, iy, core)).start()

        @pl.when(leading)
        def _():
            for s in range(1, gy_n):
                line_y(lax.rem(iy + s, gy_n), iy).start()
            share(own3, iy)
            gather[ix, iy] = own3[...]
            for distance in range(1, gy_n):
                for y in (iy + distance, iy - distance):

                    @pl.when((y >= 0) & (y < gy_n))
                    def _():
                        line_y(y, y).wait_recv()
                        share(gather.at[ix, y], y)

        late()
        size = own3.shape[0] * own3.shape[1] * own3.shape[2]

        @pl.when(leading)
        def _():
            take_rows(x_recv, (gx_n - 1) * gy_n * size)

        @pl.when(iz < leader)
        def _():
            take_rows(x_recv, gx_n * gy_n * size)

        n0, n1 = owned(3)
        window = X[3][0]

        def place(b, _):
            for i in range(gz_n * n0):
                for y in range(gy_n):
                    at = 1 + b * gz_n * n0 + i
                    window[at, :, pl.ds(YPAD + y * n1, n1), :] = gather[b, y, i]
            return 0

        lax.fori_loop(0, gx_n, place, 0)

        def drains():
            @pl.when(leading)
            def _():
                take_rows(y_send, (gy_n - 1) * size)
                for _ in range(gy_n):
                    take_rows(x_send, (gx_n * gz_n - 1) * size)

        return drains

    for c in loads:
        c.start()
    f_load.wait()
    pl.semaphore_wait(barrier, partners)
    send0(0)
    for c in loads:
        c.wait()
    setups = [setup_copies(other) for other in range(1, gz_n)]
    for group in setups:
        for c in group[:2]:
            c.start()
    clear_edges()
    for group in setups:
        for c in group[:2]:
            c.wait()
    assemble(0, 0)
    send0(1)
    for group in setups:
        group[2].start()
    local_done(0)

    def arrive0(which):
        if which:
            local_done(1)
        settle(h_recv.at[0, which], received0(which))

    def later():
        for group in setups:
            group[2].wait()
        assemble(1, 0)

    arrive = arrive0
    drains = [lambda: settle(h_send.at[0], sent0)]
    for level in range(DEEPEST):
        arrive(0)
        extra = owned(level)[0] * (gz_n - 1) if level == DEEPEST - 1 else 0
        spread(level, N[level], nearby(level, 1, extra))
        relax_twice(level, N[level], nearby(level, 0, extra), None, into(X[level][2]))
        n0, n1 = owned(level + 1)
        p, r = HALOS[level], YPAD
        if level < DEEPEST - 1:
            restrict_planes(level, N[level + 1], n0, p, r, HALOS[level + 1], YPAD, n1)
            start, following, drain = exchange(level + 1)
            drains.append(drain)
            start(0)
            if level == 0:
                later()
                gather_halo(level, arrive)
                presmooth(level)
                behind = start
            else:
                lax.fori_loop(2, levels, assemble, 0)
                behind(1)
                clear_coarse()
                start(1)

                @pl.when(iz < gz_n - 1)
                def _():
                    gather_halo(level, arrive)

                before = arrive
            arrive = following
        else:
            restrict_planes(level, own3, gz_n * n0, p - extra, r, 0, 0, n1)

            def late():
                @pl.when(iz == gz_n - 1)
                def _():
                    gather_halo(level - 1, before)

                presmooth(level - 1)
                gather_halo(level, arrive)
                presmooth(level)

            drains.append(gather_all(late))

    whole3, whole4 = region(3, 0), region(4, 0)
    spread(3, X[3][0], whole3)
    relax_twice(3, X[3][0], whole3, X[3][1], into(X[3][2]))
    restrict_planes(3, X[4][0], whole4[1], 1, YPAD, 1, YPAD, whole4[3])
    finish(4, whole4)
    correct(3, c4u, c4g, 1, YPAD)
    pad3 = HALOS[2] // 2 + 1
    finish(3, whole3, offset=pad3 - 1)
    n0, n1 = owned(3)
    margin = YPAD // 2
    for y in range(gy_n):

        @pl.when(iy == y)
        def _():
            for j in range(HALOS[2] + 2 * n0):
                for src, dst in ((c3u, cwu), (c3g, cwg)):
                    dst[j, :, pl.ds(margin, n1 + 4 * margin), :] = src[
                        bx * n0 + j, :, pl.ds(y * n1, n1 + 4 * margin), :
                    ]

    for level in (2, 1, 0):
        if level == 2:
            correct(2, cwu, cwg, 1, YPAD)
        else:
            x0 = HALOS[level + 1] - HALOS[level] // 2
            correct(level, UP[level + 1], GP[level + 1], x0, YPAD // 2)
        if level:
            finish(level, region(level, 3))
        else:
            spread(0, X[0][2], region(0, 3))

    def send_out(ref, p, c):
        for other in range(1, gz_n):
            there = lax.rem(iz + other, gz_n)
            block = ref.at[there, pl.ds(iz * nx + p, c)]
            copy(block, block, o_send, o_recv, (ix, iy, there)).start()

    own0 = nearby(0, 0)
    finest(own0, iz * nx)
    send_out(sol_ref, 0, nx)

    def store(k, p, c, r0, rows, value):
        res_ref[k, pl.ds(iz * nx + p - own0[0], c)] = value

    relax_twice(0, X[0][2], own0, None, store)
    send_out(res_ref, 0, nx)
    for drain in drains:
        drain()
    for level in range(1, DEEPEST):
        relay(level)(0).wait_send()
    for sem in (o_send, o_recv):
        take_rows(sem, (gz_n - 1) * 2 * nx * ny)


def zero_rows(ref, i, at, value):
    ref[i, :, pl.ds(at, YPAD), :] = value
    return 0


def store_kernel(pieces, sol_v, res_v, sol_hbm, res_hbm, sem):
    iz = lax.axis_index("gz")
    span = sol_hbm.shape[0] // pieces
    moves = []
    for which, (src, dst) in enumerate(((sol_v, sol_hbm), (res_v, res_hbm))):
        for i in range(pieces):
            at = pl.ds(i * span, span)
            moves.append(
                pltpu.make_async_copy(src.at[iz, at], dst.at[at], sem.at[which, i])
            )
    for move in moves:
        move.start()
    for move in moves:
        move.wait()


def fits(mesh, shape, inverse_shape):
    gx_n, gy_n, gz_n = (mesh.shape[a] for a in ("gx", "gy", "gz"))
    nx, ny = shape[0] // (gx_n * gz_n), shape[1] // gy_n
    return (
        inverse_shape[0] == LEVELS == 5
        and SWEEPS == 2
        and inverse_shape[2] == 128
        and nx % 8 == 0
        and ny % 32 == 0
        and (shape[1] >> 4) % 8 == 0
        and gz_n == 2 and gy_n <= 4
    )


def fused_body(mesh, right_side, z_faces, xy_coupling, block_inverse):
    gx_n, gy_n, gz_n = (mesh.shape[a] for a in ("gx", "gy", "gz"))
    levels, _, depth = block_inverse.shape
    nx, ny = right_side.shape[0] // gz_n, right_side.shape[1]
    windows = []
    for level in range(levels):
        if level < DEEPEST:
            size = ((nx >> level) + 2 * HALOS[level], (ny >> level) + SPARE)
        else:
            size = (
                ((nx * gx_n * gz_n) >> level) + 2,
                ((ny * gy_n) >> level) + 2 * YPAD,
            )
        windows.append((size[0], gz_n, size[1], depth))
    vmem = lambda shape: pltpu.VMEM(shape, jnp.float32)
    full3, full4 = windows[3], windows[4]
    pad3 = HALOS[2] // 2 + 1
    c4 = full4
    c3 = (full3[0] - 2 + 2 * pad3,) + full3[1:]
    cw = (windows[2][0] // 2 + 2, gz_n, (ny >> 3) + 28, depth)
    most = gz_n * (nx + 2 * HALOS[0] + 8) * (ny + 2 * YPAD)
    dma = pltpu.SemaphoreType.DMA
    chip3 = (gz_n * (nx >> 3), gz_n, ny >> 3, depth)
    scratch = (
        [
            pltpu.VMEM((levels, 2 * gz_n * depth, gz_n * depth), jnp.bfloat16),
            vmem((levels, gz_n, depth, depth)),
            vmem((gz_n, 1, depth)),
            vmem((gx_n, gy_n) + chip3),
            vmem(right_side.shape),
            pltpu.SMEM((levels,), jnp.float32),
        ]
        + [vmem(w) for w in windows[: DEEPEST + 1] for _ in range(3)]
        + [vmem(full4)]
        + [vmem(w) for w in windows[: DEEPEST + 1]] * 2
        + [vmem(windows[1])] * 2
        + [vmem(windows[2])] * 2
        + [vmem(c3), vmem(c3), vmem(c4), vmem(c4), vmem(cw), vmem(cw)]
        + [vmem(chip3), vmem((most, depth))]
        + [vmem(w) for w in windows[: DEEPEST + 1]]
        + [vmem(w) for w in windows[:DEEPEST]]
        + [dma((7,))]
        + [dma((3,))] * 2
        + [dma((DEEPEST,)), dma((DEEPEST, 2))]
        + [dma((gy_n,)), dma((5,))]
        + [dma((DEEPEST - 1,))] * 2
    )
    in_vmem = pl.BlockSpec(memory_space=pltpu.VMEM)
    in_hbm = pl.BlockSpec(memory_space=pltpu.HBM)
    staged = (gz_n,) + right_side.shape
    hold = lambda x: pltpu.with_memory_space_constraint(x, pltpu.HBM)
    halves = pl.pallas_call(
        functools.partial(cycle_kernel, (gx_n, gy_n, gz_n, nx, ny, depth, levels)),
        out_shape=[pltpu.VMEM(staged, jnp.float32)] * 2,
        in_specs=[
            in_hbm,
            in_hbm,
            in_hbm,
            in_hbm,
        ],
        out_specs=[in_vmem, in_vmem],
        scratch_shapes=scratch,
        compiler_params=pltpu.CompilerParams(
            collective_id=0, has_side_effects=True, vmem_limit_bytes=48 * 1024 * 1024
        ),
    )(hold(right_side), hold(z_faces.reshape(1, -1)), hold(xy_coupling), hold(block_inverse))
    pieces = 2
    return tuple(
        pl.pallas_call(
            functools.partial(store_kernel, pieces),
            out_shape=[jax.ShapeDtypeStruct(right_side.shape, jnp.float32)] * 2,
            in_specs=[in_vmem, in_vmem],
            out_specs=[in_hbm, in_hbm],
            scratch_shapes=[dma((2, pieces))],
        )(*[pltpu.with_memory_space_constraint(x, pltpu.VMEM) for x in halves])
    )


def solution(mesh):
    def call(right_side, z_faces, xy_coupling, block_inverse):
        local = body
        if fits(mesh, right_side.shape, block_inverse.shape):
            local = functools.partial(fused_body, mesh)
        return jax.shard_map(
            local,
            mesh=mesh,
            in_specs=(P("gx", "gy", "gz"), P("gz"), P(), P(None, "gz", None)),
            out_specs=(P("gx", "gy", "gz"), P("gx", "gy", "gz")),
            check_vma=False,
        )(right_side, z_faces, xy_coupling, block_inverse)

    return call
```

```python
import functools

import jax
import jax.numpy as jnp
from jax import lax
from jax.experimental import pallas as pl
from jax.experimental.pallas import tpu as pltpu
from jax.sharding import PartitionSpec as P

LEVELS = 5
SWEEPS = 2


damping = 0.8
highest = lax.Precision.HIGHEST


def extended(cells, sides, width):
    for axis, dim in sides:
        count = lax.axis_size(axis)
        ends = count - 1
        head = lax.slice_in_dim(cells, 0, width, axis=dim)
        tail = lax.slice_in_dim(cells, cells.shape[dim] - width, cells.shape[dim], axis=dim)
        cells = jnp.concatenate(
            [
                lax.ppermute(tail, axis, [(i, (i + 1) % count) for i in range(ends)]),
                cells,
                lax.ppermute(head, axis, [((i + 1) % count, i) for i in range(ends)]),
            ],
            axis=dim,
        )
    return cells


def interface_setup(corner_aa, corner_ab, corner_ba, corner_bb, couplings):
    determinant = corner_aa * corner_bb - corner_ab * corner_ba
    corner_inverse = (
        jnp.stack(
            [jnp.stack([corner_bb, -corner_ab], -1), jnp.stack([-corner_ba, corner_aa], -1)], -2
        )
        / determinant[:, None, None]
    )
    blocks_count = corner_aa.shape[0]
    identity = jnp.eye(blocks_count, dtype=corner_inverse.dtype)
    diagonal_part = jnp.einsum("kab,kl->kalb", corner_inverse, identity, precision=highest).reshape(
        2 * blocks_count, 2 * blocks_count
    )
    link_values = jnp.zeros((2 * blocks_count - 1,), corner_inverse.dtype).at[1::2].set(-couplings)
    schur_matrix = diagonal_part + jnp.diag(link_values, 1) + jnp.diag(link_values, -1)
    return (corner_inverse, diagonal_part, jnp.linalg.cholesky(schur_matrix))


def make_solver(inverse_block, corner_rows, couplings, device_index, down_coupling, up_coupling):
    corner_inverse, diagonal_part, factor = interface_setup(
        corner_rows[:, 0], corner_rows[:, 1], corner_rows[:, 2], corner_rows[:, 3], couplings
    )
    block_len = inverse_block.shape[0]
    forward = lax.linalg.triangular_solve(factor, diagonal_part, left_side=True, lower=True)
    reach = lax.linalg.triangular_solve(
        factor, forward, left_side=True, lower=True, transpose_a=True
    )
    padded_reach = jnp.pad(reach, ((1, 1), (0, 0)))
    slice_rows = lax.dynamic_slice_in_dim(padded_reach, 2 * device_index, 4, 0)
    needed = jnp.stack([slice_rows[0], slice_rows[3]])

    def neighbours(end_values):
        zero_carry = jnp.zeros(end_values.shape, jnp.float32)
        nearby = zero_carry + jnp.dot(
            needed, lax.all_gather(end_values, "gz", axis=0, tiled=True), precision=highest
        )
        return (nearby[0], nearby[1])

    def solve(source):
        first_extent, second_extent, depth = source.shape
        line_count = first_extent * second_extent
        local_part = jnp.einsum("xyj,ij->xyi", source, inverse_block, precision=highest)
        end_values = jnp.stack(
            [
                local_part[:, :, 0].reshape(line_count),
                local_part[:, :, block_len - 1].reshape(line_count),
            ]
        )
        below_last, above_first = neighbours(end_values)
        return (
            local_part
            + (down_coupling * below_last).reshape(first_extent, second_extent, 1)
            * inverse_block[:, 0]
            + (up_coupling * above_first).reshape(first_extent, second_extent, 1)
            * inverse_block[:, block_len - 1]
        )

    return solve


def apply_operator(iterate, lateral_weight, down_faces, up_faces):
    padded = extended(iterate, (("gx", 0), ("gy", 1), ("gz", 2)), 1)
    lateral = (
        padded[:-2, 1:-1, 1:-1]
        + padded[2:, 1:-1, 1:-1]
        + padded[1:-1, :-2, 1:-1]
        + padded[1:-1, 2:, 1:-1]
    )
    return (
        lateral_weight * (4.0 * iterate - lateral)
        + down_faces * (iterate - padded[1:-1, 1:-1, :-2])
        + up_faces * (iterate - padded[1:-1, 1:-1, 2:])
    )


def restrict(field):
    first_extent, second_extent, depth = field.shape
    return field.reshape(first_extent // 2, 2, second_extent // 2, 2, depth).sum(axis=(1, 3)) * 0.25


def prolong(padded):
    first_extent = padded.shape[0] - 2
    second_extent = padded.shape[1] - 2
    depth = padded.shape[2]
    even_rows = 0.75 * padded[1:-1] + 0.25 * padded[:-2]
    odd_rows = 0.75 * padded[1:-1] + 0.25 * padded[2:]
    widened = jnp.stack([even_rows, odd_rows], 1).reshape(
        2 * first_extent, second_extent + 2, depth
    )
    even_rows = 0.75 * widened[:, 1:-1] + 0.25 * widened[:, :-2]
    odd_rows = 0.75 * widened[:, 1:-1] + 0.25 * widened[:, 2:]
    return jnp.stack([even_rows, odd_rows], 2).reshape(2 * first_extent, 2 * second_extent, depth)


def body(right_side, z_faces, xy_coupling, block_inverse):
    device_index = lax.axis_index("gz")
    levels_count = block_inverse.shape[0]
    last_cell = block_inverse.shape[1] - 1
    corner = jnp.stack(
        [
            block_inverse[:, 0, 0],
            block_inverse[:, 0, last_cell],
            block_inverse[:, last_cell, 0],
            block_inverse[:, last_cell, last_cell],
        ],
        -1,
    )[None]
    corners, firsts = (
        lax.all_gather(corner, "gz", axis=0, tiled=True),
        lax.all_gather(z_faces[:1], "gz", axis=0, tiled=True),
    )
    couplings = firsts[1:]
    edge_faces = jnp.concatenate([firsts, jnp.ones((1,), jnp.float32)])
    top_face = lax.dynamic_slice_in_dim(edge_faces, device_index + 1, 1, 0)
    up_faces = jnp.concatenate([z_faces[1:], top_face])
    solvers = [
        make_solver(
            block_inverse[level],
            corners[:, level],
            couplings,
            device_index,
            z_faces[0],
            top_face[0],
        )
        for level in range(levels_count)
    ]

    def operator(iterate, level):
        return apply_operator(iterate, xy_coupling[level], z_faces, up_faces)

    def multigrid_cycle(source, level):
        iterate = damping * solvers[level](source)
        iterate = iterate + damping * solvers[level](source - operator(iterate, level))
        if level == LEVELS - 1:
            return iterate
        coarse = multigrid_cycle(restrict(source - operator(iterate, level)), level + 1)
        widened = extended(coarse, (("gx", 0), ("gy", 1)), 1)
        iterate = iterate + prolong(widened)
        for sweep in range(SWEEPS):
            iterate = iterate + damping * solvers[level](source - operator(iterate, level))
        return iterate

    solution = multigrid_cycle(right_side, 0)
    return (solution, right_side - operator(solution, 0))


MESH = pl.DeviceIdType.MESH
HALOS = (4, 6, 6)
ROWS = (4, 5, 6)
YPAD = 8
SPARE = 32
DEEPEST = 3
NEAR = 2


def block_range(offset, own, halo, extent):
    start = offset * own - halo
    low = max(0, start)
    high = min(extent, (offset + 1) * own + halo)
    return low, high - low, low - start


def round_up(value, unit):
    return -(-value // unit) * unit


def difference(outer, inner):
    (a, b), (c, d) = outer
    (e, f), (g, h) = inner
    if e >= f or g >= h:
        return [outer]
    parts = [((a, e), (c, d)), ((f, b), (c, d)), ((e, f), (c, g)), ((e, f), (h, d))]
    return [(x, y) for x, y in parts if x[0] < x[1] and y[0] < y[1]]


def needed(t, dy, own, size, halos):
    (n0, n1), (s0, s1), (left, right, side) = own, size, halos
    x = max(0, t * n0 - left), min(s0, (t + 1) * n0 + right)
    y = max(0, dy * n1 - side), min(s1, (dy + 1) * n1 + side)
    return x, y


def vacant(part):
    return any(low >= high for low, high in part)


def both_parts(t, dy, own, size, near, far):
    whole = needed(t, dy, own, size, far)
    inner = needed(t, dy, own, size, near) if near else ((0, 0), (0, 0))
    common = tuple((max(a, c), min(b, d)) for (a, b), (c, d) in zip(whole, inner))
    outer = [] if vacant(whole) else difference(whole, common)
    return [] if vacant(inner) else [inner], outer


def area(parts):
    return sum((x[1] - x[0]) * (y[1] - y[0]) for x, y in parts)


def split_planes(count, rows):
    return max(c for c in range(1, count + 1) if count % c == 0 and c * rows <= 520)


def cycle_kernel(geometry, f_hbm, z_hbm, e_hbm, g_hbm, sol_ref, res_ref, *scratch):
    gx_n, gy_n, gz_n, nx, ny, depth, levels = geometry
    refs = iter(scratch)
    take = lambda count: [next(refs) for _ in range(count)]
    sinv, g_all, z_all, gather, f_v, e_ref = take(6)
    X = [take(3) for _ in range(DEEPEST + 1)]
    X.append(take(1))
    C = take(DEEPEST + 1)
    E = take(DEEPEST + 1)
    (U1, G1, U2, G2, c3u, c3g, c4u, c4g, cwu, cwg) = take(10)
    UP, GP = [None, U1, U2, c3u, c4u], [None, G1, G2, c3g, c4g]
    own3, pool = take(2)
    T = take(DEEPEST + 1)
    N = take(DEEPEST)
    (in_sem, g_send, g_recv, h_send, h_recv, y_recv, p_sem) = take(7)
    r_send, r_recv = take(2)
    y_send, x_send, x_recv, o_send, o_recv = [p_sem.at[i] for i in range(5)]

    ix, iy, iz = lax.axis_index("gx"), lax.axis_index("gy"), lax.axis_index("gz")
    bx = ix * gz_n + iz
    bx_n = gx_n * gz_n
    f32 = jnp.float32

    whole = gz_n * depth
    keep = 1.0 - damping

    def owned(level):
        return nx >> level, ny >> level

    def copy(src, dst, send, recv, device):
        return pltpu.make_async_remote_copy(
            src_ref=src,
            dst_ref=dst,
            send_sem=send,
            recv_sem=recv,
            device_id=device,
            device_id_type=MESH,
        )

    def inside(x, y):
        return (x >= 0) & (x < gx_n) & (y >= 0) & (y < gy_n)

    parts = 8
    span = f_v.shape[0] // parts
    for i in range(parts):
        at = pl.ds(i * span, span)
        pltpu.make_async_copy(f_hbm.at[at], f_v.at[at], in_sem.at[0]).start()
    f_load = pltpu.make_async_copy(f_hbm, f_v, in_sem.at[0])
    rest = pl.ds(1, levels - 1)
    loads = [
        pltpu.make_async_copy(z_hbm, z_all.at[iz], in_sem.at[1]),
        pltpu.make_async_copy(g_hbm.at[0], g_all.at[0, iz], in_sem.at[2]),
        pltpu.make_async_copy(g_hbm.at[rest], g_all.at[rest, iz], in_sem.at[3]),
        pltpu.make_async_copy(e_hbm, e_ref, in_sem.at[4]),
    ]
    reach_all = max(
        gz_n - 1 - (-HALOS[0] // nx), *[-(-HALOS[k] // owned(k)[0]) for k in (1, 2)]
    )
    barrier = pltpu.get_barrier_semaphore()
    partners = jnp.int32(0)
    offsets = [
        (dx, dy)
        for dx in range(-reach_all, reach_all + 1)
        for dy in (-1, 0, 1)
        if dx or dy
    ]
    offsets.sort(key=lambda offset: -abs(offset[0]) - 2 * abs(offset[1]))
    for dx, dy in offsets:
        x, y = bx + dx, iy + dy
        ok = (x >= 0) & (x < bx_n) & (y >= 0) & (y < gy_n)

        @pl.when(ok)
        def _():
            pl.semaphore_signal(
                barrier,
                inc=1,
                device_id=(x // gz_n, y, lax.rem(x, gz_n)),
                device_id_type=MESH,
            )

        partners = partners + jnp.where(ok, 1, 0).astype(jnp.int32)

    def setup_copies(other):
        here = (ix, iy, lax.rem(iz + other, gz_n))
        out = []
        for i, block in enumerate((z_all.at[iz], g_all.at[0, iz], g_all.at[rest, iz])):
            out.append(copy(block, block, g_send.at[i], g_recv.at[i], here))
        return out

    def runs(count, key):
        out = []
        for i in range(count):
            if out and key(i) == out[-1][2]:
                out[-1][1] = i
            else:
                out.append([i, i, key(i)])
        return [(low, high) for low, high, _ in out]

    def take_rows(sem, rows):
        block = pool.at[pl.ds(0, rows)]
        pltpu.make_async_copy(block, block, sem).wait()

    def settle(sem, total):
        table = [[total(b, y) for y in range(gy_n)] for b in range(bx_n)]
        for low, high in runs(bx_n, lambda b: table[b]):
            for first, last in runs(gy_n, lambda y: [row[y] for row in table]):

                @pl.when((bx >= low) & (bx <= high) & (iy >= first) & (iy <= last))
                def _():
                    take_rows(sem, table[low][first])

    near0, far0 = N[0], X[0][0]
    plan0 = []
    reach = -(-ROWS[0] // nx)
    for t in range(-reach, gz_n + reach):
        for dy in (-1, 0, 1):
            near_halo, far_halo = (NEAR,) * 3, (ROWS[0],) * 3
            parts0 = both_parts(t, dy, (nx, ny), (nx * gz_n, ny), near_halo, far_halo)
            plan0.append((t, t // gz_n, t % gz_n, dy, parts0))
    plan0.sort(key=lambda entry: -abs(entry[1]) - abs(entry[3]))

    def target0(window, part, t, dy, source_z):
        (x0, x1), (y0, y1) = part
        p, r = x0 - t * nx + HALOS[0], y0 - dy * ny + YPAD
        return window.at[pl.ds(p, x1 - x0), source_z, pl.ds(r, y1 - y0), :]

    local0 = []
    for t, dgx, target, dy, parts0 in plan0:
        if dgx == 0 and dy == 0:
            for which, window in enumerate((near0, far0)):
                for part in parts0[which]:
                    (x0, x1), (y0, y1) = part
                    move = pltpu.make_async_copy(
                        f_hbm.at[pl.ds(x0, x1 - x0), pl.ds(y0, y1 - y0), :],
                        target0(window, part, t, dy, target),
                        in_sem.at[5 + which],
                    )
                    local0.append((target, which, move))

    for target, _, move in local0:

        @pl.when(iz == target)
        def _():
            move.start()

    def local_done(which):
        for target, other, move in local0:
            if other == which:

                @pl.when(iz == target)
                def _():
                    move.wait()

    def send0(which):
        for t, dgx, target, dy, parts0 in plan0:
            ok = inside(ix + dgx, iy + dy)
            if dgx == 0 and dy == 0:
                ok = ok & (iz != target)

            @pl.when(ok)
            def _():
                for part in parts0[which]:
                    (x0, x1), (y0, y1) = part
                    copy(
                        f_v.at[pl.ds(x0, x1 - x0), pl.ds(y0, y1 - y0), :],
                        target0((near0, far0)[which], part, t, dy, iz),
                        h_send.at[0],
                        h_recv.at[0, which],
                        (ix + dgx, iy + dy, target),
                    ).start()

    def in_grid(b, y):
        return 0 <= b < bx_n and 0 <= y < gy_n

    def sent0(b, y):
        total = 0
        for t, dgx, target, dy, parts0 in plan0:
            there = (b // gz_n + dgx) * gz_n + target
            if in_grid(there, y + dy) and (there, dy) != (b, 0):
                total += area(parts0[0]) + area(parts0[1])
        return total

    def received0(which):
        def count(b, y):
            total = 0
            for t, dgx, target, dy, parts0 in plan0:
                for source_z in range(gz_n):
                    there = (b // gz_n - dgx) * gz_n + source_z
                    ok = target == b % gz_n and in_grid(there, y - dy)
                    if ok and (there, dy) != (b, 0):
                        total += area(parts0[which])
            return total

        return count

    def clear_edges():
        for level, window in [(k, w) for k in range(DEEPEST) for w in (N[k], X[k][0])]:
            planes, zb, rows, lanes = window.shape
            halo = HALOS[level]
            n0, n1 = owned(level)
            reach = -(-halo // n0)
            for t in range(1, reach + 1):
                low = max(0, halo - t * n0)
                high = halo - (t - 1) * n0
                plane = jnp.zeros((high - low, zb, n1 + 2 * YPAD, lanes), f32)

                @pl.when(bx - t < 0)
                def _():
                    window[low:high, :, pl.ds(0, n1 + 2 * YPAD)] = plane

                low2, high2 = planes - high, planes - low

                @pl.when(bx + t >= bx_n)
                def _():
                    window[low2:high2, :, pl.ds(0, n1 + 2 * YPAD)] = plane

            edge = jnp.zeros((zb, YPAD, lanes), f32)

            @pl.when(iy == 0)
            def _():
                lax.fori_loop(0, planes, lambda i, c: zero_rows(window, i, 0, edge), 0)

            @pl.when(iy == gy_n - 1)
            def _():
                lax.fori_loop(
                    0, planes, lambda i, c: zero_rows(window, i, YPAD + n1, edge), 0
                )

    def fill_border(ref, side):
        planes, zb, rows, lanes = ref.shape
        plane = jnp.zeros((side, zb, rows, lanes), f32)
        edge = jnp.zeros((zb, YPAD, lanes), f32)
        ref[0:side] = plane
        ref[planes - side : planes] = plane

        def step(i, _):
            ref[i, :, pl.ds(0, YPAD)] = edge
            ref[i, :, pl.ds(rows - YPAD, YPAD)] = edge
            return 0

        lax.fori_loop(side, planes - side, step, 0, unroll=4)

    def clear_coarse():
        side = HALOS[2] // 2 + 1
        for ref in (X[3][0], X[3][2], T[3], C[3], X[4][0], c4u, c4g):
            fill_border(ref, 1)
        for ref in (c3u, c3g):
            fill_border(ref, side)

    def assemble(level, _):
        merged = g_all[level, 0]
        for k in range(1, gz_n):
            block = g_all[level, k]
            size, cz = merged.shape[0], block.shape[0]
            face = z_all[k][:, 0:1]
            a, d = block[0:1, 0:1], merged[size - 1 : size, size - 1 : size]
            last, first = merged[size - 1 : size], block[0:1]
            scale = face / (1.0 - face * face * a * d)
            p_row = jnp.concatenate([face * a * last, first], 1) * scale
            q_row = jnp.concatenate([last, face * d * first], 1) * scale
            top = jnp.concatenate([merged, jnp.zeros((size, cz), f32)], 1)
            low = jnp.concatenate([jnp.zeros((cz, size), f32), block], 1)
            top = top + merged[:, size - 1 : size] * p_row
            low = low + block[:, 0:1] * q_row
            merged = jnp.concatenate([top, low], 0)
        solve = (damping * merged).astype(jnp.bfloat16)
        sinv[level, pl.ds(0, whole), :] = solve
        twice = jnp.dot(solve, solve, preferred_element_type=f32)
        sinv[level, pl.ds(whole, whole), :] = twice.astype(jnp.bfloat16)
        return 0

    def plane_mask(level, i):
        n0 = owned(level)[0]
        x = bx * n0 - HALOS[level] + i
        return jnp.where((x >= 0) & (x < bx_n * n0), 1.0, 0.0).astype(f32)

    def masked(level, p, value):
        if 0 <= p - HALOS[level] < owned(level)[0]:
            return value
        return value * plane_mask(level, p)

    def row_mask(level, first, rows, stride):
        n1 = owned(level)[1]
        y = lax.broadcasted_iota(jnp.int32, (rows, depth), 0) * stride + first
        y = y + iy * n1 - YPAD
        return jnp.where((y >= 0) & (y < gy_n * n1), 1.0, 0.0).astype(f32)

    def region(level, shrink=0):
        if level < DEEPEST:
            return nearby(level, ROWS[level] - shrink)
        window = X[level][0].shape
        return 1, window[0] - 2, YPAD, window[2] - 2 * YPAD

    def nearby(level, h, extra=0):
        n0, n1 = owned(level)
        first = HALOS[level] - h - extra
        return first, n0 + 2 * h + extra, YPAD - h, round_up(n1 + 2 * h, 8)

    def weights(level, p, c, r0, rows):
        e = e_ref[level]
        if level >= DEEPEST:
            return e
        mask = row_mask(level, r0, rows, 1) * e
        return jnp.stack([masked(level, p + i, mask) for i in range(c)])

    def chunks(where):
        p0, planes, r0, rows = where
        c = split_planes(planes, rows)
        return [(p0 + s * c, c, r0, rows) for s in range(planes // c)]

    def around(src, k, p, c, r0, rows):
        at = lambda dp, dr: src[pl.ds(p + dp, c), k, pl.ds(r0 + dr, rows)]
        return (at(-1, 0) + at(1, 0)) + (at(0, -1) + at(0, 1))

    def product(level, first, *groups):
        flat = [v.reshape(-1, depth) for fields in groups for v in fields]
        lhs = jnp.concatenate(flat, 1).astype(jnp.bfloat16)
        rhs = sinv[level, pl.ds(first * whole, len(groups) * whole), :]
        out = jnp.dot(lhs, rhs, preferred_element_type=f32)
        shape = groups[0][0].shape
        return [out[:, k * depth : (k + 1) * depth].reshape(shape) for k in range(gz_n)]

    def relax(level, src, dst, where):
        for p, c, r0, rows in chunks(where):
            w = weights(level, p, c, r0, rows)
            total = [around(src, k, p, c, r0, rows) * w for k in range(gz_n)]
            out = product(level, 0, total)
            for k in range(gz_n):
                value = keep * src[pl.ds(p, c), k, pl.ds(r0, rows)] + out[k]
                dst[pl.ds(p, c), k, pl.ds(r0, rows)] = value

    def spread(level, src, where):
        for p, c, r0, rows in chunks(where):
            w = weights(level, p, c, r0, rows)
            for k in range(gz_n):
                T[level][pl.ds(p, c), k, pl.ds(r0, rows)] = around(src, k, p, c, r0, rows) * w

    def relax_twice(level, src, where, once, put):
        for p, c, r0, rows in chunks(where):
            w = weights(level, p, c, r0, rows)
            at = lambda ref, k: ref[pl.ds(p, c), k, pl.ds(r0, rows)]
            one = [at(T[level], k) for k in range(gz_n)]
            two = [around(T[level], k, p, c, r0, rows) * w for k in range(gz_n)]
            if once is None:
                out = product(level, 0, [2.0 * keep * v for v in one], two)
            else:
                first, second = product(level, 0, one), product(level, 1, two)
                out = [second[k] + 2.0 * keep * first[k] for k in range(gz_n)]
            for k in range(gz_n):
                value = at(src, k)
                if once is not None:
                    once[pl.ds(p, c), k, pl.ds(r0, rows)] = keep * value + first[k]
                put(k, p, c, r0, rows, keep * keep * value + out[k])

    def into(ref):
        def put(k, p, c, r0, rows, value):
            ref[pl.ds(p, c), k, pl.ds(r0, rows)] = value

        return put

    def sums(level, p, c, r0, rows):
        at = lambda ref, k: ref[pl.ds(p, c), k, pl.ds(r0, rows)]
        last = X[level][-1]
        total = []
        for k in range(gz_n):
            value = (1.0 + keep) * at(last, k)
            if level <= DEEPEST:
                value = value + (at(X[level][0], k) + at(X[level][1], k))
            total.append(value)
        return total

    def finish(level, where, offset=0):
        last = X[level][-1]
        for p, c, r0, rows in chunks(where):
            w = weights(level, p, c, r0, rows)
            at = lambda ref, k: ref[pl.ds(p, c), k, pl.ds(r0, rows)]
            total = sums(level, p, c, r0, rows)
            side = [around(last, k, p, c, r0, rows) * w for k in range(gz_n)]
            rest = product(level, 0, side)
            u = product(level, 0, total, side)
            for k in range(gz_n):
                if level <= DEEPEST:
                    u[k] = u[k] + at(C[level], k)
                g = damping * (total[k] + rest[k])
                g = g + (4.0 * (e_ref[level - 1] - e_ref[level])) * u[k]
                if level <= DEEPEST:
                    g = g + at(E[level], k)
                UP[level][pl.ds(p + offset, c), k, pl.ds(r0, rows)] = u[k]
                GP[level][pl.ds(p + offset, c), k, pl.ds(r0, rows)] = g

    def finest(where, place):
        for p, c, r0, rows in chunks(where):
            at = lambda ref, k: ref[pl.ds(p, c), k, pl.ds(r0, rows)]
            total = sums(0, p, c, r0, rows)
            u = product(0, 0, total, [at(T[0], k) for k in range(gz_n)])
            for k in range(gz_n):
                sol_ref[k, pl.ds(place + p - where[0], c)] = u[k] + at(C[0], k)

    def restrict_planes(level, dst, planes, x0, y0, to_plane, to_row, rows):
        src = X[level][2]
        for j in range(planes):
            for k in range(gz_n):
                total = None
                for a in (0, 1):
                    for b in (0, 1):
                        part = src[x0 + 2 * j + a, k, pl.ds(y0 + b, rows, 2), :]
                        total = part if total is None else total + part
                dst[to_plane + j, k, pl.ds(to_row, rows), :] = total * 0.25

    def prolong(level, x0, y0, coarse):
        shift = 1 if level >= DEEPEST else 0
        p0, planes, r0, rows = region(level, 1)
        low, high = p0 - shift, p0 - shift + planes
        first = r0 // 2 * 2
        half = round_up((r0 + rows - first + 1) // 2, 8) if level < DEEPEST else rows // 2
        start = y0 + (first // 2 if level < DEEPEST else 0)
        masks = [
            row_mask(level, first + b, half, 2) if level < DEEPEST else None for b in (0, 1)
        ]
        def mixed(src, j, k):
            load = lambda dy: src[x0 + j, k, pl.ds(start + dy, half), :]
            quarter = 0.25 * load(0)
            near = load(0) - quarter
            out = []
            for dy in (-1, 1):
                value = near + 0.25 * load(dy)
                far = 0.25 * value
                out.append((value - far, far))
            return out

        first_j, last_j = low // 2, (high - 1) // 2
        for src, dst in coarse:
            for k in range(gz_n):
                behind, here = mixed(src, first_j - 1, k), mixed(src, first_j, k)
                for j in range(first_j, last_j + 1):
                    ahead = mixed(src, j + 1, k)
                    for a, beside in ((0, behind), (1, ahead)):
                        p = 2 * j + a
                        if not low <= p < high:
                            continue
                        for b in (0, 1):
                            value = here[b][0] + beside[b][1]
                            if level < DEEPEST:
                                value = masked(level, p, value * masks[b])
                            dst[p + shift, k, pl.ds(first + b, half, 2), :] = value
                    behind, here = here, ahead

    def correct(level, coarse_u, coarse_g, x0, y0):
        prolong(level, x0, y0, [(coarse_u, C[level]), (coarse_g, E[level])])
        where = region(level, 2)
        target = X[level][2]
        for p, c, r0, rows in chunks(where):
            w = weights(level, p, c, r0, rows)
            for k in range(gz_n):
                at = lambda ref: ref[pl.ds(p, c), k, pl.ds(r0, rows)]
                total = around(C[level], k, p, c, r0, rows) * w
                target[pl.ds(p, c), k, pl.ds(r0, rows)] = at(target) + (total - at(E[level]))

    def near_halos(level, core):
        if level < DEEPEST - 1:
            return (NEAR,) * 3
        if core < gz_n - 1:
            return None
        return NEAR + owned(level)[0] * core, NEAR, NEAR

    def far_halos(level, core):
        width = ROWS[level]
        return (0 if core else width), (width if core else 0), width

    def relay(level):
        n0, n1 = owned(level)
        width, halo = ROWS[level], HALOS[level]
        rows = pl.ds(YPAD - width, n1 + 2 * width)
        window = X[level][0]
        def move(core):
            src, dst = ((halo + n0 - width, halo - width), (halo, halo + n0))[core]
            return copy(
                window.at[pl.ds(src, width), :, rows, :],
                window.at[pl.ds(dst, width), :, rows, :],
                r_send.at[level - 1],
                r_recv.at[level - 1],
                (ix, iy, 1 - core),
            )

        return move

    def exchange(level):
        n0, n1 = owned(level)
        width = ROWS[level]
        halo = HALOS[level]
        reach = -(-width // n0)
        pieces = []
        for t in range(-reach, reach + 1):
            for dy in (-1, 0, 1):
                if t or dy:
                    parts = [
                        both_parts(
                            t,
                            dy,
                            (n0, n1),
                            (n0, n1),
                            near_halos(level, core),
                            far_halos(level, core),
                        )
                        for core in range(gz_n)
                    ]
                    pieces.append((t, dy, parts))
        pieces.sort(key=lambda piece: -abs(piece[0]) - abs(piece[1]))

        def start(which):
            window = (N[level], X[level][0])[which]
            for t, dy, parts in pieces:
                there = bx + t + bx_n
                core = lax.rem(there, gz_n)
                x, y = bx + t, iy + dy
                alike = all(part == parts[0] for part in parts)
                for target in range(1 if alike else gz_n):
                    ok = (x >= 0) & (x < bx_n) & (y >= 0) & (y < gy_n)
                    if not alike:
                        ok = ok & (core == target)
                    if not parts[target][which]:
                        continue

                    @pl.when(ok)
                    def _():
                        for (x0, x1), (y0, y1) in parts[target][which]:
                            p, r = x0 - t * n0 + halo, y0 - dy * n1 + YPAD
                            copy(
                                N[level].at[
                                    pl.ds(halo + x0, x1 - x0),
                                    :,
                                    pl.ds(YPAD + y0, y1 - y0),
                                    :,
                                ],
                                window.at[pl.ds(p, x1 - x0), :, pl.ds(r, y1 - y0), :],
                                h_send.at[level],
                                h_recv.at[level, which],
                                (there // gz_n - gx_n, y, core),
                            ).start()

        def total(sign, wanted):
            def count(b, y):
                rows = 0
                for t, dy, parts in pieces:
                    if in_grid(b + sign * t, y + sign * dy):
                        core = (b + t) % gz_n if sign > 0 else b % gz_n
                        rows += sum(gz_n * area(parts[core][which]) for which in wanted)
                return rows

            return count

        arrive = lambda which: settle(h_recv.at[level, which], total(-1, (which,)))
        return start, arrive, lambda: settle(h_send.at[level], total(1, (0, 1)))

    def gather_halo(level, arrive):
        n0, n1 = owned(level)
        for core in range(gz_n):
            near = near_halos(level, core) or (0, 0, 0)
            far = far_halos(level, core) if level else near
            left, right, side = (min(a, b) for a, b in zip(near, far))
            rows = pl.ds(YPAD - side, n1 + 2 * side)

            @pl.when(iz == core)
            def _():
                for p in range(HALOS[level] - left, HALOS[level] + n0 + right):
                    X[level][0][p, :, rows] = N[level][p, :, rows]

        arrive(1)
        if level:
            for core in range(gz_n):

                @pl.when(iz == core)
                def _():
                    relay(level)(core).start()

    def presmooth(level):
        if level:
            relay(level)(0).wait_recv()
        relax(level, X[level][0], X[level][1], region(level, 1))
        relax(level, X[level][1], X[level][2], region(level, 2))

    def gather_all(late):
        leader = gz_n - 1
        leading = iz == leader

        def line_y(other, slot):
            return copy(own3, gather.at[ix, slot], y_send, y_recv.at[slot], (ix, other, leader))

        def share(src, slot):
            for core in range(gz_n):
                for s in range(1, gx_n):
                    other = (lax.rem(ix + s, gx_n), iy, core)
                    copy(src, gather.at[ix, slot], x_send, x_recv, other).start()
            for core in range(leader):
                copy(src, gather.at[ix, slot], x_send, x_recv, (ix, iy, core)).start()

        @pl.when(leading)
        def _():
            for distance in range(gy_n - 1, 0, -1):
                for y in (iy + distance, iy - distance):

                    @pl.when((y >= 0) & (y < gy_n))
                    def _():
                        line_y(y, iy).start()

            share(own3, iy)
            gather[ix, iy] = own3[...]
            for distance in range(1, gy_n):
                for y in (iy + distance, iy - distance):

                    @pl.when((y >= 0) & (y < gy_n))
                    def _():
                        line_y(y, y).wait_recv()
                        share(gather.at[ix, y], y)

        late()
        size = own3.shape[0] * own3.shape[1] * own3.shape[2]

        @pl.when(leading)
        def _():
            take_rows(x_recv, (gx_n - 1) * gy_n * size)

        @pl.when(iz < leader)
        def _():
            take_rows(x_recv, gx_n * gy_n * size)

        n0, n1 = owned(3)
        window = X[3][0]

        def place(b, _):
            for i in range(gz_n * n0):
                for y in range(gy_n):
                    at = 1 + b * gz_n * n0 + i
                    window[at, :, pl.ds(YPAD + y * n1, n1), :] = gather[b, y, i]
            return 0

        lax.fori_loop(0, gx_n, place, 0)

        def drains():
            @pl.when(leading)
            def _():
                take_rows(y_send, (gy_n - 1) * size)
                for _ in range(gy_n):
                    take_rows(x_send, (gx_n * gz_n - 1) * size)

        return drains

    for c in loads:
        c.start()
    f_load.wait()
    pl.semaphore_wait(barrier, partners)
    send0(0)
    for c in loads:
        c.wait()
    setups = [setup_copies(other) for other in range(1, gz_n)]
    for group in setups:
        for c in group[:2]:
            c.start()
    clear_edges()
    for group in setups:
        for c in group[:2]:
            c.wait()
    assemble(0, 0)
    send0(1)
    for group in setups:
        group[2].start()
    local_done(0)

    def arrive0(which):
        if which:
            local_done(1)
        settle(h_recv.at[0, which], received0(which))

    def later():
        for group in setups:
            group[2].wait()
        assemble(1, 0)

    arrive = arrive0
    drains = [lambda: settle(h_send.at[0], sent0)]
    for level in range(DEEPEST):
        arrive(0)
        extra = owned(level)[0] * (gz_n - 1) if level == DEEPEST - 1 else 0
        spread(level, N[level], nearby(level, 1, extra))
        relax_twice(level, N[level], nearby(level, 0, extra), None, into(X[level][2]))
        n0, n1 = owned(level + 1)
        p, r = HALOS[level], YPAD
        if level < DEEPEST - 1:
            restrict_planes(level, N[level + 1], n0, p, r, HALOS[level + 1], YPAD, n1)
            start, following, drain = exchange(level + 1)
            drains.append(drain)
            start(0)
            if level == 0:
                later()
                gather_halo(level, arrive)
                presmooth(level)
                behind = start
            else:
                lax.fori_loop(2, levels, assemble, 0)
                behind(1)
                clear_coarse()
                start(1)

                @pl.when(iz < gz_n - 1)
                def _():
                    gather_halo(level, arrive)

                before = arrive
            arrive = following
        else:
            restrict_planes(level, own3, gz_n * n0, p - extra, r, 0, 0, n1)

            def late():
                @pl.when(iz == gz_n - 1)
                def _():
                    gather_halo(level - 1, before)

                presmooth(level - 1)
                gather_halo(level, arrive)
                presmooth(level)

            drains.append(gather_all(late))

    whole3, whole4 = region(3, 0), region(4, 0)
    spread(3, X[3][0], whole3)
    relax_twice(3, X[3][0], whole3, X[3][1], into(X[3][2]))
    restrict_planes(3, X[4][0], whole4[1], 1, YPAD, 1, YPAD, whole4[3])
    finish(4, whole4)
    correct(3, c4u, c4g, 1, YPAD)
    pad3 = HALOS[2] // 2 + 1
    finish(3, whole3, offset=pad3 - 1)
    n0, n1 = owned(3)
    margin = YPAD // 2
    for y in range(gy_n):

        @pl.when(iy == y)
        def _():
            for j in range(HALOS[2] + 2 * n0):
                for src, dst in ((c3u, cwu), (c3g, cwg)):
                    dst[j, :, pl.ds(margin, n1 + 4 * margin), :] = src[
                        bx * n0 + j, :, pl.ds(y * n1, n1 + 4 * margin), :
                    ]

    for level in (2, 1, 0):
        if level == 2:
            correct(2, cwu, cwg, 1, YPAD)
        else:
            x0 = HALOS[level + 1] - HALOS[level] // 2
            correct(level, UP[level + 1], GP[level + 1], x0, YPAD // 2)
        if level:
            finish(level, region(level, 3))
        else:
            spread(0, X[0][2], region(0, 3))

    def send_out(ref, p, c):
        for other in range(1, gz_n):
            there = lax.rem(iz + other, gz_n)
            block = ref.at[there, pl.ds(iz * nx + p, c)]
            copy(block, block, o_send, o_recv, (ix, iy, there)).start()

    own0 = nearby(0, 0)
    finest(own0, iz * nx)
    send_out(sol_ref, 0, nx)

    def store(k, p, c, r0, rows, value):
        res_ref[k, pl.ds(iz * nx + p - own0[0], c)] = value

    relax_twice(0, X[0][2], own0, None, store)
    send_out(res_ref, 0, nx)
    for drain in drains:
        drain()
    for level in range(1, DEEPEST):
        relay(level)(0).wait_send()
    for sem in (o_send, o_recv):
        take_rows(sem, (gz_n - 1) * 2 * nx * ny)


def zero_rows(ref, i, at, value):
    ref[i, :, pl.ds(at, YPAD), :] = value
    return 0


def store_kernel(pieces, sol_v, res_v, sol_hbm, res_hbm, sem):
    iz = lax.axis_index("gz")
    span = sol_hbm.shape[0] // pieces
    moves = []
    for which, (src, dst) in enumerate(((sol_v, sol_hbm), (res_v, res_hbm))):
        for i in range(pieces):
            at = pl.ds(i * span, span)
            moves.append(
                pltpu.make_async_copy(src.at[iz, at], dst.at[at], sem.at[which, i])
            )
    for move in moves:
        move.start()
    for move in moves:
        move.wait()


def fits(mesh, shape, inverse_shape):
    gx_n, gy_n, gz_n = (mesh.shape[a] for a in ("gx", "gy", "gz"))
    nx, ny = shape[0] // (gx_n * gz_n), shape[1] // gy_n
    return (
        inverse_shape[0] == LEVELS == 5
        and SWEEPS == 2
        and inverse_shape[2] == 128
        and nx % 8 == 0
        and ny % 32 == 0
        and (shape[1] >> 4) % 8 == 0
        and gz_n == 2 and gy_n <= 4
    )


def fused_body(mesh, right_side, z_faces, xy_coupling, block_inverse):
    gx_n, gy_n, gz_n = (mesh.shape[a] for a in ("gx", "gy", "gz"))
    levels, _, depth = block_inverse.shape
    nx, ny = right_side.shape[0] // gz_n, right_side.shape[1]
    windows = []
    for level in range(levels):
        if level < DEEPEST:
            size = ((nx >> level) + 2 * HALOS[level], (ny >> level) + SPARE)
        else:
            size = (
                ((nx * gx_n * gz_n) >> level) + 2,
                ((ny * gy_n) >> level) + 2 * YPAD,
            )
        windows.append((size[0], gz_n, size[1], depth))
    vmem = lambda shape: pltpu.VMEM(shape, jnp.float32)
    full3, full4 = windows[3], windows[4]
    pad3 = HALOS[2] // 2 + 1
    c4 = full4
    c3 = (full3[0] - 2 + 2 * pad3,) + full3[1:]
    cw = (windows[2][0] // 2 + 2, gz_n, (ny >> 3) + 28, depth)
    most = gz_n * (nx + 2 * HALOS[0] + 8) * (ny + 2 * YPAD)
    dma = pltpu.SemaphoreType.DMA
    chip3 = (gz_n * (nx >> 3), gz_n, ny >> 3, depth)
    scratch = (
        [
            pltpu.VMEM((levels, 2 * gz_n * depth, gz_n * depth), jnp.bfloat16),
            vmem((levels, gz_n, depth, depth)),
            vmem((gz_n, 1, depth)),
            vmem((gx_n, gy_n) + chip3),
            vmem(right_side.shape),
            pltpu.SMEM((levels,), jnp.float32),
        ]
        + [vmem(w) for w in windows[: DEEPEST + 1] for _ in range(3)]
        + [vmem(full4)]
        + [vmem(w) for w in windows[: DEEPEST + 1]] * 2
        + [vmem(windows[1])] * 2
        + [vmem(windows[2])] * 2
        + [vmem(c3), vmem(c3), vmem(c4), vmem(c4), vmem(cw), vmem(cw)]
        + [vmem(chip3), vmem((most, depth))]
        + [vmem(w) for w in windows[: DEEPEST + 1]]
        + [vmem(w) for w in windows[:DEEPEST]]
        + [dma((7,))]
        + [dma((3,))] * 2
        + [dma((DEEPEST,)), dma((DEEPEST, 2))]
        + [dma((gy_n,)), dma((5,))]
        + [dma((DEEPEST - 1,))] * 2
    )
    in_vmem = pl.BlockSpec(memory_space=pltpu.VMEM)
    in_hbm = pl.BlockSpec(memory_space=pltpu.HBM)
    staged = (gz_n,) + right_side.shape
    hold = lambda x: pltpu.with_memory_space_constraint(x, pltpu.HBM)
    halves = pl.pallas_call(
        functools.partial(cycle_kernel, (gx_n, gy_n, gz_n, nx, ny, depth, levels)),
        out_shape=[pltpu.VMEM(staged, jnp.float32)] * 2,
        in_specs=[
            in_hbm,
            in_hbm,
            in_hbm,
            in_hbm,
        ],
        out_specs=[in_vmem, in_vmem],
        scratch_shapes=scratch,
        compiler_params=pltpu.CompilerParams(
            collective_id=0, has_side_effects=True, vmem_limit_bytes=48 * 1024 * 1024
        ),
    )(hold(right_side), hold(z_faces.reshape(1, -1)), hold(xy_coupling), hold(block_inverse))
    pieces = 2
    return tuple(
        pl.pallas_call(
            functools.partial(store_kernel, pieces),
            out_shape=[jax.ShapeDtypeStruct(right_side.shape, jnp.float32)] * 2,
            in_specs=[in_vmem, in_vmem],
            out_specs=[in_hbm, in_hbm],
            scratch_shapes=[dma((2, pieces))],
        )(*[pltpu.with_memory_space_constraint(x, pltpu.VMEM) for x in halves])
    )


def solution(mesh):
    def call(right_side, z_faces, xy_coupling, block_inverse):
        local = body
        if fits(mesh, right_side.shape, block_inverse.shape):
            local = functools.partial(fused_body, mesh)
        return jax.shard_map(
            local,
            mesh=mesh,
            in_specs=(P("gx", "gy", "gz"), P("gz"), P(), P(None, "gz", None)),
            out_specs=(P("gx", "gy", "gz"), P("gx", "gy", "gz")),
            check_vma=False,
        )(right_side, z_faces, xy_coupling, block_inverse)

    return call
```
